256 devices in a mesh: dp: 16 (over x, y_hi, core), pencil: 16 (over z, y_lo).
Axes of the slice: x: 4, y: 4 (y_hi: 2, y_lo: 2; y = y_hi * 2 + y_lo), z: 8, core: 2. Of those that a mesh axis runs over, the one named last changes fastest.
Arguments:
- field: bfloat16 [16, 64, 64, 64, 128], P('dp', 'pencil'), may hold values from -6 to 6
- cotangent: bfloat16 [16, 64, 64, 64, 128], P('dp', 'pencil'), may hold values from -6 to 6
- w_spec: bfloat16 [16, 16, 16, 64, 128], P('dp', 'pencil'), may hold values from -6 to 6
- w_local: bfloat16 [64, 64], replicated, may hold values from -0.75 to 0.75
Outputs:
- grad_field: bfloat16 [16, 64, 64, 64, 128], P('dp', 'pencil')
- grad_w: float32 [16, 16, 16, 64, 128], P('dp', 'pencil')
The draws below stay inside these ranges and needn't reach their ends.
All inputs are finite; a program needn't handle non-finite values.
Results may differ from the reference program's by a relative error of at most 0.02.
Values may be sent and summed in bfloat16 or wider, within the bound.
A program may use at most 128 MiB of HBM per device.

```python
import math
import jax
import jax.numpy as jnp
from jax import lax

NX = 64
NY = 64
NZ = 128
CH = 64
MX = 16
MY = 16
MZ = 16
SAMPLES = 16


def block_levels(stream_key, shape, shards, smallest, largest):
    def one(dim, parts):
        draws = jax.random.uniform(jax.random.fold_in(jax.random.fold_in(stream_key, 6), dim), (parts,), jnp.float32, smallest / len(shards), largest / len(shards))
        return jnp.repeat(jnp.exp(draws), shape[dim] // parts).reshape((-1,) + (1,) * (len(shape) - dim - 1))

    level = one(*shards[0])
    for cut in shards[1:]:
        level = level * one(*cut)
    return level


def bell_draw(own_key, shape, scale, bound, cuts=(), kind=jnp.bfloat16):
    entries = jax.random.normal(own_key, shape, jnp.float32) * scale
    if len(cuts) > 0:
        entries = block_levels(own_key, shape, cuts, -0.22, 0.18) * entries
    return jnp.clip(entries, min=-bound, max=bound).astype(kind)


def setup_inputs(seed: int = 0) -> dict:
    arg_keys = jax.random.split(jax.random.key(seed), 5)
    field = bell_draw(arg_keys[0], (SAMPLES, NX, NY, CH, NZ), 1.0, 6.0, ((0, 16), (1, 16)))
    cotangent = bell_draw(arg_keys[1], (SAMPLES, NX, NY, CH, NZ), 1.0, 6.0, ((0, 16), (1, 16)))
    w_spec = bell_draw(arg_keys[2], (MX, MY, MZ, CH, 2 * CH), 1.0, 6.0, ((0, 16), (1, 16)))
    w_local = bell_draw(arg_keys[3], (CH, CH), CH ** -0.5, 0.75)
    return {"field": field, "cotangent": cotangent, "w_spec": w_spec, "w_local": w_local}


HIGHEST = lax.Precision.HIGHEST

def phase_pair(length, mode_count, signed):
    position = jnp.arange(length, dtype=jnp.int32)
    indices = jnp.arange(mode_count, dtype=jnp.int32)
    frequency = jnp.where(indices < mode_count // 2, indices, indices - mode_count) if signed else indices
    product = jnp.mod(position[:, None] * frequency[None, :], length).astype(jnp.float32)
    angles = product * (2.0 * math.pi / length)
    return (jnp.cos(angles), jnp.sin(angles))

def grid_tables():
    cos_x, sin_x = phase_pair(NX, MX, True)
    cos_y, sin_y = phase_pair(NY, MY, True)
    cos_z, sin_z = phase_pair(NZ, MZ, False)
    forward_z = jnp.concatenate([cos_z, -sin_z], 1).astype(jnp.bfloat16)
    weight_z = jnp.where(jnp.arange(MZ, dtype=jnp.int32) == 0, 1.0, 2.0).astype(jnp.float32) / (NX * NY * NZ)
    inverse_z = jnp.concatenate([cos_z * weight_z, -sin_z * weight_z], 1).T
    adjoint_z = jnp.concatenate([cos_z, -sin_z], 1).T
    spectrum_scale = jnp.concatenate([weight_z, weight_z])
    return (cos_x, sin_x, cos_y, sin_y, forward_z, inverse_z, adjoint_z, spectrum_scale)

def rotate_half(values):
    middle = values.shape[-1] // 2
    return jnp.concatenate([values[..., middle:], -values[..., :middle]], -1)

def along_y(values, cosines, sine_table, inverse):
    pattern = 'xjck,yj->xyck' if inverse else 'xyck,yj->xjck'
    factor = -1.0 if inverse else 1.0
    direct = jnp.einsum(pattern, values, cosines, precision=HIGHEST)
    turned = jnp.einsum(pattern, rotate_half(values), sine_table, precision=HIGHEST)
    return direct + factor * turned

def along_x(values, cosines, sine_table, inverse):
    pattern = 'jbck,xj->xbck' if inverse else 'xbck,xj->jbck'
    factor = -1.0 if inverse else 1.0
    direct = jnp.einsum(pattern, values, cosines, precision=HIGHEST)
    turned = jnp.einsum(pattern, rotate_half(values), sine_table, precision=HIGHEST)
    return direct + factor * turned

def z_forward(field_in, matrix):
    shape_in = field_in.shape
    product = jnp.dot(field_in.reshape(-1, shape_in[-1]), matrix, preferred_element_type=jnp.float32)
    return product.reshape(shape_in[:-1] + (matrix.shape[1],))

def z_back(values, matrix):
    shape_in = values.shape
    product = jnp.dot(values.reshape(-1, shape_in[-1]), matrix, precision=HIGHEST, preferred_element_type=jnp.float32)
    return product.reshape(shape_in[:-1] + (matrix.shape[1],))

def gelu_slope(pre):
    normal_cdf = 0.5 * (1.0 + lax.erf(pre * (1.0 / math.sqrt(2.0))))
    return normal_cdf + pre * jnp.exp(-0.5 * pre * pre) * (1.0 / math.sqrt(2.0 * math.pi))

def apply_modes(coeffs, weights):
    real_part = coeffs[..., :MZ]
    imag_part = coeffs[..., MZ:]
    from_real = jnp.einsum('abik,abkio->abok', real_part, weights, precision=HIGHEST)
    from_imag = jnp.einsum('abik,abkio->abok', imag_part, weights, precision=HIGHEST)
    out_real = from_real[:, :, :CH] - from_imag[:, :, CH:]
    out_imag = from_real[:, :, CH:] + from_imag[:, :, :CH]
    return jnp.concatenate([out_real, out_imag], -1)

def paired(g_modes):
    g_real = g_modes[..., :MZ]
    g_imag = g_modes[..., MZ:]
    return (jnp.concatenate([g_real, g_imag], -2), jnp.concatenate([g_imag, -g_real], -2))

def adjoint_modes(g_modes, weights):
    paired_one, paired_two = paired(g_modes)
    back_real = jnp.einsum('abkio,abok->abik', weights, paired_one, precision=HIGHEST)
    back_imag = jnp.einsum('abkio,abok->abik', weights, paired_two, precision=HIGHEST)
    return jnp.concatenate([back_real, back_imag], -1)

def mode_grads(u_modes, g_modes):
    paired_one, paired_two = paired(g_modes)
    from_real = jnp.einsum('abik,abok->abkio', u_modes[..., :MZ], paired_one, precision=HIGHEST)
    from_imag = jnp.einsum('abik,abok->abkio', u_modes[..., MZ:], paired_two, precision=HIGHEST)
    return from_real + from_imag

def reference(field, cotangent, w_spec, w_local):
    cos_x, sin_x, cos_y, sin_y, forward_z, inverse_z, adjoint_z, spectrum_scale = grid_tables()
    w_full = w_spec.astype(jnp.float32)
    w_bypass = w_local.astype(jnp.float32)

    def to_modes(field_in):
        sectioned = along_y(z_forward(field_in, forward_z), cos_y, sin_y, False)
        return along_x(sectioned, cos_x, sin_x, False)

    def to_grid(coeffs, matrix):
        sectioned = along_y(along_x(coeffs, cos_x, sin_x, True), cos_y, sin_y, True)
        return z_back(sectioned, matrix)

    def one_sample(accumulated, pair_in):
        sample, target = pair_in
        u_modes = lax.optimization_barrier(to_modes(sample).astype(jnp.bfloat16)).astype(jnp.float32)
        v_modes = apply_modes(u_modes, w_full)
        values = to_grid(v_modes, inverse_z)
        bypass = jnp.einsum('xycz,co->xyoz', sample.astype(jnp.float32), w_bypass, precision=HIGHEST)
        slope_in = (target.astype(jnp.float32) * gelu_slope(values + bypass)).astype(jnp.bfloat16)
        g_modes = lax.optimization_barrier((to_modes(slope_in) * spectrum_scale).astype(jnp.bfloat16)).astype(jnp.float32)
        accumulated = accumulated + mode_grads(u_modes, g_modes)
        back_modes = adjoint_modes(g_modes, w_full)
        spread = jnp.einsum('xyoz,co->xycz', slope_in.astype(jnp.float32), w_bypass, precision=HIGHEST)
        grad_sample = (to_grid(back_modes, adjoint_z) + spread).astype(jnp.bfloat16)
        return (accumulated, grad_sample)
    initial = jnp.zeros((MX, MY, MZ, CH, 2 * CH), jnp.float32)
    grad_w, grad_field = lax.scan(one_sample, initial, (field, cotangent))
    return (grad_field, grad_w)
```

```python
import functools
import math

import jax
import jax.numpy as jnp
import numpy as np
from jax import lax
from jax.experimental import pallas as pl
from jax.experimental.pallas import tpu as pltpu
from jax.sharding import PartitionSpec as P

NX = 64
NY = 64
NZ = 128
CH = 64
MX = 16
MY = 16
MZ = 16
MESH = pl.DeviceIdType.MESH
F32 = jnp.float32
BF16 = jnp.bfloat16
CHUNKS = 2
HC = CH // CHUNKS
SCALE = 1.0 / (NX * NY * NZ)


def line_table():
    position = np.arange(NX)
    freq = np.arange(MX)
    freq = np.where(freq < MX // 2, freq, freq - MX)
    angle = 2.0 * math.pi * np.mod(position[:, None] * freq[None, :], NX) / NX
    cos, sin = np.cos(angle), np.sin(angle)
    table = np.zeros((16, 2, 4, MZ, 2, MX, MZ), np.float32)
    cosg, sing = cos.reshape(16, 4, MX), sin.reshape(16, 4, MX)
    for k in range(MZ):
        table[:, 0, :, k, 0, :, k] = cosg
        table[:, 1, :, k, 0, :, k] = sing
        table[:, 1, :, k, 1, :, k] = cosg
        table[:, 0, :, k, 1, :, k] = -sing
    return table.reshape(2048, 512)


def z_table():
    angle = 2.0 * math.pi * np.mod(np.arange(NZ)[:, None] * np.arange(MZ)[None, :], NZ) / NZ
    table = np.zeros((4, NZ, 2, 4, MZ), np.float32)
    for q in range(4):
        table[q, :, 0, q, :] = np.cos(angle)
        table[q, :, 1, q, :] = -np.sin(angle)
    return table.reshape(512, 128)


def dot(a, b):
    return jnp.dot(a, b, preferred_element_type=F32)


def dot_t(a, b):
    return lax.dot_general(a, b, (((1,), (1,)), ((), ())), preferred_element_type=F32)


def gelu_slope(pre):
    normal_cdf = 0.5 * (1.0 + lax.erf(pre * (1.0 / math.sqrt(2.0))))
    return normal_cdf + pre * jnp.exp(-0.5 * pre * pre) * (1.0 / math.sqrt(2.0 * math.pi))


def kernel(
    field_hbm, cot_hbm, w_hbm, wl_hbm, t_hbm, zf_hbm, out_hbm, gw_hbm,
    f_ref, c_ref, w_ref, wl_ref, t_ref, zf_ref, big, slope, out_v, gw_v,
    a2, ly, vy, xo, xi, wb, bw, xf, vf, ukeep,
    s0, r0, s1, r1, s2, r2, s3, r3,
    us, ur, vs, vr, gs, gr, ds_, dr,
    lsem, osem, ssem, rsem,
):
    me_d = lax.axis_index("dp")
    me_p = lax.axis_index("pencil")

    def load(src, dst, i):
        return pltpu.make_async_copy(src, dst, lsem.at[i])

    loads = [load(field_hbm.at[0, x], f_ref.at[x], x) for x in range(4)]
    loads += [
        load(zf_hbm, zf_ref, 4),
        load(t_hbm, t_ref, 5),
        load(w_hbm.at[0, 0], w_ref, 6),
        load(wl_hbm, wl_ref, 7),
        load(cot_hbm.at[0], c_ref, 8),
    ]
    for i in (4, 0, 1, 2, 3, 5, 6, 7, 8):
        loads[i].start()

    barrier = pltpu.get_barrier_semaphore()

    @pl.loop(1, 16)
    def _(d):
        pl.semaphore_signal(
            barrier, inc=1, device_id=(me_d, lax.rem(me_p + d, 16)), device_id_type=MESH
        )
        pl.semaphore_signal(
            barrier, inc=1, device_id=(lax.rem(me_d + d, 16), me_p), device_id_type=MESH
        )

    def send_pencil(e, sb, rb, h):
        rb[me_p, pl.ds(h * HC, HC)] = sb[me_p, pl.ds(h * HC, HC)]

        @pl.loop(1, 16)
        def _(d):
            to = lax.rem(me_p + d, 16)
            pltpu.make_async_remote_copy(
                src_ref=sb.at[to, pl.ds(h * HC, HC)],
                dst_ref=rb.at[me_p, pl.ds(h * HC, HC)],
                send_sem=ssem.at[e],
                recv_sem=rsem.at[e],
                device_id=(me_d, to),
                device_id_type=MESH,
            ).start()

    def send_dp(e, sb, rb):
        rb[me_d] = sb[me_d]

        @pl.loop(1, 16)
        def _(d):
            to = lax.rem(me_d + d, 16)
            pltpu.make_async_remote_copy(
                src_ref=sb.at[to],
                dst_ref=rb.at[me_d],
                send_sem=ssem.at[e],
                recv_sem=rsem.at[e],
                device_id=(to, me_p),
                device_id_type=MESH,
            ).start()

    def wait_pencil(sem, buf, h):
        part = buf.at[pl.ds(0, 15), pl.ds(h * HC, HC)]
        pltpu.make_async_copy(part, part, sem).wait()

    def wait_dp(sem, buf):
        part = buf.at[pl.ds(0, 15)]
        pltpu.make_async_copy(part, part, sem).wait()

    slot = lax.broadcasted_iota(jnp.int32, (HC, 128), 1) // 16
    masks = [slot == m for m in range(8)]

    def merge(pieces):
        out = pieces[0]
        for m in range(1, 8):
            out = jnp.where(masks[m], pieces[m], out)
        return out

    def roll(v, amount):
        amount %= 128
        return v if amount == 0 else pltpu.roll(v, amount, 1)

    def z_forward(x, h, get):
        lhs = jnp.concatenate([get(q).reshape(16 * HC, 128) for q in range(4)], axis=1)
        a = dot(lhs, zf_ref[...]).astype(BF16).reshape(16, HC, 128)
        row = pl.multiple_of(x * HC, HC)
        for g in range(16):
            a2[pl.ds(row, HC), g * 128 : (g + 1) * 128] = a[g]

    def y_forward(sb, h):
        y = dot(a2[...], t_ref[...])
        for jh in range(2):
            rolled = []
            for e in range(8):
                ri, x = e // 4, e % 4
                tile = y[x * HC : (x + 1) * HC, (ri * 2 + jh) * 128 : (ri * 2 + jh + 1) * 128]
                rolled.append(roll(tile, 16 * e))
            for j8 in range(8):
                res = merge([rolled[(m - j8) % 8] for m in range(8)])
                sb[jh * 8 + j8, h * HC : (h + 1) * HC, :] = roll(res, -16 * j8).astype(BF16)

    def y_inverse(rb, h):
        for jh in range(2):
            rolled = [
                roll(rb[jh * 8 + j8, h * HC : (h + 1) * HC, :].astype(F32), 16 * j8)
                for j8 in range(8)
            ]
            for e in range(8):
                ri, x = e // 4, e % 4
                res = merge([rolled[(m - e) % 8] for m in range(8)])
                ly[
                    x * HC : (x + 1) * HC, (ri * 2 + jh) * 128 : (ri * 2 + jh + 1) * 128
                ] = roll(res, -16 * e).astype(BF16)
        vy[...] = dot_t(ly[...], t_ref[...]).astype(BF16)

    def x_forward(rb, h):
        lhs = jnp.concatenate([rb[p, h * HC : (h + 1) * HC, :] for p in range(16)], axis=1)
        xo[h * HC : (h + 1) * HC, :] = dot(lhs, t_ref[...])

    def modes_out(dst, scale):
        both = jnp.concatenate([xo[:, :256], xo[:, 256:]], axis=0)
        turned = both.T.reshape(16, 16, 128)
        if scale is not None:
            turned = turned * scale
        dst[...] = turned.astype(BF16)

    def modes_in(src):
        both = src[...].astype(F32).reshape(256, 128).T
        xi[...] = jnp.concatenate([both[:64], both[64:]], axis=1).astype(BF16)

    def x_inverse(sb, h):
        o = dot_t(xi[h * HC : (h + 1) * HC, :], t_ref[...]).astype(BF16)
        for p in range(16):
            sb[p, h * HC : (h + 1) * HC, :] = o[:, p * 128 : (p + 1) * 128]

    def mix(lhs, src, dst):
        @pl.loop(0, 4)
        def _(x):
            @pl.loop(0, 8)
            def _(gp):
                g = gp * 2
                rhs = jnp.concatenate(
                    [src[x, g].reshape(256, 128), src[x, g + 1].reshape(256, 128)], axis=1
                )
                o = dot(lhs, rhs)
                dst[x, g] = o[:, :128].reshape(4, CH, 128)
                dst[x, g + 1] = o[:, 128:].reshape(4, CH, 128)

    load_z = loads[4]
    load_z.wait()
    for h in range(CHUNKS):
        for x in range(4):
            if h == 0:
                loads[x].wait()
            z_forward(x, h, lambda q: f_ref[x, :, q, h * HC : (h + 1) * HC, :])
        if h == 0:
            loads[5].wait()
        y_forward(s0, h)
        if h == 0:
            pl.semaphore_wait(barrier, 30)
        send_pencil(h, s0, r0, h)

    loads[6].wait()
    loads[7].wait()
    for k in range(MZ):
        w = w_ref[k].astype(F32)
        turned = pltpu.roll(w, 64, 1)
        lane = lax.broadcasted_iota(jnp.int32, (64, 128), 1)
        turned = jnp.where(lane < 64, -turned, turned)
        wb[k] = jnp.concatenate([w, turned], axis=0).astype(BF16)
    wl = wl_ref[...].astype(F32)
    wide = jnp.concatenate([wl] * 4, axis=1)
    tall = jnp.concatenate([wide] * 4, axis=0)
    row = lax.broadcasted_iota(jnp.int32, (256, 256), 0) // 64
    col = lax.broadcasted_iota(jnp.int32, (256, 256), 1) // 64
    block = jnp.where(row == col, tall, 0.0)
    bw[0] = block.T.astype(BF16)
    bw[1] = block.astype(BF16)
    mix(bw[0], f_ref, big)

    for h in range(CHUNKS):
        wait_pencil(rsem.at[h], r0, h)
        x_forward(r0, h)
    modes_out(us, None)
    send_dp(2, us, ur)
    wait_dp(rsem.at[2], ur)

    def regroup(src, keep):
        xf[...] = src[...].astype(F32).reshape(256, 128)
        for k in range(MZ):
            keep[k] = xf[pl.ds(k, 16, stride=16), :].astype(BF16)

    regroup(ur, ukeep.at[0])
    for k in range(MZ):
        scale = SCALE if k == 0 else 2.0 * SCALE
        vf[pl.ds(k, 16, stride=16), :] = dot(ukeep[0, k], wb[k]) * scale
    vs[...] = vf[...].astype(BF16).reshape(16, 16, 128)
    send_dp(3, vs, vr)
    wait_dp(rsem.at[3], vr)

    modes_in(vr)
    for h in range(CHUNKS):
        x_inverse(s1, h)
        send_pencil(4 + h, s1, r1, h)
    loads[8].wait()

    for h in range(CHUNKS):
        wait_pencil(rsem.at[4 + h], r1, h)
        y_inverse(r1, h)

        @pl.loop(0, 4)
        def _(x, h=h):
            row = pl.multiple_of(x * HC, HC)
            for gq in range(4):
                lhs = jnp.concatenate(
                    [vy[pl.ds(row, HC), g * 128 : (g + 1) * 128] for g in range(gq * 4, gq * 4 + 4)],
                    axis=0,
                )
                v = dot_t(lhs, zf_ref[...])
                parts = []
                for q in range(4):
                    pre = v[:, q * 128 : (q + 1) * 128].reshape(4, HC, 128)
                    at = (x, slice(gq * 4, gq * 4 + 4), q, slice(h * HC, (h + 1) * HC))
                    pre = pre + big[at]
                    sl = (c_ref[at].astype(F32) * gelu_slope(pre)).astype(BF16)
                    slope[at] = sl
                    parts.append(sl.reshape(4 * HC, 128))
                a = dot(jnp.concatenate(parts, axis=1), zf_ref[...]).astype(BF16)
                for i in range(4):
                    g = gq * 4 + i
                    a2[pl.ds(row, HC), g * 128 : (g + 1) * 128] = a[i * HC : (i + 1) * HC]

        y_forward(s2, h)
        send_pencil(6 + h, s2, r2, h)

    mix(bw[1], slope, big)

    for h in range(CHUNKS):
        wait_pencil(rsem.at[6 + h], r2, h)
        x_forward(r2, h)
    kk = lax.broadcasted_iota(jnp.int32, (16, 16, 128), 1)
    modes_out(gs, jnp.where(kk == 0, SCALE, 2.0 * SCALE).astype(F32))
    send_dp(8, gs, gr)
    wait_dp(rsem.at[8], gr)

    regroup(gr, ukeep.at[1])
    for k in range(MZ):
        vf[pl.ds(k, 16, stride=16), :] = dot_t(ukeep[1, k], wb[k])
    ds_[...] = vf[...].astype(BF16).reshape(16, 16, 128)
    send_dp(9, ds_, dr)

    lane = lax.broadcasted_iota(jnp.int32, (64, 128), 1)
    for k in range(MZ):
        cross = lax.dot_general(
            ukeep[0, k], ukeep[1, k], (((0,), (0,)), ((), ())), preferred_element_type=F32
        )
        low = pltpu.roll(cross[64:], 64, 1)
        gw_v[k] = cross[:64] + jnp.where(lane < 64, low, -low)
    gw_copy = pltpu.make_async_copy(gw_v, gw_hbm.at[0, 0], osem.at[2 * 4])
    gw_copy.start()

    wait_dp(rsem.at[9], dr)
    modes_in(dr)
    for h in range(CHUNKS):
        x_inverse(s3, h)
        send_pencil(10 + h, s3, r3, h)

    outs = []
    for h in range(CHUNKS):
        wait_pencil(rsem.at[10 + h], r3, h)
        y_inverse(r3, h)
        for x in range(4):
            for gq in range(4):
                lhs = jnp.concatenate(
                    [
                        vy[x * HC : (x + 1) * HC, g * 128 : (g + 1) * 128]
                        for g in range(gq * 4, gq * 4 + 4)
                    ],
                    axis=0,
                )
                v = dot_t(lhs, zf_ref[...])
                for q in range(4):
                    at = (x, slice(gq * 4, gq * 4 + 4), q, slice(h * HC, (h + 1) * HC))
                    out_v[at] = (v[:, q * 128 : (q + 1) * 128].reshape(4, HC, 128) + big[at]).astype(BF16)
            part = (x, slice(None), slice(None), pl.ds(h * HC, HC))
            copy = pltpu.make_async_copy(
                out_v.at[part], out_hbm.at[(0,) + part], osem.at[h * 4 + x]
            )
            copy.start()
            outs.append(copy)

    for h in range(CHUNKS):
        wait_pencil(ssem.at[h], s0, h)
        wait_pencil(ssem.at[4 + h], s1, h)
        wait_pencil(ssem.at[6 + h], s2, h)
        wait_pencil(ssem.at[10 + h], s3, h)
    wait_dp(ssem.at[2], us)
    wait_dp(ssem.at[3], vs)
    wait_dp(ssem.at[8], gs)
    wait_dp(ssem.at[9], ds_)
    gw_copy.wait()
    for copy in outs:
        copy.wait()


def body(field, cotangent, w_spec, w_local):
    table = jnp.asarray(line_table().astype(jnp.bfloat16))
    zf = jnp.asarray(z_table().astype(jnp.bfloat16))
    shape6 = (1, 4, 16, 4, CH, NZ)
    any_spec = pl.BlockSpec(memory_space=pl.ANY)
    pencil_buf = pltpu.VMEM((16, CH, 128), BF16)
    dp_buf = pltpu.VMEM((16, 16, 128), BF16)
    grid_f32 = pltpu.VMEM((4, 16, 4, CH, NZ), F32)
    grid_b16 = pltpu.VMEM((4, 16, 4, CH, NZ), BF16)
    out, gw = pl.pallas_call(
        kernel,
        out_shape=(
            jax.ShapeDtypeStruct(shape6, BF16),
            jax.ShapeDtypeStruct((1, 1, MZ, CH, 2 * CH), F32),
        ),
        in_specs=[any_spec] * 6,
        out_specs=[any_spec] * 2,
        scratch_shapes=[
            grid_b16,
            grid_b16,
            pltpu.VMEM((MZ, CH, 2 * CH), BF16),
            pltpu.VMEM((CH, CH), BF16),
            pltpu.VMEM((2048, 512), BF16),
            pltpu.VMEM((512, 128), BF16),
            grid_f32,
            grid_b16,
            grid_b16,
            pltpu.VMEM((MZ, CH, 2 * CH), F32),
            pltpu.VMEM((4 * HC, 2048), BF16),
            pltpu.VMEM((4 * HC, 512), BF16),
            pltpu.VMEM((4 * HC, 2048), BF16),
            pltpu.VMEM((CH, 512), F32),
            pltpu.VMEM((CH, 512), BF16),
            pltpu.VMEM((MZ, 128, 128), BF16),
            pltpu.VMEM((2, 256, 256), BF16),
            pltpu.VMEM((256, 128), F32),
            pltpu.VMEM((256, 128), F32),
            pltpu.VMEM((2, 16, 16, 128), BF16),
        ]
        + [pencil_buf] * 8
        + [dp_buf] * 8
        + [
            pltpu.SemaphoreType.DMA((9,)),
            pltpu.SemaphoreType.DMA((9,)),
            pltpu.SemaphoreType.DMA((12,)),
            pltpu.SemaphoreType.DMA((12,)),
        ],
        compiler_params=pltpu.CompilerParams(
            collective_id=0, has_side_effects=True, vmem_limit_bytes=60 * 1024 * 1024
        ),
        name="layer",
    )(field.reshape(shape6), cotangent.reshape(shape6), w_spec, w_local, table, zf)
    return (out.reshape(1, 4, NY, CH, NZ), gw)


def solution(mesh):
    placed = P("dp", "pencil", None, None, None)
    return jax.shard_map(
        body,
        mesh=mesh,
        in_specs=(placed, placed, placed, P()),
        out_specs=(placed, placed),
        check_vma=False,
    )
```

```python
import functools
import math

import jax
import jax.numpy as jnp
import numpy as np
from jax import lax
from jax.experimental import pallas as pl
from jax.experimental.pallas import tpu as pltpu
from jax.sharding import PartitionSpec as P

NX = 64
NY = 64
NZ = 128
CH = 64
MX = 16
MY = 16
MZ = 16
KH = 8
MESH = pl.DeviceIdType.MESH
F32 = jnp.float32
BF16 = jnp.bfloat16
CHUNKS = 2
HC = CH // CHUNKS
SCALE = 1.0 / (NX * NY * NZ)


def line_table():
    position = np.arange(NX)
    freq = np.arange(MX)
    freq = np.where(freq < MX // 2, freq, freq - MX)
    angle = 2.0 * math.pi * np.mod(position[:, None] * freq[None, :], NX) / NX
    cos, sin = np.cos(angle).reshape(8, 2, 4, MX), np.sin(angle).reshape(8, 2, 4, MX)
    table = np.zeros((8, 2, 2, 4, KH, 2, MX, KH), np.float32)
    for k in range(KH):
        table[:, :, 0, :, k, 0, :, k] = cos
        table[:, :, 1, :, k, 0, :, k] = sin
        table[:, :, 1, :, k, 1, :, k] = cos
        table[:, :, 0, :, k, 1, :, k] = -sin
    return table.reshape(1024, 256)


def z_table():
    angle = 2.0 * math.pi * np.mod(np.arange(NZ)[:, None] * np.arange(MZ)[None, :], NZ) / NZ
    angle = angle.reshape(NZ, 2, KH)
    table = np.zeros((2, 4, NZ, 2, 2, 2, 4, KH), np.float32)
    for half in range(2):
        for q in range(4):
            table[half, q, :, :, half, 0, q, :] = np.cos(angle)
            table[half, q, :, :, half, 1, q, :] = -np.sin(angle)
    return table.reshape(1024, 256)


def dot(a, b):
    return jnp.dot(a, b, preferred_element_type=F32)


def dot_t(a, b):
    return lax.dot_general(a, b, (((1,), (1,)), ((), ())), preferred_element_type=F32)


def gelu_slope(pre):
    normal_cdf = 0.5 * (1.0 + lax.erf(pre * (1.0 / math.sqrt(2.0))))
    return normal_cdf + pre * jnp.exp(-0.5 * pre * pre) * (1.0 / math.sqrt(2.0 * math.pi))


def roll(v, amount):
    amount %= 128
    return v if amount == 0 else pltpu.roll(v, amount, 1)


def halves(low, high):
    lane = lax.broadcasted_iota(jnp.int32, low.shape, 1)
    return jnp.where(lane < 64, low, high)


def slot_masks(rows):
    slot = lax.broadcasted_iota(jnp.int32, (rows, 128), 1) // KH
    return [slot == m for m in range(16)]


def turn_slots(masks, get, put):
    rolled = [roll(get(j), KH * j) for j in range(16)]
    for e in range(16):
        out = rolled[(0 - e) % 16]
        for m in range(1, 16):
            out = jnp.where(masks[m], rolled[(m - e) % 16], out)
        put(e, roll(out, -KH * e))


def y_inverse(rb, c0, rows, ly):
    masks = slot_masks(rows)

    def put(e, tile):
        kh, ri, x = e // 8, (e // 4) % 2, e % 4
        at = (kh * 4 + x) * rows
        ly[at : at + rows, ri * 128 : (ri + 1) * 128] = tile.astype(BF16)

    turn_slots(masks, lambda j: rb[j, c0 : c0 + rows, :].astype(F32), put)


def kernel(
    field_hbm, cot_hbm, w_hbm, wl_hbm, t_hbm, tt_hbm, zf_hbm, zt_hbm,
    r3, sp_hbm, keep_hbm,
    f_ref, c_ref, w_ref, wl_ref, t_ref, tt_ref, zf_ref, zt_ref, big, slope, sp,
    a2, ly, vy, xo, xi, wb, bw, xf, vf, ukeep,
    s0, r0, s1, r1, s2, r2, s3,
    us, ur, vs, vr, gs, gr, ds_, dr,
    lsem, osem, ssem, rsem,
):
    me_d = lax.axis_index("dp")
    me_p = lax.axis_index("pencil")

    def load(src, dst, i):
        return pltpu.make_async_copy(src, dst, lsem.at[i])

    loads = [load(field_hbm.at[0, x], f_ref.at[x], x) for x in range(4)]
    loads += [
        load(zf_hbm, zf_ref, 4),
        load(t_hbm, t_ref, 5),
        load(w_hbm.at[0, 0], w_ref, 6),
        load(wl_hbm, wl_ref, 7),
        load(cot_hbm.at[0], c_ref, 8),
        load(tt_hbm, tt_ref, 9),
        load(zt_hbm, zt_ref, 10),
    ]
    for i in (4, 0, 1, 2, 3, 5, 6, 7, 9, 10, 8):
        loads[i].start()

    barrier = pltpu.get_barrier_semaphore()

    @pl.loop(1, 16)
    def _(d):
        pl.semaphore_signal(
            barrier, inc=1, device_id=(me_d, lax.rem(me_p + d, 16)), device_id_type=MESH
        )
        pl.semaphore_signal(
            barrier, inc=1, device_id=(lax.rem(me_d + d, 16), me_p), device_id_type=MESH
        )

    def send_pencil(e, sb, rb, h):
        @pl.loop(1, 16)
        def _(d):
            to = lax.rem(me_p + d, 16)
            pltpu.make_async_remote_copy(
                src_ref=sb.at[to, pl.ds(h * HC, HC)],
                dst_ref=rb.at[me_p, pl.ds(h * HC, HC)],
                send_sem=ssem.at[e],
                recv_sem=rsem.at[e],
                device_id=(me_d, to),
                device_id_type=MESH,
            ).start()

    def keep_pencil(sb, rb, h):
        rb[me_p, pl.ds(h * HC, HC)] = sb[me_p, pl.ds(h * HC, HC)]

    def send_dp(e, sb, rb):
        @pl.loop(1, 16)
        def _(d):
            to = lax.rem(me_d + d, 16)
            pltpu.make_async_remote_copy(
                src_ref=sb.at[to],
                dst_ref=rb.at[me_d],
                send_sem=ssem.at[e],
                recv_sem=rsem.at[e],
                device_id=(to, me_p),
                device_id_type=MESH,
            ).start()

        rb[me_d] = sb[me_d]

    def wait_pencil(sem, buf, h):
        part = buf.at[pl.ds(0, 15), pl.ds(h * HC, HC)]
        pltpu.make_async_copy(part, part, sem).wait()

    def wait_dp(sem, buf):
        part = buf.at[pl.ds(0, 15)]
        pltpu.make_async_copy(part, part, sem).wait()

    def z_store(a, x, g0, n):
        for i in range(n):
            for kh in range(2):
                row = pl.multiple_of((kh * 4 + x) * HC, HC)
                a2[pl.ds(row, HC), (g0 + i) * 128 : (g0 + i + 1) * 128] = a[
                    i * HC : (i + 1) * HC, kh * 128 : (kh + 1) * 128
                ]

    def y_forward(sb, h):
        y = dot(a2[...], t_ref[...])

        def get(e):
            kh, ri, x = e // 8, (e // 4) % 2, e % 4
            at = (kh * 4 + x) * HC
            return y[at : at + HC, ri * 128 : (ri + 1) * 128]

        def put(j, tile):
            sb[j, h * HC : (h + 1) * HC, :] = tile.astype(BF16)

        turn_slots(slot_masks(HC), get, put)

    def x_forward(rb, h):
        low, high = [], []
        for g in range(8):
            a = rb[2 * g, h * HC : (h + 1) * HC, :].astype(F32)
            b = roll(rb[2 * g + 1, h * HC : (h + 1) * HC, :].astype(F32), 64)
            low.append(halves(a, b).astype(BF16))
            high.append(roll(halves(b, a), 64).astype(BF16))
        lhs = jnp.concatenate(
            [jnp.concatenate(low, axis=1), jnp.concatenate(high, axis=1)], axis=0
        )
        o = dot(lhs, t_ref[...])
        for kh in range(2):
            xo[kh * CH + h * HC : kh * CH + (h + 1) * HC, :] = o[kh * HC : (kh + 1) * HC]

    def modes_out(dst, scaled):
        turned = xo[...].T
        if scaled:
            row = lax.broadcasted_iota(jnp.int32, (256, 128), 0)
            lane = lax.broadcasted_iota(jnp.int32, (256, 128), 1)
            zero = ((row % KH) == 0) & (lane < 64)
            turned = turned * jnp.where(zero, SCALE, 2.0 * SCALE)
        for j in range(16):
            dst[j] = jnp.concatenate(
                [turned[j * 8 : j * 8 + 8], turned[128 + j * 8 : 136 + j * 8]], axis=0
            ).astype(BF16)

    def modes_in(src):
        v = [src[j].astype(F32) for j in range(16)]
        both = jnp.concatenate([t[:8] for t in v] + [t[8:] for t in v], axis=0)
        xi[...] = both.T.astype(BF16)

    def x_inverse(sb, h):
        lhs = jnp.concatenate(
            [xi[kh * CH + h * HC : kh * CH + (h + 1) * HC, :] for kh in range(2)], axis=0
        )
        o = dot(lhs, tt_ref[...])
        for g in range(8):
            low = o[:HC, g * 128 : (g + 1) * 128]
            high = o[HC:, g * 128 : (g + 1) * 128]
            sb[2 * g, h * HC : (h + 1) * HC, :] = halves(low, roll(high, 64)).astype(BF16)
            sb[2 * g + 1, h * HC : (h + 1) * HC, :] = halves(roll(low, 64), high).astype(BF16)

    def mix(lhs, src, dst):
        @pl.loop(0, 4)
        def _(x):
            for g in range(8):
                rhs = jnp.concatenate(
                    [src[x, g, :4].reshape(256, 128), src[x, g, 4:].reshape(256, 128)], axis=1
                )
                o = dot(lhs, rhs).astype(dst.dtype)
                dst[x, g, :4] = o[:, :128].reshape(4, CH, 128)
                dst[x, g, 4:] = o[:, 128:].reshape(4, CH, 128)

    loads[4].wait()
    for h in range(CHUNKS):
        for x in range(4):
            if h == 0:
                loads[x].wait()
            lhs = jnp.concatenate(
                [
                    f_ref[x, :, p, h * HC : (h + 1) * HC, :].reshape(8 * HC, 128)
                    for p in range(8)
                ],
                axis=1,
            )
            z_store(dot(lhs, zf_ref[...]).astype(BF16), x, 0, 8)
        if h == 0:
            loads[5].wait()
        y_forward(s0, h)
        if h == 0:
            pl.semaphore_wait(barrier, 30)
        send_pencil(h, s0, r0, h)
        keep_pencil(s0, r0, h)

    loads[6].wait()
    loads[7].wait()
    lane64 = lax.broadcasted_iota(jnp.int32, (64, 128), 1)
    for k in range(MZ):
        w = w_ref[k].astype(F32)
        turned = roll(w, 64)
        turned = jnp.where(lane64 < 64, -turned, turned)
        wb[k] = jnp.concatenate([w, turned], axis=0).astype(BF16)
    wl = wl_ref[...].astype(F32)
    wide = jnp.concatenate([wl] * 4, axis=1)
    tall = jnp.concatenate([wide] * 4, axis=0)
    row = lax.broadcasted_iota(jnp.int32, (256, 256), 0) // 64
    col = lax.broadcasted_iota(jnp.int32, (256, 256), 1) // 64
    block = jnp.where(row == col, tall, 0.0)
    bw[0] = block.T.astype(BF16)
    bw[1] = block.astype(BF16)
    mix(bw[0], f_ref, big)

    for h in range(CHUNKS):
        wait_pencil(rsem.at[h], r0, h)
        x_forward(r0, h)
    modes_out(us, False)
    send_dp(2, us, ur)
    loads[9].wait()
    loads[10].wait()
    loads[8].wait()
    wait_dp(rsem.at[2], ur)

    def regroup(src, i):
        xf[...] = src[...].astype(F32).reshape(256, 128)
        for k in range(KH):
            re = xf[pl.ds(k, 16, stride=16), :]
            im = xf[pl.ds(KH + k, 16, stride=16), :]
            ukeep[i, k] = halves(re, roll(im, 64)).astype(BF16)
            ukeep[i, KH + k] = halves(roll(re, 64), im).astype(BF16)

    def products(mode, dst):
        for k in range(KH):
            low, high = mode(k), mode(KH + k)
            vf[pl.ds(k, 16, stride=16), :] = halves(low, roll(high, 64))
            vf[pl.ds(KH + k, 16, stride=16), :] = halves(roll(low, 64), high)
        dst[...] = vf[...].astype(BF16).reshape(16, 16, 128)

    regroup(ur, 0)
    products(lambda k: dot(ukeep[0, k], wb[k]) * (SCALE if k == 0 else 2.0 * SCALE), vs)
    send_dp(3, vs, vr)
    wait_dp(rsem.at[3], vr)

    modes_in(vr)
    for h in range(CHUNKS):
        x_inverse(s1, h)
        send_pencil(4 + h, s1, r1, h)
        keep_pencil(s1, r1, h)

    for h in range(CHUNKS):
        wait_pencil(rsem.at[4 + h], r1, h)
        y_inverse(r1, h * HC, HC, ly)
        vy[...] = dot(ly[...], tt_ref[...]).astype(BF16)

        @pl.loop(0, 4)
        def _(x, h=h):
            for g0 in (0, 4):
                parts = []
                for g in range(g0, g0 + 4):
                    rows = [pl.ds(pl.multiple_of((kh * 4 + x) * HC, HC), HC) for kh in range(2)]
                    parts.append(
                        jnp.concatenate([vy[r, g * 128 : (g + 1) * 128] for r in rows], axis=1)
                    )
                v = dot(jnp.concatenate(parts, axis=0), zt_ref[...])
                parts = []
                for p in range(8):
                    at = (x, slice(g0, g0 + 4), p, slice(h * HC, (h + 1) * HC))
                    pre = v[:, p * 128 : (p + 1) * 128].reshape(4, HC, 128) + big[at]
                    sl = (c_ref[at].astype(F32) * gelu_slope(pre)).astype(BF16)
                    slope[at] = sl
                    parts.append(sl.reshape(4 * HC, 128))
                z_store(dot(jnp.concatenate(parts, axis=1), zf_ref[...]).astype(BF16), x, g0, 4)

        y_forward(s2, h)
        send_pencil(6 + h, s2, r2, h)
        keep_pencil(s2, r2, h)

    mix(bw[1], slope, sp)
    sp_copy = pltpu.make_async_copy(sp, sp_hbm, osem.at[0])
    sp_copy.start()

    for h in range(CHUNKS):
        wait_pencil(rsem.at[6 + h], r2, h)
        x_forward(r2, h)
    modes_out(gs, True)
    send_dp(8, gs, gr)
    wait_dp(rsem.at[8], gr)

    regroup(gr, 1)
    products(lambda k: dot_t(ukeep[1, k], wb[k]), ds_)
    send_dp(9, ds_, dr)
    keep_copy = pltpu.make_async_copy(ukeep, keep_hbm, osem.at[1])
    keep_copy.start()
    wait_dp(rsem.at[9], dr)

    modes_in(dr)
    own = []
    for h in range(CHUNKS):
        x_inverse(s3, h)
        send_pencil(10 + h, s3, r3, h)
        part = pl.ds(h * HC, HC)
        own.append(pltpu.make_async_copy(s3.at[me_p, part], r3.at[me_p, part], osem.at[2 + h]))
        own[h].start()

    for h in range(CHUNKS):
        wait_pencil(ssem.at[h], s0, h)
        wait_pencil(ssem.at[4 + h], s1, h)
        wait_pencil(ssem.at[6 + h], s2, h)
    wait_dp(ssem.at[2], us)
    wait_dp(ssem.at[3], vs)
    wait_dp(ssem.at[8], gs)
    wait_dp(ssem.at[9], ds_)
    sp_copy.wait()
    keep_copy.wait()
    for h in range(CHUNKS):
        own[h].wait()
        wait_pencil(ssem.at[10 + h], s3, h)
        wait_pencil(rsem.at[10 + h], r3, h)


def last_kernel(
    r_hbm, sp_hbm, keep_hbm, tt_hbm, zt_hbm, out_hbm, gw_hbm,
    r_ref, sp, keep, tt_ref, zt_ref, ly, vy, out_v, gw_v, lsem, osem,
):
    loads = [
        pltpu.make_async_copy(r_hbm, r_ref, lsem.at[0]),
        pltpu.make_async_copy(tt_hbm, tt_ref, lsem.at[1]),
        pltpu.make_async_copy(zt_hbm, zt_ref, lsem.at[2]),
        pltpu.make_async_copy(keep_hbm, keep, lsem.at[3]),
    ]
    loads += [pltpu.make_async_copy(sp_hbm.at[x], sp.at[x], lsem.at[4 + x]) for x in range(4)]
    for copy in loads:
        copy.start()
    loads[0].wait()
    y_inverse(r_ref, 0, CH, ly)
    loads[1].wait()
    vy[...] = dot(ly[...], tt_ref[...]).astype(BF16)
    loads[2].wait()
    outs = []
    for x in range(4):
        loads[4 + x].wait()
        for g in range(8):
            lhs = jnp.concatenate(
                [
                    vy[(kh * 4 + x) * CH : (kh * 4 + x + 1) * CH, g * 128 : (g + 1) * 128]
                    for kh in range(2)
                ],
                axis=1,
            )
            v = dot(lhs, zt_ref[...])
            for p in range(8):
                out_v[x, g, p] = (v[:, p * 128 : (p + 1) * 128] + sp[x, g, p].astype(F32)).astype(BF16)
        outs.append(pltpu.make_async_copy(out_v.at[x], out_hbm.at[0, x], osem.at[x]))
        outs[x].start()

    loads[3].wait()
    lane = lax.broadcasted_iota(jnp.int32, (64, 128), 1)
    for k in range(MZ):
        cross = lax.dot_general(
            keep[0, k], keep[1, k], (((0,), (0,)), ((), ())), preferred_element_type=F32
        )
        low = roll(cross[64:], 64)
        gw_v[k] = cross[:64] + jnp.where(lane < 64, low, -low)
    outs.append(pltpu.make_async_copy(gw_v, gw_hbm.at[0, 0], osem.at[4]))
    outs[4].start()
    for copy in outs:
        copy.wait()


def body(field, cotangent, w_spec, w_local):
    table, zf = line_table(), z_table()
    t, tt, zf, zt = (jnp.asarray(m.astype(jnp.bfloat16)) for m in (table, table.T, zf, zf.T))
    grid = (4, 8, 8, CH, NZ)
    any_spec = pl.BlockSpec(memory_space=pl.ANY)
    pencil_buf = pltpu.VMEM((16, CH, 128), BF16)
    dp_buf = pltpu.VMEM((16, 16, 128), BF16)
    grid_b16 = pltpu.VMEM(grid, BF16)
    line = pltpu.VMEM((1024, 256), BF16)
    line_t = pltpu.VMEM((256, 1024), BF16)
    keep = pltpu.VMEM((2, MZ, 16, 128), BF16)
    r3, sp, kept = pl.pallas_call(
        kernel,
        out_shape=(
            jax.ShapeDtypeStruct((16, CH, 128), BF16),
            jax.ShapeDtypeStruct(grid, BF16),
            jax.ShapeDtypeStruct((2, MZ, 16, 128), BF16),
        ),
        in_specs=[any_spec] * 8,
        out_specs=[any_spec] * 3,
        scratch_shapes=[
            grid_b16,
            grid_b16,
            pltpu.VMEM((MZ, CH, 2 * CH), BF16),
            pltpu.VMEM((CH, CH), BF16),
            line,
            line_t,
            line,
            line_t,
            pltpu.VMEM(grid, F32),
            grid_b16,
            grid_b16,
            pltpu.VMEM((8 * HC, 1024), BF16),
            pltpu.VMEM((8 * HC, 256), BF16),
            pltpu.VMEM((8 * HC, 1024), BF16),
            pltpu.VMEM((128, 256), F32),
            pltpu.VMEM((128, 256), BF16),
            pltpu.VMEM((MZ, 128, 128), BF16),
            pltpu.VMEM((2, 256, 256), BF16),
            pltpu.VMEM((256, 128), F32),
            pltpu.VMEM((256, 128), F32),
            keep,
        ]
        + [pencil_buf] * 7
        + [dp_buf] * 8
        + [
            pltpu.SemaphoreType.DMA((11,)),
            pltpu.SemaphoreType.DMA((4,)),
            pltpu.SemaphoreType.DMA((12,)),
            pltpu.SemaphoreType.DMA((12,)),
        ],
        compiler_params=pltpu.CompilerParams(
            collective_id=0, has_side_effects=True, vmem_limit_bytes=60 * 1024 * 1024
        ),
        name="layer",
    )(field.reshape((1,) + grid), cotangent.reshape((1,) + grid), w_spec, w_local, t, tt, zf, zt)
    out, gw = pl.pallas_call(
        last_kernel,
        out_shape=(
            jax.ShapeDtypeStruct((1,) + grid, BF16),
            jax.ShapeDtypeStruct((1, 1, MZ, CH, 2 * CH), F32),
        ),
        in_specs=[any_spec] * 5,
        out_specs=[any_spec] * 2,
        scratch_shapes=[
            pencil_buf,
            grid_b16,
            keep,
            line_t,
            line_t,
            pltpu.VMEM((8 * CH, 256), BF16),
            pltpu.VMEM((8 * CH, 1024), BF16),
            grid_b16,
            pltpu.VMEM((MZ, CH, 2 * CH), F32),
            pltpu.SemaphoreType.DMA((8,)),
            pltpu.SemaphoreType.DMA((5,)),
        ],
        compiler_params=pltpu.CompilerParams(vmem_limit_bytes=60 * 1024 * 1024),
        name="last",
    )(r3, sp, kept, tt, zt)
    return (out.reshape(1, 4, NY, CH, NZ), gw)


def solution(mesh):
    placed = P("dp", "pencil", None, None, None)
    return jax.shard_map(
        body,
        mesh=mesh,
        in_specs=(placed, placed, placed, P()),
        out_specs=(placed, placed),
        check_vma=False,
    )
```

```python
import functools
import math

import jax
import jax.numpy as jnp
import numpy as np
from jax import lax
from jax.experimental import pallas as pl
from jax.experimental.pallas import tpu as pltpu
from jax.sharding import PartitionSpec as P

NX = 64
NY = 64
NZ = 128
CH = 64
MX = 16
MY = 16
MZ = 16
KH = 8
MESH = pl.DeviceIdType.MESH
F32 = jnp.float32
BF16 = jnp.bfloat16
CHUNKS = 2
HC = CH // CHUNKS
SCALE = 1.0 / (NX * NY * NZ)


def line_table():
    position = np.arange(NX)
    freq = np.arange(MX)
    freq = np.where(freq < MX // 2, freq, freq - MX)
    angle = 2.0 * math.pi * np.mod(position[:, None] * freq[None, :], NX) / NX
    cos, sin = np.cos(angle).reshape(8, 2, 4, MX), np.sin(angle).reshape(8, 2, 4, MX)
    table = np.zeros((8, 2, 2, 4, KH, 2, MX, KH), np.float32)
    for k in range(KH):
        table[:, :, 0, :, k, 0, :, k] = cos
        table[:, :, 1, :, k, 0, :, k] = sin
        table[:, :, 1, :, k, 1, :, k] = cos
        table[:, :, 0, :, k, 1, :, k] = -sin
    return table.reshape(1024, 256)


def z_table():
    angle = 2.0 * math.pi * np.mod(np.arange(NZ)[:, None] * np.arange(MZ)[None, :], NZ) / NZ
    angle = angle.reshape(NZ, 2, KH)
    table = np.zeros((2, 4, NZ, 2, 2, 2, 4, KH), np.float32)
    for half in range(2):
        for q in range(4):
            table[half, q, :, :, half, 0, q, :] = np.cos(angle)
            table[half, q, :, :, half, 1, q, :] = -np.sin(angle)
    return table.reshape(1024, 256)


def dot(a, b):
    return jnp.dot(a, b, preferred_element_type=F32)


def dot_t(a, b):
    return lax.dot_general(a, b, (((1,), (1,)), ((), ())), preferred_element_type=F32)


def gelu_slope(t):
    bell = jnp.exp2(t * t * (-1.0 / math.log(2.0)) - 0.5 * math.log2(math.pi))
    return 0.5 * lax.erf(t) + (t * bell + 0.5)


def roll(v, amount):
    amount %= 128
    return v if amount == 0 else pltpu.roll(v, amount, 1)


def halves(low, high):
    lane = lax.broadcasted_iota(jnp.int32, low.shape, 1)
    return jnp.where(lane < 64, low, high)


def slot_masks(rows):
    slot = lax.broadcasted_iota(jnp.int32, (rows, 128), 1) // KH
    return [slot == m for m in range(16)]


def turn_slots(masks, get, put):
    rolled = [roll(get(j), KH * j) for j in range(16)]
    for e in range(16):
        out = rolled[(0 - e) % 16]
        for m in range(1, 16):
            out = jnp.where(masks[m], rolled[(m - e) % 16], out)
        put(e, roll(out, -KH * e))


def y_inverse(rb, c0, rows, ly):
    masks = slot_masks(rows)

    def put(e, tile):
        kh, ri, x = e // 8, (e // 4) % 2, e % 4
        at = (kh * 4 + x) * rows
        ly[at : at + rows, ri * 128 : (ri + 1) * 128] = tile.astype(BF16)

    turn_slots(masks, lambda j: rb[j, c0 : c0 + rows, :].astype(F32), put)


def kernel(
    field_hbm, cot_hbm, w_hbm, wl_hbm, t_hbm, tt_hbm, zf_hbm, zt_hbm,
    r3, sp_hbm, gw_hbm,
    f_ref, c_ref, w_ref, wl_ref, t_ref, tt_ref, zf_ref, zt_ref, big, slope, sp, gw_v,
    a2, ly, vy, xo, xi, wb, bw, xf, vf, ukeep,
    s0, r0, s1, r1, s2, r2, s3,
    us, ur, vs, vr, gs, gr, ds_, dr,
    lsem, osem, ssem, rsem,
):
    me_d = lax.axis_index("dp")
    me_p = lax.axis_index("pencil")

    def load(src, dst, i):
        return pltpu.make_async_copy(src, dst, lsem.at[i])

    loads = [load(field_hbm.at[0, x], f_ref.at[x], x) for x in range(4)]
    loads += [
        load(zf_hbm, zf_ref, 4),
        load(t_hbm, t_ref, 5),
        load(w_hbm.at[0, 0], w_ref, 6),
        load(wl_hbm, wl_ref, 7),
        load(cot_hbm.at[0], c_ref, 8),
        load(tt_hbm, tt_ref, 9),
        load(zt_hbm, zt_ref, 10),
    ]
    for i in (4, 0, 1, 2, 3, 5, 6, 7, 9, 10, 8):
        loads[i].start()

    barrier = pltpu.get_barrier_semaphore()

    @pl.loop(1, 16)
    def _(d):
        pl.semaphore_signal(
            barrier, inc=1, device_id=(me_d, lax.rem(me_p + d, 16)), device_id_type=MESH
        )
        pl.semaphore_signal(
            barrier, inc=1, device_id=(lax.rem(me_d + d, 16), me_p), device_id_type=MESH
        )

    def send_pencil(e, sb, rb, h):
        @pl.loop(1, 16)
        def _(d):
            to = lax.rem(me_p + d, 16)
            pltpu.make_async_remote_copy(
                src_ref=sb.at[to, pl.ds(h * HC, HC)],
                dst_ref=rb.at[me_p, pl.ds(h * HC, HC)],
                send_sem=ssem.at[e],
                recv_sem=rsem.at[e],
                device_id=(me_d, to),
                device_id_type=MESH,
            ).start()

    def keep_pencil(sb, rb, h):
        rb[me_p, pl.ds(h * HC, HC)] = sb[me_p, pl.ds(h * HC, HC)]

    def send_dp(e, sb, rb):
        @pl.loop(1, 16)
        def _(d):
            to = lax.rem(me_d + d, 16)
            pltpu.make_async_remote_copy(
                src_ref=sb.at[to],
                dst_ref=rb.at[me_d],
                send_sem=ssem.at[e],
                recv_sem=rsem.at[e],
                device_id=(to, me_p),
                device_id_type=MESH,
            ).start()

        rb[me_d] = sb[me_d]

    def wait_pencil(sem, buf, h):
        part = buf.at[pl.ds(0, 15), pl.ds(h * HC, HC)]
        pltpu.make_async_copy(part, part, sem).wait()

    def wait_dp(sem, buf):
        part = buf.at[pl.ds(0, 15)]
        pltpu.make_async_copy(part, part, sem).wait()

    def z_store(a, x, g0, n):
        for i in range(n):
            for kh in range(2):
                row = pl.multiple_of((kh * 4 + x) * HC, HC)
                a2[pl.ds(row, HC), (g0 + i) * 128 : (g0 + i + 1) * 128] = a[
                    i * HC : (i + 1) * HC, kh * 128 : (kh + 1) * 128
                ]

    def y_forward(sb, h):
        y = dot(a2[...], t_ref[...])

        def get(e):
            kh, ri, x = e // 8, (e // 4) % 2, e % 4
            at = (kh * 4 + x) * HC
            return y[at : at + HC, ri * 128 : (ri + 1) * 128]

        def put(j, tile):
            sb[j, h * HC : (h + 1) * HC, :] = tile.astype(BF16)

        turn_slots(slot_masks(HC), get, put)

    def x_forward(rb, h):
        low, high = [], []
        for g in range(8):
            a = rb[2 * g, h * HC : (h + 1) * HC, :].astype(F32)
            b = roll(rb[2 * g + 1, h * HC : (h + 1) * HC, :].astype(F32), 64)
            low.append(halves(a, b).astype(BF16))
            high.append(roll(halves(b, a), 64).astype(BF16))
        lhs = jnp.concatenate(
            [jnp.concatenate(low, axis=1), jnp.concatenate(high, axis=1)], axis=0
        )
        o = dot(lhs, t_ref[...])
        for kh in range(2):
            xo[kh * CH + h * HC : kh * CH + (h + 1) * HC, :] = o[kh * HC : (kh + 1) * HC]

    def modes_out(dst, scaled):
        turned = xo[...].T
        if scaled:
            row = lax.broadcasted_iota(jnp.int32, (256, 128), 0)
            lane = lax.broadcasted_iota(jnp.int32, (256, 128), 1)
            zero = ((row % KH) == 0) & (lane < 64)
            turned = turned * jnp.where(zero, SCALE, 2.0 * SCALE)
        for j in range(16):
            dst[j] = jnp.concatenate(
                [turned[j * 8 : j * 8 + 8], turned[128 + j * 8 : 136 + j * 8]], axis=0
            ).astype(BF16)

    def modes_in(src):
        v = [src[j].astype(F32) for j in range(16)]
        both = jnp.concatenate([t[:8] for t in v] + [t[8:] for t in v], axis=0)
        xi[...] = both.T.astype(BF16)

    def x_inverse(sb, h):
        lhs = jnp.concatenate(
            [xi[kh * CH + h * HC : kh * CH + (h + 1) * HC, :] for kh in range(2)], axis=0
        )
        o = dot(lhs, tt_ref[...])
        for g in range(8):
            low = o[:HC, g * 128 : (g + 1) * 128]
            high = o[HC:, g * 128 : (g + 1) * 128]
            sb[2 * g, h * HC : (h + 1) * HC, :] = halves(low, roll(high, 64)).astype(BF16)
            sb[2 * g + 1, h * HC : (h + 1) * HC, :] = halves(roll(low, 64), high).astype(BF16)

    def mix(lhs, src, dst, scale):
        @pl.loop(0, 4)
        def _(x):
            for g in range(8):
                rhs = jnp.concatenate(
                    [src[x, g, :4].reshape(256, 128), src[x, g, 4:].reshape(256, 128)], axis=1
                )
                o = dot(lhs, rhs)
                o = (o if scale is None else o * scale).astype(dst.dtype)
                dst[x, g, :4] = o[:, :128].reshape(4, CH, 128)
                dst[x, g, 4:] = o[:, 128:].reshape(4, CH, 128)

    loads[4].wait()
    for h in range(CHUNKS):
        for x in range(4):
            if h == 0:
                loads[x].wait()
            lhs = jnp.concatenate(
                [
                    f_ref[x, :, p, h * HC : (h + 1) * HC, :].reshape(8 * HC, 128)
                    for p in range(8)
                ],
                axis=1,
            )
            z_store(dot(lhs, zf_ref[...]).astype(BF16), x, 0, 8)
        if h == 0:
            loads[5].wait()
        y_forward(s0, h)
        if h == 0:
            pl.semaphore_wait(barrier, 30)
        send_pencil(h, s0, r0, h)
        keep_pencil(s0, r0, h)

    loads[6].wait()
    loads[7].wait()
    lane64 = lax.broadcasted_iota(jnp.int32, (64, 128), 1)
    for k in range(MZ):
        w = w_ref[k].astype(F32)
        turned = roll(w, 64)
        turned = jnp.where(lane64 < 64, -turned, turned)
        wb[k] = jnp.concatenate([w, turned], axis=0).astype(BF16)
    wl = wl_ref[...].astype(F32)
    wide = jnp.concatenate([wl] * 4, axis=1)
    tall = jnp.concatenate([wide] * 4, axis=0)
    row = lax.broadcasted_iota(jnp.int32, (256, 256), 0) // 64
    col = lax.broadcasted_iota(jnp.int32, (256, 256), 1) // 64
    block = jnp.where(row == col, tall, 0.0)
    bw[0] = block.T.astype(BF16)
    bw[1] = block.astype(BF16)
    mix(bw[0], f_ref, big, math.sqrt(0.5))

    for h in range(CHUNKS):
        wait_pencil(rsem.at[h], r0, h)
        x_forward(r0, h)
    modes_out(us, False)
    send_dp(2, us, ur)
    loads[9].wait()
    loads[10].wait()
    loads[8].wait()
    wait_dp(rsem.at[2], ur)

    def regroup(src, i):
        xf[...] = src[...].astype(F32).reshape(256, 128)
        for k in range(KH):
            re = xf[pl.ds(k, 16, stride=16), :]
            im = xf[pl.ds(KH + k, 16, stride=16), :]
            ukeep[i, k] = halves(re, roll(im, 64)).astype(BF16)
            ukeep[i, KH + k] = halves(roll(re, 64), im).astype(BF16)

    def products(mode, dst):
        for k in range(KH):
            low, high = mode(k), mode(KH + k)
            vf[pl.ds(k, 16, stride=16), :] = halves(low, roll(high, 64))
            vf[pl.ds(KH + k, 16, stride=16), :] = halves(roll(low, 64), high)
        dst[...] = vf[...].astype(BF16).reshape(16, 16, 128)

    regroup(ur, 0)
    root = math.sqrt(0.5)
    products(lambda k: dot(ukeep[0, k], wb[k]) * (root * SCALE if k == 0 else 2.0 * root * SCALE), vs)
    send_dp(3, vs, vr)
    wait_dp(rsem.at[3], vr)

    modes_in(vr)
    for h in range(CHUNKS):
        x_inverse(s1, h)
        send_pencil(4 + h, s1, r1, h)
        keep_pencil(s1, r1, h)

    for h in range(CHUNKS):
        wait_pencil(rsem.at[4 + h], r1, h)
        y_inverse(r1, h * HC, HC, ly)
        vy[...] = dot(ly[...], tt_ref[...]).astype(BF16)

        @pl.loop(0, 2)
        def _(x2, h=h):
            for xi_ in range(2):
                x = 2 * x2 + xi_
                rows = [pl.ds(pl.multiple_of((kh * 4 + x) * HC, HC), HC) for kh in range(2)]
                lhs = jnp.concatenate(
                    [
                        jnp.concatenate([vy[r, g * 128 : (g + 1) * 128] for r in rows], axis=1)
                        for g in range(8)
                    ],
                    axis=0,
                )
                parts = []
                for n in range(4):
                    v = dot(lhs, zt_ref[:, n * 256 : (n + 1) * 256])
                    for i in range(2):
                        at = (x, slice(None), 2 * n + i, slice(h * HC, (h + 1) * HC))
                        pre = v[:, i * 128 : (i + 1) * 128].reshape(8, HC, 128) + big[at]
                        sl = (c_ref[at].astype(F32) * gelu_slope(pre)).astype(BF16)
                        slope[at] = sl
                        parts.append(sl.reshape(8 * HC, 128))
                z_store(dot(jnp.concatenate(parts, axis=1), zf_ref[...]).astype(BF16), x, 0, 8)

        y_forward(s2, h)
        send_pencil(6 + h, s2, r2, h)
        keep_pencil(s2, r2, h)

    mix(bw[1], slope, sp, None)
    sp_copy = pltpu.make_async_copy(sp, sp_hbm, osem.at[0])
    sp_copy.start()

    for h in range(CHUNKS):
        wait_pencil(rsem.at[6 + h], r2, h)
        x_forward(r2, h)
    modes_out(gs, True)
    send_dp(8, gs, gr)
    wait_dp(rsem.at[8], gr)

    regroup(gr, 1)
    products(lambda k: dot_t(ukeep[1, k], wb[k]), ds_)
    send_dp(9, ds_, dr)
    wait_dp(rsem.at[9], dr)

    modes_in(dr)
    own = []
    for h in range(CHUNKS):
        x_inverse(s3, h)
        send_pencil(10 + h, s3, r3, h)
        part = pl.ds(h * HC, HC)
        own.append(pltpu.make_async_copy(s3.at[me_p, part], r3.at[me_p, part], osem.at[2 + h]))
        own[h].start()

    for k in range(MZ):
        cross = lax.dot_general(
            ukeep[0, k], ukeep[1, k], (((0,), (0,)), ((), ())), preferred_element_type=F32
        )
        low = roll(cross[64:], 64)
        gw_v[k] = cross[:64] + jnp.where(lane64 < 64, low, -low)
    gw_copy = pltpu.make_async_copy(gw_v, gw_hbm, osem.at[1])
    gw_copy.start()

    for h in range(CHUNKS):
        wait_pencil(ssem.at[h], s0, h)
        wait_pencil(ssem.at[4 + h], s1, h)
        wait_pencil(ssem.at[6 + h], s2, h)
    wait_dp(ssem.at[2], us)
    wait_dp(ssem.at[3], vs)
    wait_dp(ssem.at[8], gs)
    wait_dp(ssem.at[9], ds_)
    sp_copy.wait()
    gw_copy.wait()
    for h in range(CHUNKS):
        own[h].wait()
        wait_pencil(ssem.at[10 + h], s3, h)
        wait_pencil(rsem.at[10 + h], r3, h)


def last_kernel(
    r_hbm, sp_hbm, gw_in, tt_hbm, zt_hbm, out_hbm, gw_hbm,
    r_ref, sp, tt_ref, zt_ref, ly, vy, out_v, gw_v, lsem, osem,
):
    loads = [
        pltpu.make_async_copy(r_hbm, r_ref, lsem.at[0]),
        pltpu.make_async_copy(tt_hbm, tt_ref, lsem.at[1]),
        pltpu.make_async_copy(zt_hbm, zt_ref, lsem.at[2]),
        pltpu.make_async_copy(gw_in, gw_v, lsem.at[3]),
    ]
    loads += [pltpu.make_async_copy(sp_hbm.at[x], sp.at[x], lsem.at[4 + x]) for x in range(4)]
    for copy in loads:
        copy.start()
    loads[0].wait()
    y_inverse(r_ref, 0, CH, ly)
    loads[1].wait()
    vy[...] = dot(ly[...], tt_ref[...]).astype(BF16)
    loads[2].wait()
    outs = []
    for x in range(4):
        loads[4 + x].wait()
        lhs = jnp.concatenate(
            [
                jnp.concatenate(
                    [
                        vy[(kh * 4 + x) * CH : (kh * 4 + x + 1) * CH, g * 128 : (g + 1) * 128]
                        for kh in range(2)
                    ],
                    axis=1,
                )
                for g in range(8)
            ],
            axis=0,
        )
        for n in range(4):
            v = dot(lhs, zt_ref[:, n * 256 : (n + 1) * 256])
            for i in range(2):
                part = v[:, i * 128 : (i + 1) * 128].reshape(8, CH, 128)
                out_v[x, :, 2 * n + i] = (part + sp[x, :, 2 * n + i].astype(F32)).astype(BF16)
        outs.append(pltpu.make_async_copy(out_v.at[x], out_hbm.at[0, x], osem.at[x]))
        outs[x].start()
        if x == 0:
            loads[3].wait()
            outs_gw = pltpu.make_async_copy(gw_v, gw_hbm.at[0, 0], osem.at[4])
            outs_gw.start()
    for copy in outs:
        copy.wait()
    outs_gw.wait()


def body(field, cotangent, w_spec, w_local):
    table, zf = line_table(), z_table()
    t, tt, zf, zt = (jnp.asarray(m.astype(jnp.bfloat16)) for m in (table, table.T, zf, zf.T))
    grid = (4, 8, 8, CH, NZ)
    any_spec = pl.BlockSpec(memory_space=pl.ANY)
    pencil_buf = pltpu.VMEM((16, CH, 128), BF16)
    dp_buf = pltpu.VMEM((16, 16, 128), BF16)
    grid_b16 = pltpu.VMEM(grid, BF16)
    line = pltpu.VMEM((1024, 256), BF16)
    line_t = pltpu.VMEM((256, 1024), BF16)
    keep = pltpu.VMEM((2, MZ, 16, 128), BF16)
    r3, sp, gw = pl.pallas_call(
        kernel,
        out_shape=(
            jax.ShapeDtypeStruct((16, CH, 128), BF16),
            jax.ShapeDtypeStruct(grid, BF16),
            jax.ShapeDtypeStruct((MZ, CH, 2 * CH), F32),
        ),
        in_specs=[any_spec] * 8,
        out_specs=[any_spec] * 3,
        scratch_shapes=[
            grid_b16,
            grid_b16,
            pltpu.VMEM((MZ, CH, 2 * CH), BF16),
            pltpu.VMEM((CH, CH), BF16),
            line,
            line_t,
            line,
            line_t,
            pltpu.VMEM(grid, F32),
            grid_b16,
            grid_b16,
            pltpu.VMEM((MZ, CH, 2 * CH), F32),
            pltpu.VMEM((8 * HC, 1024), BF16),
            pltpu.VMEM((8 * HC, 256), BF16),
            pltpu.VMEM((8 * HC, 1024), BF16),
            pltpu.VMEM((128, 256), F32),
            pltpu.VMEM((128, 256), BF16),
            pltpu.VMEM((MZ, 128, 128), BF16),
            pltpu.VMEM((2, 256, 256), BF16),
            pltpu.VMEM((256, 128), F32),
            pltpu.VMEM((256, 128), F32),
            keep,
        ]
        + [pencil_buf] * 7
        + [dp_buf] * 8
        + [
            pltpu.SemaphoreType.DMA((11,)),
            pltpu.SemaphoreType.DMA((4,)),
            pltpu.SemaphoreType.DMA((12,)),
            pltpu.SemaphoreType.DMA((12,)),
        ],
        compiler_params=pltpu.CompilerParams(
            collective_id=0, has_side_effects=True, vmem_limit_bytes=60 * 1024 * 1024
        ),
        name="layer",
    )(field.reshape((1,) + grid), cotangent.reshape((1,) + grid), w_spec, w_local, t, tt, zf, zt)
    out, gw = pl.pallas_call(
        last_kernel,
        out_shape=(
            jax.ShapeDtypeStruct((1,) + grid, BF16),
            jax.ShapeDtypeStruct((1, 1, MZ, CH, 2 * CH), F32),
        ),
        in_specs=[any_spec] * 5,
        out_specs=[any_spec] * 2,
        scratch_shapes=[
            pencil_buf,
            grid_b16,
            line_t,
            line_t,
            pltpu.VMEM((8 * CH, 256), BF16),
            pltpu.VMEM((8 * CH, 1024), BF16),
            grid_b16,
            pltpu.VMEM((MZ, CH, 2 * CH), F32),
            pltpu.SemaphoreType.DMA((8,)),
            pltpu.SemaphoreType.DMA((5,)),
        ],
        compiler_params=pltpu.CompilerParams(vmem_limit_bytes=60 * 1024 * 1024),
        name="last",
    )(r3, sp, gw, tt, zt)
    return (out.reshape(1, 4, NY, CH, NZ), gw)


def solution(mesh):
    placed = P("dp", "pencil", None, None, None)
    return jax.shard_map(
        body,
        mesh=mesh,
        in_specs=(placed, placed, placed, P()),
        out_specs=(placed, placed),
        check_vma=False,
    )
```

```python
import functools
import math

import jax
import jax.numpy as jnp
import numpy as np
from jax import lax
from jax.experimental import pallas as pl
from jax.experimental.pallas import tpu as pltpu
from jax.sharding import PartitionSpec as P

NX = 64
NY = 64
NZ = 128
CH = 64
MX = 16
MY = 16
MZ = 16
KH = 8
MESH = pl.DeviceIdType.MESH
F32 = jnp.float32
BF16 = jnp.bfloat16
CHUNKS = 2
HC = CH // CHUNKS
SCALE = 1.0 / (NX * NY * NZ)


def line_table():
    position = np.arange(NX)
    freq = np.arange(MX)
    freq = np.where(freq < MX // 2, freq, freq - MX)
    angle = 2.0 * math.pi * np.mod(position[:, None] * freq[None, :], NX) / NX
    cos, sin = np.cos(angle).reshape(8, 2, 4, MX), np.sin(angle).reshape(8, 2, 4, MX)
    table = np.zeros((8, 2, 2, 4, KH, 2, MX, KH), np.float32)
    for k in range(KH):
        table[:, :, 0, :, k, 0, :, k] = cos
        table[:, :, 1, :, k, 0, :, k] = sin
        table[:, :, 1, :, k, 1, :, k] = cos
        table[:, :, 0, :, k, 1, :, k] = -sin
    return table.reshape(1024, 256)


def z_table():
    angle = 2.0 * math.pi * np.mod(np.arange(NZ)[:, None] * np.arange(MZ)[None, :], NZ) / NZ
    angle = angle.reshape(NZ, 2, KH)
    table = np.zeros((2, 4, NZ, 2, 2, 2, 4, KH), np.float32)
    for half in range(2):
        for q in range(4):
            table[half, q, :, :, half, 0, q, :] = np.cos(angle)
            table[half, q, :, :, half, 1, q, :] = -np.sin(angle)
    return table.reshape(1024, 256)


def dot(a, b):
    return jnp.dot(a, b, preferred_element_type=F32)


def dot_t(a, b):
    return lax.dot_general(a, b, (((1,), (1,)), ((), ())), preferred_element_type=F32)


def gelu_slope(t):
    bell = jnp.exp2(t * t * (-1.0 / math.log(2.0)) - 0.5 * math.log2(math.pi))
    return 0.5 * lax.erf(t) + (t * bell + 0.5)


def roll(v, amount):
    amount %= 128
    return v if amount == 0 else pltpu.roll(v, amount, 1)


def halves(low, high):
    lane = lax.broadcasted_iota(jnp.int32, low.shape, 1)
    return jnp.where(lane < 64, low, high)


def slot_masks(rows):
    slot = lax.broadcasted_iota(jnp.int32, (rows, 128), 1) // KH
    return [slot == m for m in range(16)]


def turn_slots(masks, get, put):
    rolled = [roll(get(j), KH * j) for j in range(16)]
    for e in range(16):
        out = rolled[(0 - e) % 16]
        for m in range(1, 16):
            out = jnp.where(masks[m], rolled[(m - e) % 16], out)
        put(e, roll(out, -KH * e))


def y_inverse(rb, c0, rows, ly):
    masks = slot_masks(rows)

    def put(e, tile):
        kh, ri, x = e // 8, (e // 4) % 2, e % 4
        at = (kh * 4 + x) * rows
        ly[at : at + rows, ri * 128 : (ri + 1) * 128] = tile.astype(BF16)

    turn_slots(masks, lambda j: rb[j, c0 : c0 + rows, :].astype(F32), put)


def kernel(
    field_hbm, cot_hbm, w_hbm, wl_hbm, t_hbm, tt_hbm, zf_hbm, zt_hbm,
    r3, sp_hbm, gw_hbm,
    f_ref, c_ref, wall, wl_ref, t_ref, tt_ref, zf_ref, zt_ref, big, slope, sp, gw_v,
    a2, ly, vy, xo, xi, bw, xf, ukeep,
    s0, r0, s1, r1, s2, r2, s3,
    us, ur, gs, gr, row_u, row_v, back_v, row_g, row_d, back_d,
    lsem, osem, ssem, rsem, wssem, wrsem, yssem, yrsem,
):
    me_d = lax.axis_index("dp")
    me_p = lax.axis_index("pencil")
    me_x, me_y, me_c = me_d // 4, lax.rem(me_d // 2, 2), lax.rem(me_d, 2)
    x_up, x_down, x_far = lax.rem(me_x + 1, 4), lax.rem(me_x + 3, 4), lax.rem(me_x + 2, 4)
    partner = me_d + 2 - 4 * me_y

    def load(src, dst, i):
        return pltpu.make_async_copy(src, dst, lsem.at[i])

    loads = [load(field_hbm.at[0, x], f_ref.at[x], x) for x in range(4)]
    loads += [
        load(zf_hbm, zf_ref, 4),
        load(t_hbm, t_ref, 5),
        load(w_hbm.at[0, 0], wall.at[2 * me_x + me_c], 6),
        load(wl_hbm, wl_ref, 7),
        load(cot_hbm.at[0], c_ref, 8),
        load(tt_hbm, tt_ref, 9),
        load(zt_hbm, zt_ref, 10),
    ]
    for i in (4, 0, 1, 2, 3, 5, 6, 7, 9, 10, 8):
        loads[i].start()

    barrier = pltpu.get_barrier_semaphore()

    @pl.loop(1, 16)
    def _(d):
        pl.semaphore_signal(
            barrier, inc=1, device_id=(me_d, lax.rem(me_p + d, 16)), device_id_type=MESH
        )
        pl.semaphore_signal(
            barrier, inc=1, device_id=(lax.rem(me_d + d, 16), me_p), device_id_type=MESH
        )

    def send_pencil(e, sb, rb, h):
        @pl.loop(1, 16)
        def _(d):
            to = lax.rem(me_p + d, 16)
            pltpu.make_async_remote_copy(
                src_ref=sb.at[to, pl.ds(h * HC, HC)],
                dst_ref=rb.at[me_p, pl.ds(h * HC, HC)],
                send_sem=ssem.at[e],
                recv_sem=rsem.at[e],
                device_id=(me_d, to),
                device_id_type=MESH,
            ).start()

    def keep_pencil(sb, rb, h):
        rb[me_p, pl.ds(h * HC, HC)] = sb[me_p, pl.ds(h * HC, HC)]

    def place(d):
        return lax.rem(d // 2, 2), 2 * (d // 4) + lax.rem(d, 2)

    def send_dp(e, sb, rb):
        @pl.loop(1, 16)
        def _(d):
            to = lax.rem(me_d + d, 16)
            pltpu.make_async_remote_copy(
                src_ref=sb.at[place(to)],
                dst_ref=rb.at[me_d],
                send_sem=ssem.at[e],
                recv_sem=rsem.at[e],
                device_id=(to, me_p),
                device_id_type=MESH,
            ).start()

        rb[me_d] = sb[place(me_d)]

    def swap(i, src, dst):
        return pltpu.make_async_remote_copy(
            src_ref=src,
            dst_ref=dst,
            send_sem=yssem.at[i],
            recv_sem=yrsem.at[i],
            device_id=(partner, me_p),
            device_id_type=MESH,
        )

    def piece(x, c):
        return 2 * x + c

    def part(r, half):
        return wall.at[r, pl.ds(half * KH, KH)]

    def weights(i, r, half, x, c):
        return pltpu.make_async_remote_copy(
            src_ref=part(r, half),
            dst_ref=part(r, half),
            send_sem=wssem.at[i],
            recv_sem=wrsem.at[i],
            device_id=(4 * x + 2 * me_y + c, me_p),
            device_id_type=MESH,
        )

    sib = 1 - me_c
    own, up, down, far = (piece(x, me_c) for x in (me_x, x_up, x_down, x_far))
    moves = [
        weights(0, own, 0, x_up, me_c),
        weights(1, own, 1, x_down, me_c),
        weights(2, own, 1, x_up, me_c),
        weights(3, own, 0, x_down, me_c),
        weights(4, own, 0, me_x, sib),
        weights(5, own, 1, me_x, sib),
        weights(6, down, 0, x_up, me_c),
        weights(7, up, 1, x_down, me_c),
        weights(8, down, 0, me_x, sib),
        weights(9, up, 1, me_x, sib),
        weights(10, down, 1, me_x, sib),
        weights(11, up, 0, me_x, sib),
        weights(12, far, 0, me_x, sib),
        weights(13, far, 1, me_x, sib),
    ]

    def arrived(i):
        moves[i].wait_recv()

    def wait_pencil(sem, buf, h):
        part = buf.at[pl.ds(0, 15), pl.ds(h * HC, HC)]
        pltpu.make_async_copy(part, part, sem).wait()

    def wait_dp(sem, buf):
        part = buf.at[pl.ds(0, 15)]
        pltpu.make_async_copy(part, part, sem).wait()

    def z_store(a, x, g0, n):
        for i in range(n):
            for kh in range(2):
                row = pl.multiple_of((kh * 4 + x) * HC, HC)
                a2[pl.ds(row, HC), (g0 + i) * 128 : (g0 + i + 1) * 128] = a[
                    i * HC : (i + 1) * HC, kh * 128 : (kh + 1) * 128
                ]

    def y_forward(sb, h):
        y = dot(a2[...], t_ref[...])

        def get(e):
            kh, ri, x = e // 8, (e // 4) % 2, e % 4
            at = (kh * 4 + x) * HC
            return y[at : at + HC, ri * 128 : (ri + 1) * 128]

        def put(j, tile):
            sb[j, h * HC : (h + 1) * HC, :] = tile.astype(BF16)

        turn_slots(slot_masks(HC), get, put)

    def x_forward(rb, h):
        low, high = [], []
        for g in range(8):
            a = rb[2 * g, h * HC : (h + 1) * HC, :].astype(F32)
            b = roll(rb[2 * g + 1, h * HC : (h + 1) * HC, :].astype(F32), 64)
            low.append(halves(a, b).astype(BF16))
            high.append(roll(halves(b, a), 64).astype(BF16))
        lhs = jnp.concatenate(
            [jnp.concatenate(low, axis=1), jnp.concatenate(high, axis=1)], axis=0
        )
        o = dot(lhs, t_ref[...])
        for kh in range(2):
            xo[kh * CH + h * HC : kh * CH + (h + 1) * HC, :] = o[kh * HC : (kh + 1) * HC]

    def modes_out(dst, scaled):
        turned = xo[...].T
        if scaled:
            row = lax.broadcasted_iota(jnp.int32, (256, 128), 0)
            lane = lax.broadcasted_iota(jnp.int32, (256, 128), 1)
            zero = ((row % KH) == 0) & (lane < 64)
            turned = turned * jnp.where(zero, SCALE, 2.0 * SCALE)
        for j in range(16):
            dst[(j // 2) % 2, 2 * (j // 4) + j % 2] = jnp.concatenate(
                [turned[j * 8 : j * 8 + 8], turned[128 + j * 8 : 136 + j * 8]], axis=0
            ).astype(BF16)

    def modes_in(src):
        v = [src[(j // 2) % 2, 2 * (j // 4) + j % 2].astype(F32) for j in range(16)]
        both = jnp.concatenate([t[:8] for t in v] + [t[8:] for t in v], axis=0)
        xi[...] = both.T.astype(BF16)

    def x_inverse(sb, h):
        lhs = jnp.concatenate(
            [xi[kh * CH + h * HC : kh * CH + (h + 1) * HC, :] for kh in range(2)], axis=0
        )
        o = dot(lhs, tt_ref[...])
        for g in range(8):
            low = o[:HC, g * 128 : (g + 1) * 128]
            high = o[HC:, g * 128 : (g + 1) * 128]
            sb[2 * g, h * HC : (h + 1) * HC, :] = halves(low, roll(high, 64)).astype(BF16)
            sb[2 * g + 1, h * HC : (h + 1) * HC, :] = halves(roll(low, 64), high).astype(BF16)

    def mix(lhs, src, dst, scale):
        @pl.loop(0, 4)
        def _(x):
            for g in range(8):
                rhs = jnp.concatenate(
                    [src[x, g, :4].reshape(256, 128), src[x, g, 4:].reshape(256, 128)], axis=1
                )
                o = dot(lhs, rhs)
                o = (o if scale is None else o * scale).astype(dst.dtype)
                dst[x, g, :4] = o[:, :128].reshape(4, CH, 128)
                dst[x, g, 4:] = o[:, 128:].reshape(4, CH, 128)

    loads[4].wait()
    for h in range(CHUNKS):
        for x in range(4):
            if h == 0:
                loads[x].wait()
            lhs = jnp.concatenate(
                [
                    f_ref[x, :, p, h * HC : (h + 1) * HC, :].reshape(8 * HC, 128)
                    for p in range(8)
                ],
                axis=1,
            )
            z_store(dot(lhs, zf_ref[...]).astype(BF16), x, 0, 8)
        if h == 0:
            loads[5].wait()
        y_forward(s0, h)
        if h == 0:
            pl.semaphore_wait(barrier, 30)
        send_pencil(h, s0, r0, h)
        if h == 0:
            loads[6].wait()
            for i in range(6):
                moves[i].start()
        keep_pencil(s0, r0, h)

    loads[7].wait()
    lane64 = lax.broadcasted_iota(jnp.int32, (64, 128), 1)
    wl = wl_ref[...].astype(F32)
    wide = jnp.concatenate([wl] * 4, axis=1)
    tall = jnp.concatenate([wide] * 4, axis=0)
    row = lax.broadcasted_iota(jnp.int32, (256, 256), 0) // 64
    col = lax.broadcasted_iota(jnp.int32, (256, 256), 1) // 64
    block = jnp.where(row == col, tall, 0.0)
    bw[0] = block.T.astype(BF16)
    bw[1] = block.astype(BF16)
    mix(bw[0], f_ref, big, math.sqrt(0.5))

    for h in range(CHUNKS):
        wait_pencil(rsem.at[h], r0, h)
        x_forward(r0, h)
        if h == 0:
            arrived(0)
            arrived(1)
            for i in range(6, 10):
                moves[i].start()
    modes_out(us, False)
    ask_u = swap(0, us.at[1 - me_y], row_u)
    ask_u.start()
    arrived(2)
    arrived(3)
    moves[10].start()
    moves[11].start()
    arrived(6)
    arrived(7)
    moves[12].start()
    moves[13].start()
    loads[9].wait()
    loads[10].wait()
    loads[8].wait()

    row16 = lax.broadcasted_iota(jnp.int32, (16, 128), 0)
    lane16 = lax.broadcasted_iota(jnp.int32, (16, 128), 1)
    block16 = [(row16 % KH) == (2 * t + lane16 // 64) for t in range(4)]
    sign8 = jnp.where(lax.broadcasted_iota(jnp.int32, (8, 128), 1) < 64, -1.0, 1.0)
    first8 = lax.broadcasted_iota(jnp.int32, (8, 128), 0) == 0
    root = math.sqrt(0.5)

    def forward_mode(u, r):
        u = u.astype(F32)
        turned = roll(u, 64)
        v = []
        for kh in range(2):
            twice = halves(u, turned) if kh == 0 else halves(turned, u)
            lhs = jnp.concatenate([jnp.where(m, twice, 0.0) for m in block16], axis=1)
            o = dot(lhs.astype(BF16), wall[r, kh * KH : (kh + 1) * KH].reshape(512, 128))
            o = o[:8] + sign8 * roll(o[8:], 64)
            scale = jnp.where(first8, root * SCALE, 2.0 * root * SCALE) if kh == 0 else 2.0 * root * SCALE
            v.append(o * scale)
        return jnp.concatenate(
            [halves(v[0], roll(v[1], 64)), halves(roll(v[0], 64), v[1])], axis=0
        ).astype(BF16)

    def adjoint_mode(g, r):
        g = g.astype(F32)
        re, im = g[:8], g[8:]
        re_t, im_t = roll(re, 64), roll(im, 64)
        d = []
        for kh in range(2):
            if kh == 0:
                lhs = [halves(re, im_t), halves(im, -re_t)]
            else:
                lhs = [halves(re_t, im), halves(im_t, -re)]
            lhs = jnp.concatenate(lhs, axis=0).astype(BF16)
            o = dot_t(lhs, wall[r, kh * KH : (kh + 1) * KH].reshape(512, 128))
            o = sum(jnp.where(block16[t], o[:, t * 128 : (t + 1) * 128], 0.0) for t in range(4))
            d.append(o + roll(o, 64))
        return halves(d[0], d[1]).astype(BF16)

    def local_modes(mode, src, dst, pieces):
        for r in pieces:
            dst[me_y, r] = mode(src[me_y, r], r)

    def row_modes(mode, src, dst):
        for r in range(8):
            dst[r] = mode(src[r], r)

    local_modes(forward_mode, us, row_v, (own, up, down, far))
    for i in (4, 5, 8, 9, 10, 11, 12, 13):
        arrived(i)
    local_modes(forward_mode, us, row_v, [piece(x, sib) for x in (me_x, x_up, x_down, x_far)])
    ask_u.wait_recv()
    row_modes(forward_mode, row_u, back_v)
    give_v = swap(1, back_v, row_v.at[me_y])
    give_v.start()
    send_dp(2, us, ur)
    give_v.wait_recv()
    modes_in(row_v)
    for h in range(CHUNKS):
        x_inverse(s1, h)
        send_pencil(4 + h, s1, r1, h)
        keep_pencil(s1, r1, h)

    for h in range(CHUNKS):
        wait_pencil(rsem.at[4 + h], r1, h)
        y_inverse(r1, h * HC, HC, ly)
        vy[...] = dot(ly[...], tt_ref[...]).astype(BF16)

        @pl.loop(0, 2)
        def _(x2, h=h):
            for xi_ in range(2):
                x = 2 * x2 + xi_
                rows = [pl.ds(pl.multiple_of((kh * 4 + x) * HC, HC), HC) for kh in range(2)]
                lhs = jnp.concatenate(
                    [
                        jnp.concatenate([vy[r, g * 128 : (g + 1) * 128] for r in rows], axis=1)
                        for g in range(8)
                    ],
                    axis=0,
                )
                parts = []
                for n in range(4):
                    v = dot(lhs, zt_ref[:, n * 256 : (n + 1) * 256])
                    for i in range(2):
                        at = (x, slice(None), 2 * n + i, slice(h * HC, (h + 1) * HC))
                        pre = v[:, i * 128 : (i + 1) * 128].reshape(8, HC, 128) + big[at]
                        sl = (c_ref[at].astype(F32) * gelu_slope(pre)).astype(BF16)
                        slope[at] = sl
                        parts.append(sl.reshape(8 * HC, 128))
                z_store(dot(jnp.concatenate(parts, axis=1), zf_ref[...]).astype(BF16), x, 0, 8)

        y_forward(s2, h)
        send_pencil(6 + h, s2, r2, h)
        keep_pencil(s2, r2, h)

    mix(bw[1], slope, sp, None)
    sp_copy = pltpu.make_async_copy(sp, sp_hbm, osem.at[0])
    sp_copy.start()

    for h in range(CHUNKS):
        wait_pencil(rsem.at[6 + h], r2, h)
        x_forward(r2, h)
    modes_out(gs, True)
    ask_g = swap(2, gs.at[1 - me_y], row_g)
    ask_g.start()
    local_modes(adjoint_mode, gs, row_d, range(8))
    ask_g.wait_recv()
    row_modes(adjoint_mode, row_g, back_d)
    give_d = swap(3, back_d, row_d.at[me_y])
    give_d.start()
    send_dp(8, gs, gr)
    give_d.wait_recv()
    modes_in(row_d)
    own_copies = []
    for h in range(CHUNKS):
        x_inverse(s3, h)
        send_pencil(10 + h, s3, r3, h)
        rows = pl.ds(h * HC, HC)
        own_copies.append(
            pltpu.make_async_copy(s3.at[me_p, rows], r3.at[me_p, rows], osem.at[2 + h])
        )
        own_copies[h].start()

    def regroup(src, i):
        xf[...] = src[...].astype(F32).reshape(256, 128)
        for k in range(KH):
            re = xf[pl.ds(k, 16, stride=16), :]
            im = xf[pl.ds(KH + k, 16, stride=16), :]
            ukeep[i, k] = halves(re, roll(im, 64)).astype(BF16)
            ukeep[i, KH + k] = halves(roll(re, 64), im).astype(BF16)

    wait_dp(rsem.at[2], ur)
    regroup(ur, 0)
    wait_dp(rsem.at[8], gr)
    regroup(gr, 1)
    for k in range(MZ):
        cross = lax.dot_general(
            ukeep[0, k], ukeep[1, k], (((0,), (0,)), ((), ())), preferred_element_type=F32
        )
        low = roll(cross[64:], 64)
        gw_v[k] = cross[:64] + jnp.where(lane64 < 64, low, -low)
    gw_copy = pltpu.make_async_copy(gw_v, gw_hbm, osem.at[1])
    gw_copy.start()

    for h in range(CHUNKS):
        wait_pencil(ssem.at[h], s0, h)
        wait_pencil(ssem.at[4 + h], s1, h)
        wait_pencil(ssem.at[6 + h], s2, h)
    wait_dp(ssem.at[2], ur)
    wait_dp(ssem.at[8], gr)
    for copy in moves + [ask_u, give_v, ask_g, give_d]:
        copy.wait_send()
    sp_copy.wait()
    gw_copy.wait()
    for h in range(CHUNKS):
        own_copies[h].wait()
        wait_pencil(ssem.at[10 + h], s3, h)
        wait_pencil(rsem.at[10 + h], r3, h)


def last_kernel(
    r_hbm, sp_hbm, gw_in, tt_hbm, zt_hbm, out_hbm, gw_hbm,
    r_ref, sp, tt_ref, zt_ref, ly, vy, out_v, gw_v, lsem, osem,
):
    loads = [
        pltpu.make_async_copy(r_hbm, r_ref, lsem.at[0]),
        pltpu.make_async_copy(tt_hbm, tt_ref, lsem.at[1]),
        pltpu.make_async_copy(zt_hbm, zt_ref, lsem.at[2]),
        pltpu.make_async_copy(gw_in, gw_v, lsem.at[3]),
    ]
    loads += [pltpu.make_async_copy(sp_hbm.at[x], sp.at[x], lsem.at[4 + x]) for x in range(4)]
    for copy in loads:
        copy.start()
    loads[0].wait()
    y_inverse(r_ref, 0, CH, ly)
    loads[1].wait()
    vy[...] = dot(ly[...], tt_ref[...]).astype(BF16)
    loads[2].wait()
    outs = []
    for x in range(4):
        loads[4 + x].wait()
        lhs = jnp.concatenate(
            [
                jnp.concatenate(
                    [
                        vy[(kh * 4 + x) * CH : (kh * 4 + x + 1) * CH, g * 128 : (g + 1) * 128]
                        for kh in range(2)
                    ],
                    axis=1,
                )
                for g in range(8)
            ],
            axis=0,
        )
        for n in range(4):
            v = dot(lhs, zt_ref[:, n * 256 : (n + 1) * 256])
            for i in range(2):
                part = v[:, i * 128 : (i + 1) * 128].reshape(8, CH, 128)
                out_v[x, :, 2 * n + i] = (part + sp[x, :, 2 * n + i].astype(F32)).astype(BF16)
        outs.append(pltpu.make_async_copy(out_v.at[x], out_hbm.at[0, x], osem.at[x]))
        outs[x].start()
        if x == 0:
            loads[3].wait()
            outs_gw = pltpu.make_async_copy(gw_v, gw_hbm.at[0, 0], osem.at[4])
            outs_gw.start()
    for copy in outs:
        copy.wait()
    outs_gw.wait()


def body(field, cotangent, w_spec, w_local):
    table, zf = line_table(), z_table()
    t, tt, zf, zt = (jnp.asarray(m.astype(jnp.bfloat16)) for m in (table, table.T, zf, zf.T))
    grid = (4, 8, 8, CH, NZ)
    any_spec = pl.BlockSpec(memory_space=pl.ANY)
    pencil_buf = pltpu.VMEM((16, CH, 128), BF16)
    dp_buf = pltpu.VMEM((16, 16, 128), BF16)
    both = pltpu.VMEM((2, 8, 16, 128), BF16)
    row = pltpu.VMEM((8, 16, 128), BF16)
    grid_b16 = pltpu.VMEM(grid, BF16)
    line = pltpu.VMEM((1024, 256), BF16)
    line_t = pltpu.VMEM((256, 1024), BF16)
    keep = pltpu.VMEM((2, MZ, 16, 128), BF16)
    r3, sp, gw = pl.pallas_call(
        kernel,
        out_shape=(
            jax.ShapeDtypeStruct((16, CH, 128), BF16),
            jax.ShapeDtypeStruct(grid, BF16),
            jax.ShapeDtypeStruct((MZ, CH, 2 * CH), F32),
        ),
        in_specs=[any_spec] * 8,
        out_specs=[any_spec] * 3,
        scratch_shapes=[
            grid_b16,
            grid_b16,
            pltpu.VMEM((8, MZ, CH, 2 * CH), BF16),
            pltpu.VMEM((CH, CH), BF16),
            line,
            line_t,
            line,
            line_t,
            pltpu.VMEM(grid, F32),
            grid_b16,
            grid_b16,
            pltpu.VMEM((MZ, CH, 2 * CH), F32),
            pltpu.VMEM((8 * HC, 1024), BF16),
            pltpu.VMEM((8 * HC, 256), BF16),
            pltpu.VMEM((8 * HC, 1024), BF16),
            pltpu.VMEM((128, 256), F32),
            pltpu.VMEM((128, 256), BF16),
            pltpu.VMEM((2, 256, 256), BF16),
            pltpu.VMEM((256, 128), F32),
            keep,
        ]
        + [pencil_buf] * 7
        + [both, dp_buf, both, dp_buf, row, both, row, row, both, row]
        + [
            pltpu.SemaphoreType.DMA((11,)),
            pltpu.SemaphoreType.DMA((4,)),
            pltpu.SemaphoreType.DMA((12,)),
            pltpu.SemaphoreType.DMA((12,)),
            pltpu.SemaphoreType.DMA((14,)),
            pltpu.SemaphoreType.DMA((14,)),
            pltpu.SemaphoreType.DMA((4,)),
            pltpu.SemaphoreType.DMA((4,)),
        ],
        compiler_params=pltpu.CompilerParams(
            collective_id=0, has_side_effects=True, vmem_limit_bytes=60 * 1024 * 1024
        ),
        name="layer",
    )(field.reshape((1,) + grid), cotangent.reshape((1,) + grid), w_spec, w_local, t, tt, zf, zt)
    out, gw = pl.pallas_call(
        last_kernel,
        out_shape=(
            jax.ShapeDtypeStruct((1,) + grid, BF16),
            jax.ShapeDtypeStruct((1, 1, MZ, CH, 2 * CH), F32),
        ),
        in_specs=[any_spec] * 5,
        out_specs=[any_spec] * 2,
        scratch_shapes=[
            pencil_buf,
            grid_b16,
            line_t,
            line_t,
            pltpu.VMEM((8 * CH, 256), BF16),
            pltpu.VMEM((8 * CH, 1024), BF16),
            grid_b16,
            pltpu.VMEM((MZ, CH, 2 * CH), F32),
            pltpu.SemaphoreType.DMA((8,)),
            pltpu.SemaphoreType.DMA((5,)),
        ],
        compiler_params=pltpu.CompilerParams(vmem_limit_bytes=60 * 1024 * 1024),
        name="last",
    )(r3, sp, gw, tt, zt)
    return (out.reshape(1, 4, NY, CH, NZ), gw)


def solution(mesh):
    placed = P("dp", "pencil", None, None, None)
    return jax.shard_map(
        body,
        mesh=mesh,
        in_specs=(placed, placed, placed, P()),
        out_specs=(placed, placed),
        check_vma=False,
    )
```

```python
import functools
import math

import jax
import jax.numpy as jnp
import numpy as np
from jax import lax
from jax.experimental import pallas as pl
from jax.experimental.pallas import tpu as pltpu
from jax.sharding import PartitionSpec as P

NX = 64
NY = 64
NZ = 128
CH = 64
MX = 16
MY = 16
MZ = 16
KH = 8
MESH = pl.DeviceIdType.MESH
F32 = jnp.float32
BF16 = jnp.bfloat16
CHUNKS = 4
HC = CH // CHUNKS
SCALE = 1.0 / (NX * NY * NZ)


def line_table():
    position = np.arange(NX)
    freq = np.arange(MX)
    freq = np.where(freq < MX // 2, freq, freq - MX)
    angle = 2.0 * math.pi * np.mod(position[:, None] * freq[None, :], NX) / NX
    cos, sin = np.cos(angle).reshape(8, 2, 4, MX), np.sin(angle).reshape(8, 2, 4, MX)
    table = np.zeros((8, 2, 2, 4, KH, 2, MX, KH), np.float32)
    for k in range(KH):
        table[:, :, 0, :, k, 0, :, k] = cos
        table[:, :, 1, :, k, 0, :, k] = sin
        table[:, :, 1, :, k, 1, :, k] = cos
        table[:, :, 0, :, k, 1, :, k] = -sin
    return table.reshape(1024, 256)


def z_table():
    angle = 2.0 * math.pi * np.mod(np.arange(NZ)[:, None] * np.arange(MZ)[None, :], NZ) / NZ
    angle = angle.reshape(NZ, 2, KH)
    table = np.zeros((2, 4, NZ, 2, 2, 2, 4, KH), np.float32)
    for half in range(2):
        for q in range(4):
            table[half, q, :, :, half, 0, q, :] = np.cos(angle)
            table[half, q, :, :, half, 1, q, :] = -np.sin(angle)
    return table.reshape(1024, 256)


def dot(a, b):
    return jnp.dot(a, b, preferred_element_type=F32)


def dot_t(a, b):
    return lax.dot_general(a, b, (((1,), (1,)), ((), ())), preferred_element_type=F32)


def gelu_slope(t):
    bell = jnp.exp2(t * t * (-1.0 / math.log(2.0)) - 0.5 * math.log2(math.pi))
    return 0.5 * lax.erf(t) + (t * bell + 0.5)


def roll(v, amount):
    amount %= 128
    return v if amount == 0 else pltpu.roll(v, amount, 1)


def halves(low, high):
    lane = lax.broadcasted_iota(jnp.int32, low.shape, 1)
    return jnp.where(lane < 64, low, high)


def slot_masks(rows):
    slot = lax.broadcasted_iota(jnp.int32, (rows, 128), 1) // KH
    return [slot == m for m in range(16)]


def turn_slots(masks, get, put):
    rolled = [roll(get(j), KH * j) for j in range(16)]
    for e in range(16):
        out = rolled[(0 - e) % 16]
        for m in range(1, 16):
            out = jnp.where(masks[m], rolled[(m - e) % 16], out)
        put(e, roll(out, -KH * e))


def y_inverse(rb, c0, rows, ly):
    masks = slot_masks(rows)

    def put(e, tile):
        kh, ri, x = e // 8, (e // 4) % 2, e % 4
        at = (kh * 4 + x) * rows
        ly[at : at + rows, ri * 128 : (ri + 1) * 128] = tile.astype(BF16)

    turn_slots(masks, lambda j: rb[j, pl.ds(c0, rows), :].astype(F32), put)


def kernel(
    field_hbm, cot_hbm, w_hbm, wl_hbm, t_hbm, tt_hbm, zf_hbm, zt_hbm,
    r3, sp_hbm, gw_hbm,
    f_ref, c_ref, wall, wl_ref, t_ref, tt_ref, zf_ref, zt_ref, big, slope, sp, gw_v,
    a2, ly, vy, xo, xi, bw, xf, ukeep,
    s0, r0, s1, r1, s2, r2, s3,
    us, ur, gs, gr, row_u, row_v, back_v, row_g, row_d, back_d,
    lsem, osem, ssem, rsem, wssem, wrsem, yssem, yrsem,
):
    me_d = lax.axis_index("dp")
    me_p = lax.axis_index("pencil")
    me_x, me_y, me_c = me_d // 4, lax.rem(me_d // 2, 2), lax.rem(me_d, 2)
    x_up, x_down, x_far = lax.rem(me_x + 1, 4), lax.rem(me_x + 3, 4), lax.rem(me_x + 2, 4)
    partner = me_d + 2 - 4 * me_y

    def load(src, dst, i):
        return pltpu.make_async_copy(src, dst, lsem.at[i])

    def rows_of(h):
        return pl.ds(pl.multiple_of(h * HC, HC), HC)

    every = slice(None)
    loads = [
        load(
            field_hbm.at[0, every, every, every, rows_of(h)],
            f_ref.at[every, every, every, rows_of(h)],
            h,
        )
        for h in range(CHUNKS)
    ]
    loads += [
        load(zf_hbm, zf_ref, 4),
        load(t_hbm, t_ref, 5),
        load(w_hbm.at[0, 0], wall.at[2 * me_x + me_c], 6),
        load(wl_hbm, wl_ref, 7),
        load(cot_hbm.at[0], c_ref, 8),
        load(tt_hbm, tt_ref, 9),
        load(zt_hbm, zt_ref, 10),
    ]
    for i in (4, 0, 5, 6, 1, 2, 3, 7, 9, 10, 8):
        loads[i].start()

    barrier = pltpu.get_barrier_semaphore()

    @pl.loop(1, 16)
    def _(d):
        pl.semaphore_signal(
            barrier, inc=1, device_id=(me_d, lax.rem(me_p + d, 16)), device_id_type=MESH
        )
        pl.semaphore_signal(
            barrier, inc=1, device_id=(lax.rem(me_d + d, 16), me_p), device_id_type=MESH
        )

    def send_pencil(e, sb, rb, h):
        @pl.loop(1, 16)
        def _(d):
            to = lax.rem(me_p + d, 16)
            pltpu.make_async_remote_copy(
                src_ref=sb.at[to, rows_of(h)],
                dst_ref=rb.at[me_p, rows_of(h)],
                send_sem=ssem.at[e],
                recv_sem=rsem.at[e],
                device_id=(me_d, to),
                device_id_type=MESH,
            ).start()

    def keep_pencil(sb, rb, h):
        rb[me_p, rows_of(h)] = sb[me_p, rows_of(h)]

    def place(d):
        return lax.rem(d // 2, 2), 2 * (d // 4) + lax.rem(d, 2)

    def send_dp(e, sb, rb):
        @pl.loop(1, 16)
        def _(d):
            to = lax.rem(me_d + d, 16)
            pltpu.make_async_remote_copy(
                src_ref=sb.at[place(to)],
                dst_ref=rb.at[me_d],
                send_sem=ssem.at[e],
                recv_sem=rsem.at[e],
                device_id=(to, me_p),
                device_id_type=MESH,
            ).start()

        rb[me_d] = sb[place(me_d)]

    def swap(i, src, dst):
        return pltpu.make_async_remote_copy(
            src_ref=src,
            dst_ref=dst,
            send_sem=yssem.at[i],
            recv_sem=yrsem.at[i],
            device_id=(partner, me_p),
            device_id_type=MESH,
        )

    def piece(x, c):
        return 2 * x + c

    def part(r, half):
        return wall.at[r, pl.ds(half * KH, KH)]

    def weights(i, r, half, x, c):
        return pltpu.make_async_remote_copy(
            src_ref=part(r, half),
            dst_ref=part(r, half),
            send_sem=wssem.at[i],
            recv_sem=wrsem.at[i],
            device_id=(4 * x + 2 * me_y + c, me_p),
            device_id_type=MESH,
        )

    sib = 1 - me_c
    own, up, down, far = (piece(x, me_c) for x in (me_x, x_up, x_down, x_far))
    moves = [
        weights(0, own, 0, x_up, me_c),
        weights(1, own, 1, x_down, me_c),
        weights(2, own, 1, x_up, me_c),
        weights(3, own, 0, x_down, me_c),
        weights(4, own, 0, me_x, sib),
        weights(5, own, 1, me_x, sib),
        weights(6, down, 0, x_up, me_c),
        weights(7, up, 1, x_down, me_c),
        weights(8, down, 0, me_x, sib),
        weights(9, up, 1, me_x, sib),
        weights(10, down, 1, me_x, sib),
        weights(11, up, 0, me_x, sib),
        weights(12, far, 0, me_x, sib),
        weights(13, far, 1, me_x, sib),
    ]

    def arrived(i):
        moves[i].wait_recv()

    def wait_pencil(sem, buf, h):
        part = buf.at[pl.ds(0, 15), rows_of(h)]
        pltpu.make_async_copy(part, part, sem).wait()

    def wait_dp(sem, buf):
        part = buf.at[pl.ds(0, 15)]
        pltpu.make_async_copy(part, part, sem).wait()

    def z_forward(parts):
        a = dot(jnp.concatenate(parts, axis=1), zf_ref[...]).astype(BF16)
        for x in range(4):
            for g in range(8):
                for kh in range(2):
                    a2[(kh * 4 + x) * HC : (kh * 4 + x + 1) * HC, g * 128 : (g + 1) * 128] = a[
                        (x * 8 + g) * HC : (x * 8 + g + 1) * HC, kh * 128 : (kh + 1) * 128
                    ]

    def y_forward(sb, h):
        y = dot(a2[...], t_ref[...])

        def get(e):
            kh, ri, x = e // 8, (e // 4) % 2, e % 4
            at = (kh * 4 + x) * HC
            return y[at : at + HC, ri * 128 : (ri + 1) * 128]

        def put(j, tile):
            sb[j, rows_of(h), :] = tile.astype(BF16)

        turn_slots(slot_masks(HC), get, put)

    def x_forward(rb, h):
        low, high = [], []
        for g in range(8):
            a = rb[2 * g, h * HC : (h + 1) * HC, :].astype(F32)
            b = roll(rb[2 * g + 1, h * HC : (h + 1) * HC, :].astype(F32), 64)
            low.append(halves(a, b).astype(BF16))
            high.append(roll(halves(b, a), 64).astype(BF16))
        lhs = jnp.concatenate(
            [jnp.concatenate(low, axis=1), jnp.concatenate(high, axis=1)], axis=0
        )
        o = dot(lhs, t_ref[...])
        for kh in range(2):
            xo[kh * CH + h * HC : kh * CH + (h + 1) * HC, :] = o[kh * HC : (kh + 1) * HC]

    def modes_out(dst, scaled):
        turned = xo[...].T
        if scaled:
            row = lax.broadcasted_iota(jnp.int32, (256, 128), 0)
            lane = lax.broadcasted_iota(jnp.int32, (256, 128), 1)
            zero = ((row % KH) == 0) & (lane < 64)
            turned = turned * jnp.where(zero, SCALE, 2.0 * SCALE)
        for j in range(16):
            dst[(j // 2) % 2, 2 * (j // 4) + j % 2] = jnp.concatenate(
                [turned[j * 8 : j * 8 + 8], turned[128 + j * 8 : 136 + j * 8]], axis=0
            ).astype(BF16)

    def modes_in(src):
        v = [src[(j // 2) % 2, 2 * (j // 4) + j % 2].astype(F32) for j in range(16)]
        both = jnp.concatenate([t[:8] for t in v] + [t[8:] for t in v], axis=0)
        xi[...] = both.T.astype(BF16)

    def x_inverse(sb, send):
        o = dot(xi[...], tt_ref[...])
        for h in range(CHUNKS):
            for g in range(8):
                low = o[h * HC : (h + 1) * HC, g * 128 : (g + 1) * 128]
                high = o[CH + h * HC : CH + (h + 1) * HC, g * 128 : (g + 1) * 128]
                sb[2 * g, h * HC : (h + 1) * HC, :] = halves(low, roll(high, 64)).astype(BF16)
                sb[2 * g + 1, h * HC : (h + 1) * HC, :] = halves(roll(low, 64), high).astype(BF16)
            send(h)

    def mix(lhs, src, dst, scale):
        @pl.loop(0, 4)
        def _(x):
            for g in range(8):
                rhs = jnp.concatenate(
                    [src[x, g, :4].reshape(256, 128), src[x, g, 4:].reshape(256, 128)], axis=1
                )
                o = dot(lhs, rhs)
                o = (o if scale is None else o * scale).astype(dst.dtype)
                dst[x, g, :4] = o[:, :128].reshape(4, CH, 128)
                dst[x, g, 4:] = o[:, 128:].reshape(4, CH, 128)

    loads[4].wait()
    for h in range(CHUNKS):
        loads[h].wait()
        z_forward(
            [
                f_ref[:, :, p, h * HC : (h + 1) * HC, :].reshape(32 * HC, 128)
                for p in range(8)
            ]
        )
        if h == 0:
            loads[5].wait()
        y_forward(s0, h)
        if h == 0:
            loads[6].wait()
            pl.semaphore_wait(barrier, 30)
        send_pencil(h, s0, r0, h)
        if h == 0:
            for i in range(6):
                moves[i].start()
        keep_pencil(s0, r0, h)

    loads[7].wait()
    lane64 = lax.broadcasted_iota(jnp.int32, (64, 128), 1)
    wl = wl_ref[...].astype(F32)
    wide = jnp.concatenate([wl] * 4, axis=1)
    tall = jnp.concatenate([wide] * 4, axis=0)
    row = lax.broadcasted_iota(jnp.int32, (256, 256), 0) // 64
    col = lax.broadcasted_iota(jnp.int32, (256, 256), 1) // 64
    block = jnp.where(row == col, tall, 0.0)
    bw[0] = block.T.astype(BF16)
    bw[1] = block.astype(BF16)
    mix(bw[0], f_ref, big, math.sqrt(0.5))

    arrived(0)
    arrived(1)
    for i in range(6, 10):
        moves[i].start()
    for h in range(CHUNKS):
        wait_pencil(rsem.at[h], r0, h)
        x_forward(r0, h)
    modes_out(us, False)
    ask_u = swap(0, us.at[1 - me_y], row_u)
    ask_u.start()
    arrived(2)
    arrived(3)
    moves[10].start()
    moves[11].start()
    arrived(6)
    arrived(7)
    moves[12].start()
    moves[13].start()
    loads[9].wait()
    loads[10].wait()
    loads[8].wait()

    row16 = lax.broadcasted_iota(jnp.int32, (16, 128), 0)
    lane16 = lax.broadcasted_iota(jnp.int32, (16, 128), 1)
    block16 = [(row16 % KH) == (2 * t + lane16 // 64) for t in range(4)]
    sign8 = jnp.where(lax.broadcasted_iota(jnp.int32, (8, 128), 1) < 64, -1.0, 1.0)
    first8 = lax.broadcasted_iota(jnp.int32, (8, 128), 0) == 0
    root = math.sqrt(0.5)

    def forward_mode(u, r):
        u = u.astype(F32)
        turned = roll(u, 64)
        v = []
        for kh in range(2):
            twice = halves(u, turned) if kh == 0 else halves(turned, u)
            lhs = jnp.concatenate([jnp.where(m, twice, 0.0) for m in block16], axis=1)
            o = dot(lhs.astype(BF16), wall[r, kh * KH : (kh + 1) * KH].reshape(512, 128))
            o = o[:8] + sign8 * roll(o[8:], 64)
            scale = jnp.where(first8, root * SCALE, 2.0 * root * SCALE) if kh == 0 else 2.0 * root * SCALE
            v.append(o * scale)
        return jnp.concatenate(
            [halves(v[0], roll(v[1], 64)), halves(roll(v[0], 64), v[1])], axis=0
        ).astype(BF16)

    def adjoint_mode(g, r):
        g = g.astype(F32)
        re, im = g[:8], g[8:]
        re_t, im_t = roll(re, 64), roll(im, 64)
        d = []
        for kh in range(2):
            if kh == 0:
                lhs = [halves(re, im_t), halves(im, -re_t)]
            else:
                lhs = [halves(re_t, im), halves(im_t, -re)]
            lhs = jnp.concatenate(lhs, axis=0).astype(BF16)
            o = dot_t(lhs, wall[r, kh * KH : (kh + 1) * KH].reshape(512, 128))
            o = sum(jnp.where(block16[t], o[:, t * 128 : (t + 1) * 128], 0.0) for t in range(4))
            d.append(o + roll(o, 64))
        return halves(d[0], d[1]).astype(BF16)

    def local_modes(mode, src, dst, pieces):
        for r in pieces:
            dst[me_y, r] = mode(src[me_y, r], r)

    def row_modes(mode, src, dst):
        for r in range(8):
            dst[r] = mode(src[r], r)

    local_modes(forward_mode, us, row_v, (own, up, down, far))
    for i in (4, 5, 8, 9, 10, 11, 12, 13):
        arrived(i)
    local_modes(forward_mode, us, row_v, [piece(x, sib) for x in (me_x, x_up, x_down, x_far)])
    ask_u.wait_recv()
    row_modes(forward_mode, row_u, back_v)
    give_v = swap(1, back_v, row_v.at[me_y])
    give_v.start()
    send_dp(16, us, ur)
    give_v.wait_recv()
    modes_in(row_v)
    x_inverse(s1, lambda h: send_pencil(4 + h, s1, r1, h))
    for h in range(CHUNKS):
        keep_pencil(s1, r1, h)

    @pl.loop(0, CHUNKS)
    def _(h):
        wait_pencil(rsem.at[4 + h], r1, h)
        y_inverse(r1, pl.multiple_of(h * HC, HC), HC, ly)
        vy[...] = dot(ly[...], tt_ref[...]).astype(BF16)
        lhs = jnp.concatenate(
            [
                jnp.concatenate(
                    [
                        vy[(kh * 4 + x) * HC : (kh * 4 + x + 1) * HC, g * 128 : (g + 1) * 128]
                        for kh in range(2)
                    ],
                    axis=1,
                )
                for x in range(4)
                for g in range(8)
            ],
            axis=0,
        )
        parts = []
        for n in range(4):
            v = dot(lhs, zt_ref[:, n * 256 : (n + 1) * 256])
            for i in range(2):
                at = (every, every, 2 * n + i, rows_of(h))
                t = v[:, i * 128 : (i + 1) * 128].reshape(4, 8, HC, 128) + big[at]
                sl = (c_ref[at].astype(F32) * gelu_slope(t)).astype(BF16)
                slope[at] = sl
                parts.append(sl.reshape(32 * HC, 128))
        z_forward(parts)
        y_forward(s2, h)
        send_pencil(8 + h, s2, r2, h)
        keep_pencil(s2, r2, h)

    mix(bw[1], slope, sp, None)
    sp_copy = pltpu.make_async_copy(sp, sp_hbm, osem.at[0])
    sp_copy.start()

    for h in range(CHUNKS):
        wait_pencil(rsem.at[8 + h], r2, h)
        x_forward(r2, h)
    modes_out(gs, True)
    ask_g = swap(2, gs.at[1 - me_y], row_g)
    ask_g.start()
    local_modes(adjoint_mode, gs, row_d, range(8))
    ask_g.wait_recv()
    row_modes(adjoint_mode, row_g, back_d)
    give_d = swap(3, back_d, row_d.at[me_y])
    give_d.start()
    send_dp(17, gs, gr)
    give_d.wait_recv()
    modes_in(row_d)
    x_inverse(s3, lambda h: send_pencil(12 + h, s3, r3, h))
    own_copy = pltpu.make_async_copy(s3.at[me_p], r3.at[me_p], osem.at[2])
    own_copy.start()

    def regroup(src, i):
        xf[...] = src[...].astype(F32).reshape(256, 128)
        for k in range(KH):
            re = xf[pl.ds(k, 16, stride=16), :]
            im = xf[pl.ds(KH + k, 16, stride=16), :]
            ukeep[i, k] = halves(re, roll(im, 64)).astype(BF16)
            ukeep[i, KH + k] = halves(roll(re, 64), im).astype(BF16)

    wait_dp(rsem.at[16], ur)
    regroup(ur, 0)
    wait_dp(rsem.at[17], gr)
    regroup(gr, 1)
    for k in range(MZ):
        cross = lax.dot_general(
            ukeep[0, k], ukeep[1, k], (((0,), (0,)), ((), ())), preferred_element_type=F32
        )
        low = roll(cross[64:], 64)
        gw_v[k] = cross[:64] + jnp.where(lane64 < 64, low, -low)
    gw_copy = pltpu.make_async_copy(gw_v, gw_hbm, osem.at[1])
    gw_copy.start()

    for copy in moves + [ask_u, give_v, ask_g, give_d]:
        copy.wait_send()
    for h in range(CHUNKS):
        wait_pencil(ssem.at[h], s0, h)
        wait_pencil(ssem.at[4 + h], s1, h)
        wait_pencil(ssem.at[8 + h], s2, h)
    wait_dp(ssem.at[16], ur)
    wait_dp(ssem.at[17], gr)
    sp_copy.wait()
    gw_copy.wait()
    own_copy.wait()
    for h in range(CHUNKS):
        wait_pencil(ssem.at[12 + h], s3, h)
        wait_pencil(rsem.at[12 + h], r3, h)


def last_kernel(
    r_hbm, sp_hbm, gw_in, tt_hbm, zt_hbm, out_hbm, gw_hbm,
    r_ref, sp, tt_ref, zt_ref, ly, vy, out_v, gw_v, lsem, osem,
):
    loads = [
        pltpu.make_async_copy(r_hbm, r_ref, lsem.at[0]),
        pltpu.make_async_copy(tt_hbm, tt_ref, lsem.at[1]),
        pltpu.make_async_copy(zt_hbm, zt_ref, lsem.at[2]),
        pltpu.make_async_copy(gw_in, gw_v, lsem.at[3]),
    ]
    loads += [pltpu.make_async_copy(sp_hbm.at[x], sp.at[x], lsem.at[4 + x]) for x in range(4)]
    for copy in loads:
        copy.start()
    loads[0].wait()
    y_inverse(r_ref, 0, CH, ly)
    loads[1].wait()
    vy[...] = dot(ly[...], tt_ref[...]).astype(BF16)
    loads[2].wait()
    outs = []
    for x in range(4):
        loads[4 + x].wait()
        lhs = jnp.concatenate(
            [
                jnp.concatenate(
                    [
                        vy[(kh * 4 + x) * CH : (kh * 4 + x + 1) * CH, g * 128 : (g + 1) * 128]
                        for kh in range(2)
                    ],
                    axis=1,
                )
                for g in range(8)
            ],
            axis=0,
        )
        for n in range(4):
            v = dot(lhs, zt_ref[:, n * 256 : (n + 1) * 256])
            for i in range(2):
                part = v[:, i * 128 : (i + 1) * 128].reshape(8, CH, 128)
                out_v[x, :, 2 * n + i] = (part + sp[x, :, 2 * n + i].astype(F32)).astype(BF16)
        outs.append(pltpu.make_async_copy(out_v.at[x], out_hbm.at[0, x], osem.at[x]))
        outs[x].start()
        if x == 0:
            loads[3].wait()
            outs_gw = pltpu.make_async_copy(gw_v, gw_hbm.at[0, 0], osem.at[4])
            outs_gw.start()
    for copy in outs:
        copy.wait()
    outs_gw.wait()


def body(field, cotangent, w_spec, w_local):
    table, zf = line_table(), z_table()
    t, tt, zf, zt = (jnp.asarray(m.astype(jnp.bfloat16)) for m in (table, table.T, zf, zf.T))
    grid = (4, 8, 8, CH, NZ)
    any_spec = pl.BlockSpec(memory_space=pl.ANY)
    pencil_buf = pltpu.VMEM((16, CH, 128), BF16)
    dp_buf = pltpu.VMEM((16, 16, 128), BF16)
    both = pltpu.VMEM((2, 8, 16, 128), BF16)
    row = pltpu.VMEM((8, 16, 128), BF16)
    grid_b16 = pltpu.VMEM(grid, BF16)
    line = pltpu.VMEM((1024, 256), BF16)
    line_t = pltpu.VMEM((256, 1024), BF16)
    keep = pltpu.VMEM((2, MZ, 16, 128), BF16)
    r3, sp, gw = pl.pallas_call(
        kernel,
        out_shape=(
            jax.ShapeDtypeStruct((16, CH, 128), BF16),
            jax.ShapeDtypeStruct(grid, BF16),
            jax.ShapeDtypeStruct((MZ, CH, 2 * CH), F32),
        ),
        in_specs=[any_spec] * 8,
        out_specs=[any_spec] * 3,
        scratch_shapes=[
            grid_b16,
            grid_b16,
            pltpu.VMEM((8, MZ, CH, 2 * CH), BF16),
            pltpu.VMEM((CH, CH), BF16),
            line,
            line_t,
            line,
            line_t,
            pltpu.VMEM(grid, F32),
            grid_b16,
            grid_b16,
            pltpu.VMEM((MZ, CH, 2 * CH), F32),
            pltpu.VMEM((8 * HC, 1024), BF16),
            pltpu.VMEM((8 * HC, 256), BF16),
            pltpu.VMEM((8 * HC, 1024), BF16),
            pltpu.VMEM((128, 256), F32),
            pltpu.VMEM((128, 256), BF16),
            pltpu.VMEM((2, 256, 256), BF16),
            pltpu.VMEM((256, 128), F32),
            keep,
        ]
        + [pencil_buf] * 7
        + [both, dp_buf, both, dp_buf, row, both, row, row, both, row]
        + [
            pltpu.SemaphoreType.DMA((11,)),
            pltpu.SemaphoreType.DMA((4,)),
            pltpu.SemaphoreType.DMA((18,)),
            pltpu.SemaphoreType.DMA((18,)),
            pltpu.SemaphoreType.DMA((14,)),
            pltpu.SemaphoreType.DMA((14,)),
            pltpu.SemaphoreType.DMA((4,)),
            pltpu.SemaphoreType.DMA((4,)),
        ],
        compiler_params=pltpu.CompilerParams(
            collective_id=0, has_side_effects=True, vmem_limit_bytes=60 * 1024 * 1024
        ),
        name="layer",
    )(field.reshape((1,) + grid), cotangent.reshape((1,) + grid), w_spec, w_local, t, tt, zf, zt)
    out, gw = pl.pallas_call(
        last_kernel,
        out_shape=(
            jax.ShapeDtypeStruct((1,) + grid, BF16),
            jax.ShapeDtypeStruct((1, 1, MZ, CH, 2 * CH), F32),
        ),
        in_specs=[any_spec] * 5,
        out_specs=[any_spec] * 2,
        scratch_shapes=[
            pencil_buf,
            grid_b16,
            line_t,
            line_t,
            pltpu.VMEM((8 * CH, 256), BF16),
            pltpu.VMEM((8 * CH, 1024), BF16),
            grid_b16,
            pltpu.VMEM((MZ, CH, 2 * CH), F32),
            pltpu.SemaphoreType.DMA((8,)),
            pltpu.SemaphoreType.DMA((5,)),
        ],
        compiler_params=pltpu.CompilerParams(vmem_limit_bytes=60 * 1024 * 1024),
        name="last",
    )(r3, sp, gw, tt, zt)
    return (out.reshape(1, 4, NY, CH, NZ), gw)


def solution(mesh):
    placed = P("dp", "pencil", None, None, None)
    return jax.shard_map(
        body,
        mesh=mesh,
        in_specs=(placed, placed, placed, P()),
        out_specs=(placed, placed),
        check_vma=False,
    )
```

```python
import functools
import math

import jax
import jax.numpy as jnp
import numpy as np
from jax import lax
from jax.experimental import pallas as pl
from jax.experimental.pallas import tpu as pltpu
from jax.sharding import PartitionSpec as P

NX = 64
NY = 64
NZ = 128
CH = 64
MX = 16
MY = 16
MZ = 16
KH = 8
MESH = pl.DeviceIdType.MESH
F32 = jnp.float32
BF16 = jnp.bfloat16
CHUNKS = 4
HC = CH // CHUNKS
SCALE = 1.0 / (NX * NY * NZ)


def line_table():
    position = np.arange(NX)
    freq = np.arange(MX)
    freq = np.where(freq < MX // 2, freq, freq - MX)
    angle = 2.0 * math.pi * np.mod(position[:, None] * freq[None, :], NX) / NX
    cos, sin = np.cos(angle).reshape(8, 2, 4, MX), np.sin(angle).reshape(8, 2, 4, MX)
    table = np.zeros((8, 2, 2, 4, KH, 2, MX, KH), np.float32)
    for k in range(KH):
        table[:, :, 0, :, k, 0, :, k] = cos
        table[:, :, 1, :, k, 0, :, k] = sin
        table[:, :, 1, :, k, 1, :, k] = cos
        table[:, :, 0, :, k, 1, :, k] = -sin
    return table.reshape(1024, 256)


def z_table():
    angle = 2.0 * math.pi * np.mod(np.arange(NZ)[:, None] * np.arange(MZ)[None, :], NZ) / NZ
    angle = angle.reshape(NZ, 2, KH)
    table = np.zeros((2, 4, NZ, 2, 2, 2, 4, KH), np.float32)
    for half in range(2):
        for q in range(4):
            table[half, q, :, :, half, 0, q, :] = np.cos(angle)
            table[half, q, :, :, half, 1, q, :] = -np.sin(angle)
    return table.reshape(1024, 256)


def dot(a, b):
    return jnp.dot(a, b, preferred_element_type=F32)


def dot_t(a, b):
    return lax.dot_general(a, b, (((1,), (1,)), ((), ())), preferred_element_type=F32)


def gelu_slope(t):
    bell = jnp.exp2(t * t * (-1.0 / math.log(2.0)) - 0.5 * math.log2(math.pi))
    return 0.5 * lax.erf(t) + (t * bell + 0.5)


def roll(v, amount):
    amount %= 128
    return v if amount == 0 else pltpu.roll(v, amount, 1)


def halves(low, high):
    lane = lax.broadcasted_iota(jnp.int32, low.shape, 1)
    return jnp.where(lane < 64, low, high)


def slot_masks(rows):
    slot = lax.broadcasted_iota(jnp.int32, (rows, 128), 1) // KH
    return [slot == m for m in range(16)]


def turn_slots(masks, get, put):
    rolled = [roll(get(j), KH * j) for j in range(16)]
    for e in range(16):
        out = rolled[(0 - e) % 16]
        for m in range(1, 16):
            out = jnp.where(masks[m], rolled[(m - e) % 16], out)
        put(e, roll(out, -KH * e))


def y_inverse(rb, c0, rows, ly):
    masks = slot_masks(rows)

    def put(e, tile):
        kh, ri, x = e // 8, (e // 4) % 2, e % 4
        at = (kh * 4 + x) * rows
        ly[at : at + rows, ri * 128 : (ri + 1) * 128] = tile.astype(BF16)

    turn_slots(masks, lambda j: rb[j, pl.ds(c0, rows), :].astype(F32), put)


def kernel(
    field_hbm, cot_hbm, w_hbm, wl_hbm, t_hbm, tt_hbm, zf_hbm, zt_hbm,
    r3, sp, gw_v, tt_ref, zt_ref,
    f_ref, c_ref, wall, wl_ref, t_ref, zf_ref, big, slope,
    a2, ly, vy, xo, xi, bw, xf, ukeep,
    s0, r0, s1, r1, s2, r2, s3,
    us, ur, gs, gr, row_u, row_v, back_v, row_g, row_d, back_d,
    lsem, ssem, rsem, wssem, wrsem, yssem, yrsem,
):
    me_d = lax.axis_index("dp")
    me_p = lax.axis_index("pencil")
    me_x, me_y, me_c = me_d // 4, lax.rem(me_d // 2, 2), lax.rem(me_d, 2)
    x_up, x_down, x_far = lax.rem(me_x + 1, 4), lax.rem(me_x + 3, 4), lax.rem(me_x + 2, 4)
    partner = me_d + 2 - 4 * me_y

    def load(src, dst, i):
        return pltpu.make_async_copy(src, dst, lsem.at[i])

    def rows_of(h):
        return pl.ds(pl.multiple_of(h * HC, HC), HC)

    every = slice(None)
    loads = [
        load(
            field_hbm.at[0, every, every, every, rows_of(h)],
            f_ref.at[every, every, every, rows_of(h)],
            h,
        )
        for h in range(CHUNKS)
    ]
    loads += [
        load(zf_hbm, zf_ref, 4),
        load(t_hbm, t_ref, 5),
        load(w_hbm.at[0, 0], wall.at[2 * me_x + me_c], 6),
        load(wl_hbm, wl_ref, 7),
        load(cot_hbm.at[0], c_ref, 8),
        load(tt_hbm, tt_ref, 9),
        load(zt_hbm, zt_ref, 10),
    ]
    for i in (4, 0, 5, 6, 1, 2, 3, 7, 9, 10, 8):
        loads[i].start()

    barrier = pltpu.get_barrier_semaphore()

    @pl.loop(1, 16)
    def _(d):
        pl.semaphore_signal(
            barrier, inc=1, device_id=(me_d, lax.rem(me_p + d, 16)), device_id_type=MESH
        )
        pl.semaphore_signal(
            barrier, inc=1, device_id=(lax.rem(me_d + d, 16), me_p), device_id_type=MESH
        )

    def send_pencil(e, sb, rb, h):
        @pl.loop(1, 16)
        def _(d):
            to = lax.rem(me_p + d, 16)
            pltpu.make_async_remote_copy(
                src_ref=sb.at[to, rows_of(h)],
                dst_ref=rb.at[me_p, rows_of(h)],
                send_sem=ssem.at[e],
                recv_sem=rsem.at[e],
                device_id=(me_d, to),
                device_id_type=MESH,
            ).start()

    def keep_pencil(sb, rb, h):
        rb[me_p, rows_of(h)] = sb[me_p, rows_of(h)]

    def place(d):
        return lax.rem(d // 2, 2), 2 * (d // 4) + lax.rem(d, 2)

    def send_dp(e, sb, rb):
        @pl.loop(1, 16)
        def _(d):
            to = lax.rem(me_d + d, 16)
            pltpu.make_async_remote_copy(
                src_ref=sb.at[place(to)],
                dst_ref=rb.at[me_d],
                send_sem=ssem.at[e],
                recv_sem=rsem.at[e],
                device_id=(to, me_p),
                device_id_type=MESH,
            ).start()

        rb[me_d] = sb[place(me_d)]

    def swap(i, src, dst):
        return pltpu.make_async_remote_copy(
            src_ref=src,
            dst_ref=dst,
            send_sem=yssem.at[i],
            recv_sem=yrsem.at[i],
            device_id=(partner, me_p),
            device_id_type=MESH,
        )

    def piece(x, c):
        return 2 * x + c

    def part(r, half):
        return wall.at[r, pl.ds(half * KH, KH)]

    def weights(i, r, half, x, c):
        return pltpu.make_async_remote_copy(
            src_ref=part(r, half),
            dst_ref=part(r, half),
            send_sem=wssem.at[i],
            recv_sem=wrsem.at[i],
            device_id=(4 * x + 2 * me_y + c, me_p),
            device_id_type=MESH,
        )

    sib = 1 - me_c
    own, up, down, far = (piece(x, me_c) for x in (me_x, x_up, x_down, x_far))
    moves = [
        weights(0, own, 0, x_up, me_c),
        weights(1, own, 1, x_down, me_c),
        weights(2, own, 1, x_up, me_c),
        weights(3, own, 0, x_down, me_c),
        weights(4, own, 0, me_x, sib),
        weights(5, own, 1, me_x, sib),
        weights(6, down, 0, x_up, me_c),
        weights(7, up, 1, x_down, me_c),
        weights(8, down, 0, me_x, sib),
        weights(9, up, 1, me_x, sib),
        weights(10, down, 1, me_x, sib),
        weights(11, up, 0, me_x, sib),
        weights(12, far, 0, me_x, sib),
        weights(13, far, 1, me_x, sib),
    ]

    def arrived(i):
        moves[i].wait_recv()

    def wait_pencil(sem, buf, h):
        part = buf.at[pl.ds(0, 15), rows_of(h)]
        pltpu.make_async_copy(part, part, sem).wait()

    def wait_dp(sem, buf):
        part = buf.at[pl.ds(0, 15)]
        pltpu.make_async_copy(part, part, sem).wait()

    def z_forward(parts):
        a = dot(jnp.concatenate(parts, axis=1), zf_ref[...]).astype(BF16)
        for x in range(4):
            for g in range(8):
                for kh in range(2):
                    a2[(kh * 4 + x) * HC : (kh * 4 + x + 1) * HC, g * 128 : (g + 1) * 128] = a[
                        (x * 8 + g) * HC : (x * 8 + g + 1) * HC, kh * 128 : (kh + 1) * 128
                    ]

    def y_forward(sb, h):
        y = dot(a2[...], t_ref[...])

        def get(e):
            kh, ri, x = e // 8, (e // 4) % 2, e % 4
            at = (kh * 4 + x) * HC
            return y[at : at + HC, ri * 128 : (ri + 1) * 128]

        def put(j, tile):
            sb[j, rows_of(h), :] = tile.astype(BF16)

        turn_slots(slot_masks(HC), get, put)

    def x_forward(rb, h):
        low, high = [], []
        for g in range(8):
            a = rb[2 * g, h * HC : (h + 1) * HC, :].astype(F32)
            b = roll(rb[2 * g + 1, h * HC : (h + 1) * HC, :].astype(F32), 64)
            low.append(halves(a, b).astype(BF16))
            high.append(roll(halves(b, a), 64).astype(BF16))
        lhs = jnp.concatenate(
            [jnp.concatenate(low, axis=1), jnp.concatenate(high, axis=1)], axis=0
        )
        o = dot(lhs, t_ref[...])
        for kh in range(2):
            xo[kh * CH + h * HC : kh * CH + (h + 1) * HC, :] = o[kh * HC : (kh + 1) * HC]

    def modes_out(dst, scaled):
        turned = xo[...].T
        if scaled:
            row = lax.broadcasted_iota(jnp.int32, (256, 128), 0)
            lane = lax.broadcasted_iota(jnp.int32, (256, 128), 1)
            zero = ((row % KH) == 0) & (lane < 64)
            turned = turned * jnp.where(zero, SCALE, 2.0 * SCALE)
        for j in range(16):
            dst[(j // 2) % 2, 2 * (j // 4) + j % 2] = jnp.concatenate(
                [turned[j * 8 : j * 8 + 8], turned[128 + j * 8 : 136 + j * 8]], axis=0
            ).astype(BF16)

    def modes_in(src):
        v = [src[(j // 2) % 2, 2 * (j // 4) + j % 2].astype(F32) for j in range(16)]
        both = jnp.concatenate([t[:8] for t in v] + [t[8:] for t in v], axis=0)
        xi[...] = both.T.astype(BF16)

    def x_inverse(sb, send):
        o = dot(xi[...], tt_ref[...])
        for h in range(CHUNKS):
            for g in range(8):
                low = o[h * HC : (h + 1) * HC, g * 128 : (g + 1) * 128]
                high = o[CH + h * HC : CH + (h + 1) * HC, g * 128 : (g + 1) * 128]
                sb[2 * g, h * HC : (h + 1) * HC, :] = halves(low, roll(high, 64)).astype(BF16)
                sb[2 * g + 1, h * HC : (h + 1) * HC, :] = halves(roll(low, 64), high).astype(BF16)
            send(h)

    def mix(lhs, src, dst, scale):
        @pl.loop(0, 4)
        def _(x):
            for g in range(8):
                rhs = jnp.concatenate(
                    [src[x, g, :4].reshape(256, 128), src[x, g, 4:].reshape(256, 128)], axis=1
                )
                o = dot(lhs, rhs)
                o = (o if scale is None else o * scale).astype(dst.dtype)
                dst[x, g, :4] = o[:, :128].reshape(4, CH, 128)
                dst[x, g, 4:] = o[:, 128:].reshape(4, CH, 128)

    loads[4].wait()
    for h in range(CHUNKS):
        loads[h].wait()
        z_forward(
            [
                f_ref[:, :, p, h * HC : (h + 1) * HC, :].reshape(32 * HC, 128)
                for p in range(8)
            ]
        )
        if h == 0:
            loads[5].wait()
        y_forward(s0, h)
        if h == 0:
            loads[6].wait()
            pl.semaphore_wait(barrier, 30)
        send_pencil(h, s0, r0, h)
        if h == 0:
            for i in range(6):
                moves[i].start()
        keep_pencil(s0, r0, h)

    loads[7].wait()
    lane64 = lax.broadcasted_iota(jnp.int32, (64, 128), 1)
    wl = wl_ref[...].astype(F32)
    wide = jnp.concatenate([wl] * 4, axis=1)
    tall = jnp.concatenate([wide] * 4, axis=0)
    row = lax.broadcasted_iota(jnp.int32, (256, 256), 0) // 64
    col = lax.broadcasted_iota(jnp.int32, (256, 256), 1) // 64
    block = jnp.where(row == col, tall, 0.0)
    bw[0] = block.T.astype(BF16)
    bw[1] = block.astype(BF16)
    mix(bw[0], f_ref, big, math.sqrt(0.5))

    arrived(0)
    arrived(1)
    for i in range(6, 10):
        moves[i].start()
    for h in range(CHUNKS):
        wait_pencil(rsem.at[h], r0, h)
        x_forward(r0, h)
    modes_out(us, False)
    ask_u = swap(0, us.at[1 - me_y], row_u)
    ask_u.start()
    arrived(2)
    arrived(3)
    moves[10].start()
    moves[11].start()
    arrived(6)
    arrived(7)
    moves[12].start()
    moves[13].start()
    loads[9].wait()
    loads[10].wait()
    loads[8].wait()

    row16 = lax.broadcasted_iota(jnp.int32, (16, 128), 0)
    lane16 = lax.broadcasted_iota(jnp.int32, (16, 128), 1)
    block16 = [(row16 % KH) == (2 * t + lane16 // 64) for t in range(4)]
    sign8 = jnp.where(lax.broadcasted_iota(jnp.int32, (8, 128), 1) < 64, -1.0, 1.0)
    first8 = lax.broadcasted_iota(jnp.int32, (8, 128), 0) == 0
    root = math.sqrt(0.5)

    def forward_mode(u, r):
        u = u.astype(F32)
        turned = roll(u, 64)
        v = []
        for kh in range(2):
            twice = halves(u, turned) if kh == 0 else halves(turned, u)
            lhs = jnp.concatenate([jnp.where(m, twice, 0.0) for m in block16], axis=1)
            o = dot(lhs.astype(BF16), wall[r, kh * KH : (kh + 1) * KH].reshape(512, 128))
            o = o[:8] + sign8 * roll(o[8:], 64)
            scale = jnp.where(first8, root * SCALE, 2.0 * root * SCALE) if kh == 0 else 2.0 * root * SCALE
            v.append(o * scale)
        return jnp.concatenate(
            [halves(v[0], roll(v[1], 64)), halves(roll(v[0], 64), v[1])], axis=0
        ).astype(BF16)

    def adjoint_mode(g, r):
        g = g.astype(F32)
        re, im = g[:8], g[8:]
        re_t, im_t = roll(re, 64), roll(im, 64)
        d = []
        for kh in range(2):
            if kh == 0:
                lhs = [halves(re, im_t), halves(im, -re_t)]
            else:
                lhs = [halves(re_t, im), halves(im_t, -re)]
            lhs = jnp.concatenate(lhs, axis=0).astype(BF16)
            o = dot_t(lhs, wall[r, kh * KH : (kh + 1) * KH].reshape(512, 128))
            o = sum(jnp.where(block16[t], o[:, t * 128 : (t + 1) * 128], 0.0) for t in range(4))
            d.append(o + roll(o, 64))
        return halves(d[0], d[1]).astype(BF16)

    def local_modes(mode, src, dst, pieces):
        for r in pieces:
            dst[me_y, r] = mode(src[me_y, r], r)

    def row_modes(mode, src, dst):
        for r in range(8):
            dst[r] = mode(src[r], r)

    local_modes(forward_mode, us, row_v, (own, up, down, far))
    for i in (4, 5, 8, 9, 10, 11, 12, 13):
        arrived(i)
    local_modes(forward_mode, us, row_v, [piece(x, sib) for x in (me_x, x_up, x_down, x_far)])
    ask_u.wait_recv()
    row_modes(forward_mode, row_u, back_v)
    give_v = swap(1, back_v, row_v.at[me_y])
    give_v.start()
    send_dp(16, us, ur)
    give_v.wait_recv()
    modes_in(row_v)
    x_inverse(s1, lambda h: send_pencil(4 + h, s1, r1, h))
    for h in range(CHUNKS):
        keep_pencil(s1, r1, h)

    @pl.loop(0, CHUNKS)
    def _(h):
        wait_pencil(rsem.at[4 + h], r1, h)
        y_inverse(r1, pl.multiple_of(h * HC, HC), HC, ly)
        vy[...] = dot(ly[...], tt_ref[...]).astype(BF16)
        lhs = jnp.concatenate(
            [
                jnp.concatenate(
                    [
                        vy[(kh * 4 + x) * HC : (kh * 4 + x + 1) * HC, g * 128 : (g + 1) * 128]
                        for kh in range(2)
                    ],
                    axis=1,
                )
                for x in range(4)
                for g in range(8)
            ],
            axis=0,
        )
        parts = []
        for n in range(4):
            v = dot(lhs, zt_ref[:, n * 256 : (n + 1) * 256])
            for i in range(2):
                at = (every, every, 2 * n + i, rows_of(h))
                t = v[:, i * 128 : (i + 1) * 128].reshape(4, 8, HC, 128) + big[at]
                sl = (c_ref[at].astype(F32) * gelu_slope(t)).astype(BF16)
                slope[at] = sl
                parts.append(sl.reshape(32 * HC, 128))
        z_forward(parts)
        y_forward(s2, h)
        send_pencil(8 + h, s2, r2, h)
        keep_pencil(s2, r2, h)

    mix(bw[1], slope, sp, None)

    for h in range(CHUNKS):
        wait_pencil(rsem.at[8 + h], r2, h)
        x_forward(r2, h)
    modes_out(gs, True)
    ask_g = swap(2, gs.at[1 - me_y], row_g)
    ask_g.start()
    local_modes(adjoint_mode, gs, row_d, range(8))
    ask_g.wait_recv()
    row_modes(adjoint_mode, row_g, back_d)
    give_d = swap(3, back_d, row_d.at[me_y])
    give_d.start()
    send_dp(17, gs, gr)
    give_d.wait_recv()
    modes_in(row_d)
    x_inverse(s3, lambda h: send_pencil(12 + h, s3, r3, h))
    r3[me_p] = s3[me_p]

    def regroup(src, i):
        xf[...] = src[...].astype(F32).reshape(256, 128)
        for k in range(KH):
            re = xf[pl.ds(k, 16, stride=16), :]
            im = xf[pl.ds(KH + k, 16, stride=16), :]
            ukeep[i, k] = halves(re, roll(im, 64)).astype(BF16)
            ukeep[i, KH + k] = halves(roll(re, 64), im).astype(BF16)

    wait_dp(rsem.at[16], ur)
    regroup(ur, 0)
    wait_dp(rsem.at[17], gr)
    regroup(gr, 1)
    for k in range(MZ):
        cross = lax.dot_general(
            ukeep[0, k], ukeep[1, k], (((0,), (0,)), ((), ())), preferred_element_type=F32
        )
        low = roll(cross[64:], 64)
        gw_v[k] = cross[:64] + jnp.where(lane64 < 64, low, -low)

    for copy in moves + [ask_u, give_v, ask_g, give_d]:
        copy.wait_send()
    for h in range(CHUNKS):
        wait_pencil(ssem.at[h], s0, h)
        wait_pencil(ssem.at[4 + h], s1, h)
        wait_pencil(ssem.at[8 + h], s2, h)
    wait_dp(ssem.at[16], ur)
    wait_dp(ssem.at[17], gr)
    for h in range(CHUNKS):
        wait_pencil(ssem.at[12 + h], s3, h)
        wait_pencil(rsem.at[12 + h], r3, h)


def last_kernel(
    r_ref, sp, gw_v, tt_ref, zt_ref, out_hbm, gw_hbm, ly, vy, out_v, osem,
):
    gw_copy = pltpu.make_async_copy(gw_v, gw_hbm.at[0, 0], osem.at[4])
    gw_copy.start()
    y_inverse(r_ref, 0, CH, ly)
    vy[...] = dot(ly[...], tt_ref[...]).astype(BF16)
    outs = []
    for x in range(4):
        lhs = jnp.concatenate(
            [
                jnp.concatenate(
                    [
                        vy[(kh * 4 + x) * CH : (kh * 4 + x + 1) * CH, g * 128 : (g + 1) * 128]
                        for kh in range(2)
                    ],
                    axis=1,
                )
                for g in range(8)
            ],
            axis=0,
        )
        for n in range(4):
            v = dot(lhs, zt_ref[:, n * 256 : (n + 1) * 256])
            for i in range(2):
                part = v[:, i * 128 : (i + 1) * 128].reshape(8, CH, 128)
                out_v[x, :, 2 * n + i] = (part + sp[x, :, 2 * n + i].astype(F32)).astype(BF16)
        outs.append(pltpu.make_async_copy(out_v.at[x], out_hbm.at[0, x], osem.at[x]))
        outs[x].start()
    for copy in outs:
        copy.wait()
    gw_copy.wait()


def body(field, cotangent, w_spec, w_local):
    table, zf = line_table(), z_table()
    t, tt, zf, zt = (jnp.asarray(m.astype(jnp.bfloat16)) for m in (table, table.T, zf, zf.T))
    grid = (4, 8, 8, CH, NZ)
    any_spec = pl.BlockSpec(memory_space=pltpu.HBM)
    vmem_spec = pl.BlockSpec(memory_space=pltpu.VMEM)
    pencil_buf = pltpu.VMEM((16, CH, 128), BF16)
    dp_buf = pltpu.VMEM((16, 16, 128), BF16)
    both = pltpu.VMEM((2, 8, 16, 128), BF16)
    row = pltpu.VMEM((8, 16, 128), BF16)
    grid_b16 = pltpu.VMEM(grid, BF16)
    line = pltpu.VMEM((1024, 256), BF16)
    line_t = pltpu.VMEM((256, 1024), BF16)
    keep = pltpu.VMEM((2, MZ, 16, 128), BF16)
    r3, sp, gw, tt, zt = pl.pallas_call(
        kernel,
        out_shape=(
            pencil_buf,
            grid_b16,
            pltpu.VMEM((MZ, CH, 2 * CH), F32),
            line_t,
            line_t,
        ),
        in_specs=[any_spec] * 8,
        out_specs=[vmem_spec] * 5,
        scratch_shapes=[
            grid_b16,
            grid_b16,
            pltpu.VMEM((8, MZ, CH, 2 * CH), BF16),
            pltpu.VMEM((CH, CH), BF16),
            line,
            line,
            pltpu.VMEM(grid, F32),
            grid_b16,
            pltpu.VMEM((8 * HC, 1024), BF16),
            pltpu.VMEM((8 * HC, 256), BF16),
            pltpu.VMEM((8 * HC, 1024), BF16),
            pltpu.VMEM((128, 256), F32),
            pltpu.VMEM((128, 256), BF16),
            pltpu.VMEM((2, 256, 256), BF16),
            pltpu.VMEM((256, 128), F32),
            keep,
        ]
        + [pencil_buf] * 7
        + [both, dp_buf, both, dp_buf, row, both, row, row, both, row]
        + [
            pltpu.SemaphoreType.DMA((11,)),
            pltpu.SemaphoreType.DMA((18,)),
            pltpu.SemaphoreType.DMA((18,)),
            pltpu.SemaphoreType.DMA((14,)),
            pltpu.SemaphoreType.DMA((14,)),
            pltpu.SemaphoreType.DMA((4,)),
            pltpu.SemaphoreType.DMA((4,)),
        ],
        compiler_params=pltpu.CompilerParams(
            collective_id=0, has_side_effects=True, vmem_limit_bytes=60_900_000
        ),
        name="layer",
    )(field.reshape((1,) + grid), cotangent.reshape((1,) + grid), w_spec, w_local, t, tt, zf, zt)
    out, gw = pl.pallas_call(
        last_kernel,
        out_shape=(
            jax.ShapeDtypeStruct((1,) + grid, BF16),
            jax.ShapeDtypeStruct((1, 1, MZ, CH, 2 * CH), F32),
        ),
        in_specs=[vmem_spec] * 5,
        out_specs=[any_spec] * 2,
        scratch_shapes=[
            pltpu.VMEM((8 * CH, 256), BF16),
            pltpu.VMEM((8 * CH, 1024), BF16),
            grid_b16,
            pltpu.SemaphoreType.DMA((5,)),
        ],
        compiler_params=pltpu.CompilerParams(vmem_limit_bytes=20 * 1024 * 1024),
        name="last",
    )(r3, sp, gw, tt, zt)
    return (out.reshape(1, 4, NY, CH, NZ), gw)


def solution(mesh):
    placed = P("dp", "pencil", None, None, None)
    return jax.shard_map(
        body,
        mesh=mesh,
        in_specs=(placed, placed, placed, P()),
        out_specs=(placed, placed),
        check_vma=False,
    )
```

```python
import functools
import math

import jax
import jax.numpy as jnp
import numpy as np
from jax import lax
from jax.experimental import pallas as pl
from jax.experimental.pallas import tpu as pltpu
from jax.sharding import PartitionSpec as P

NX = 64
NY = 64
NZ = 128
CH = 64
MX = 16
MY = 16
MZ = 16
KH = 8
MESH = pl.DeviceIdType.MESH
F32 = jnp.float32
BF16 = jnp.bfloat16
CHUNKS = 4
HC = CH // CHUNKS
SCALE = 1.0 / (NX * NY * NZ)


def line_table():
    position = np.arange(NX)
    freq = np.arange(MX)
    freq = np.where(freq < MX // 2, freq, freq - MX)
    angle = 2.0 * math.pi * np.mod(position[:, None] * freq[None, :], NX) / NX
    cos, sin = np.cos(angle).reshape(8, 2, 4, MX), np.sin(angle).reshape(8, 2, 4, MX)
    table = np.zeros((8, 2, 2, 4, KH, 2, MX, KH), np.float32)
    for k in range(KH):
        table[:, :, 0, :, k, 0, :, k] = cos
        table[:, :, 1, :, k, 0, :, k] = sin
        table[:, :, 1, :, k, 1, :, k] = cos
        table[:, :, 0, :, k, 1, :, k] = -sin
    return table.reshape(1024, 256)


def z_table():
    angle = 2.0 * math.pi * np.mod(np.arange(NZ)[:, None] * np.arange(MZ)[None, :], NZ) / NZ
    angle = angle.reshape(NZ, 2, KH)
    table = np.zeros((2, 4, NZ, 2, 2, 2, 4, KH), np.float32)
    for half in range(2):
        for q in range(4):
            table[half, q, :, :, half, 0, q, :] = np.cos(angle)
            table[half, q, :, :, half, 1, q, :] = -np.sin(angle)
    return table.reshape(1024, 256)


def dot(a, b):
    return jnp.dot(a, b, preferred_element_type=F32)


def dot_t(a, b):
    return lax.dot_general(a, b, (((1,), (1,)), ((), ())), preferred_element_type=F32)


def gelu_slope_twice(t):
    bell = jnp.exp2(t * t * (-1.0 / math.log(2.0)) + math.log2(2.0 / math.sqrt(math.pi)))
    return lax.erf(t) + (t * bell + 1.0)


def roll(v, amount):
    amount %= 128
    return v if amount == 0 else pltpu.roll(v, amount, 1)


def halves(low, high):
    lane = lax.broadcasted_iota(jnp.int32, low.shape, 1)
    return jnp.where(lane < 64, low, high)


def slot_masks(rows):
    slot = lax.broadcasted_iota(jnp.int32, (rows, 128), 1) // KH
    return [slot == m for m in range(16)]


def turn_slots(masks, get, put):
    rolled = [roll(get(j), KH * j) for j in range(16)]
    for e in range(16):
        out = rolled[(0 - e) % 16]
        for m in range(1, 16):
            out = jnp.where(masks[m], rolled[(m - e) % 16], out)
        put(e, roll(out, -KH * e))


def y_inverse(rb, c0, rows, ly):
    masks = slot_masks(rows)

    def put(e, tile):
        kh, ri, x = e // 8, (e // 4) % 2, e % 4
        at = (kh * 4 + x) * rows
        ly[at : at + rows, ri * 128 : (ri + 1) * 128] = tile.astype(BF16)

    turn_slots(masks, lambda j: rb[j, pl.ds(c0, rows), :].astype(F32), put)


def kernel(
    field_hbm, cot_hbm, w_hbm, wl_hbm, t_hbm, tt_hbm, zf_hbm, zt_hbm,
    r3, sp, gw_v, tt_ref, zt_ref,
    f_ref, c_ref, wall, wl_ref, t_ref, zf_ref, big, slope,
    a2, ly, vy, xo, xi, bw, xf, ukeep,
    s0, r0, s1, r1, s2, r2, s3,
    us, ur, gs, gr, row_u, row_v, back_v, row_g, row_d, back_d,
    lsem, ssem, rsem, wssem, wrsem, yssem, yrsem,
):
    me_d = lax.axis_index("dp")
    me_p = lax.axis_index("pencil")
    me_x, me_y, me_c = me_d // 4, lax.rem(me_d // 2, 2), lax.rem(me_d, 2)
    x_up, x_down, x_far = lax.rem(me_x + 1, 4), lax.rem(me_x + 3, 4), lax.rem(me_x + 2, 4)
    partner = me_d + 2 - 4 * me_y

    def load(src, dst, i):
        return pltpu.make_async_copy(src, dst, lsem.at[i])

    def rows_of(h):
        return pl.ds(pl.multiple_of(h * HC, HC), HC)

    every = slice(None)
    loads = [
        load(
            field_hbm.at[0, every, every, every, rows_of(h)],
            f_ref.at[every, every, every, rows_of(h)],
            h,
        )
        for h in range(CHUNKS)
    ]
    loads += [
        load(zf_hbm, zf_ref, 4),
        load(t_hbm, t_ref, 5),
        load(w_hbm.at[0, 0], wall.at[2 * me_x + me_c], 6),
        load(wl_hbm, wl_ref, 7),
        load(cot_hbm.at[0], c_ref, 8),
        load(tt_hbm, tt_ref, 9),
        load(zt_hbm, zt_ref, 10),
    ]
    for i in (4, 0, 5, 6, 1, 2, 3, 7, 9, 10, 8):
        loads[i].start()

    barrier = pltpu.get_barrier_semaphore()

    @pl.loop(1, 16)
    def _(d):
        pl.semaphore_signal(
            barrier, inc=1, device_id=(me_d, lax.rem(me_p + d, 16)), device_id_type=MESH
        )
        pl.semaphore_signal(
            barrier, inc=1, device_id=(lax.rem(me_d + d, 16), me_p), device_id_type=MESH
        )

    def send_pencil(e, sb, rb, h):
        for d in (8, 7, 9, 6, 10, 5, 11, 4, 12, 3, 13, 2, 14, 1, 15):
            to = lax.rem(me_p + d, 16)
            pltpu.make_async_remote_copy(
                src_ref=sb.at[to, rows_of(h)],
                dst_ref=rb.at[me_p, rows_of(h)],
                send_sem=ssem.at[e],
                recv_sem=rsem.at[e],
                device_id=(me_d, to),
                device_id_type=MESH,
            ).start()

    def keep_pencil(sb, rb, h):
        rb[me_p, rows_of(h)] = sb[me_p, rows_of(h)]

    def place(d):
        return lax.rem(d // 2, 2), 2 * (d // 4) + lax.rem(d, 2)

    def send_dp(e, sb, rb):
        @pl.loop(1, 16)
        def _(d):
            to = lax.rem(me_d + d, 16)
            pltpu.make_async_remote_copy(
                src_ref=sb.at[place(to)],
                dst_ref=rb.at[me_d],
                send_sem=ssem.at[e],
                recv_sem=rsem.at[e],
                device_id=(to, me_p),
                device_id_type=MESH,
            ).start()

        rb[me_d] = sb[place(me_d)]

    def swap(i, src, dst):
        return pltpu.make_async_remote_copy(
            src_ref=src,
            dst_ref=dst,
            send_sem=yssem.at[i],
            recv_sem=yrsem.at[i],
            device_id=(partner, me_p),
            device_id_type=MESH,
        )

    def piece(x, c):
        return 2 * x + c

    def part(r, half):
        return wall.at[r, pl.ds(half * KH, KH)]

    def weights(i, r, half, x, c):
        return pltpu.make_async_remote_copy(
            src_ref=part(r, half),
            dst_ref=part(r, half),
            send_sem=wssem.at[i],
            recv_sem=wrsem.at[i],
            device_id=(4 * x + 2 * me_y + c, me_p),
            device_id_type=MESH,
        )

    sib = 1 - me_c
    own, up, down, far = (piece(x, me_c) for x in (me_x, x_up, x_down, x_far))
    moves = [
        weights(0, own, 0, x_up, me_c),
        weights(1, own, 1, x_down, me_c),
        weights(2, own, 1, x_up, me_c),
        weights(3, own, 0, x_down, me_c),
        weights(4, own, 0, me_x, sib),
        weights(5, own, 1, me_x, sib),
        weights(6, down, 0, x_up, me_c),
        weights(7, up, 1, x_down, me_c),
        weights(8, down, 0, me_x, sib),
        weights(9, up, 1, me_x, sib),
        weights(10, down, 1, me_x, sib),
        weights(11, up, 0, me_x, sib),
        weights(12, far, 0, me_x, sib),
        weights(13, far, 1, me_x, sib),
    ]

    def arrived(i):
        moves[i].wait_recv()

    def wait_pencil(sem, buf, h):
        part = buf.at[pl.ds(0, 15), rows_of(h)]
        pltpu.make_async_copy(part, part, sem).wait()

    def wait_dp(sem, buf):
        part = buf.at[pl.ds(0, 15)]
        pltpu.make_async_copy(part, part, sem).wait()

    def z_forward(parts):
        a = dot(jnp.concatenate(parts, axis=1), zf_ref[...]).astype(BF16)
        for x in range(4):
            for g in range(8):
                for kh in range(2):
                    a2[(kh * 4 + x) * HC : (kh * 4 + x + 1) * HC, g * 128 : (g + 1) * 128] = a[
                        (x * 8 + g) * HC : (x * 8 + g + 1) * HC, kh * 128 : (kh + 1) * 128
                    ]

    def y_forward(sb, h):
        y = dot(a2[...], t_ref[...])

        def get(e):
            kh, ri, x = e // 8, (e // 4) % 2, e % 4
            at = (kh * 4 + x) * HC
            return y[at : at + HC, ri * 128 : (ri + 1) * 128]

        def put(j, tile):
            sb[j, rows_of(h), :] = tile.astype(BF16)

        turn_slots(slot_masks(HC), get, put)

    def x_forward(rb, h):
        low, high = [], []
        for g in range(8):
            a = rb[2 * g, h * HC : (h + 1) * HC, :].astype(F32)
            b = roll(rb[2 * g + 1, h * HC : (h + 1) * HC, :].astype(F32), 64)
            low.append(halves(a, b).astype(BF16))
            high.append(roll(halves(b, a), 64).astype(BF16))
        lhs = jnp.concatenate(
            [jnp.concatenate(low, axis=1), jnp.concatenate(high, axis=1)], axis=0
        )
        o = dot(lhs, t_ref[...])
        for kh in range(2):
            xo[kh * CH + h * HC : kh * CH + (h + 1) * HC, :] = o[kh * HC : (kh + 1) * HC]

    def modes_out(dst, scaled):
        turned = xo[...].T
        if scaled:
            row = lax.broadcasted_iota(jnp.int32, (256, 128), 0)
            lane = lax.broadcasted_iota(jnp.int32, (256, 128), 1)
            zero = ((row % KH) == 0) & (lane < 64)
            turned = turned * jnp.where(zero, 0.5 * SCALE, SCALE)
        for j in range(16):
            dst[(j // 2) % 2, 2 * (j // 4) + j % 2] = jnp.concatenate(
                [turned[j * 8 : j * 8 + 8], turned[128 + j * 8 : 136 + j * 8]], axis=0
            ).astype(BF16)

    def modes_in(src):
        v = [src[(j // 2) % 2, 2 * (j // 4) + j % 2].astype(F32) for j in range(16)]
        both = jnp.concatenate([t[:8] for t in v] + [t[8:] for t in v], axis=0)
        xi[...] = both.T.astype(BF16)

    def x_inverse(sb, send):
        o = dot(xi[...], tt_ref[...])
        for h in range(CHUNKS):
            for g in range(8):
                low = o[h * HC : (h + 1) * HC, g * 128 : (g + 1) * 128]
                high = o[CH + h * HC : CH + (h + 1) * HC, g * 128 : (g + 1) * 128]
                sb[2 * g, h * HC : (h + 1) * HC, :] = halves(low, roll(high, 64)).astype(BF16)
                sb[2 * g + 1, h * HC : (h + 1) * HC, :] = halves(roll(low, 64), high).astype(BF16)
            send(h)

    def mix(lhs, src, dst, scale, first, last):
        @pl.loop(first, last)
        def _(x):
            for g in range(8):
                rhs = jnp.concatenate(
                    [src[x, g, :4].reshape(256, 128), src[x, g, 4:].reshape(256, 128)], axis=1
                )
                o = dot(lhs, rhs)
                o = (o if scale is None else o * scale).astype(dst.dtype)
                dst[x, g, :4] = o[:, :128].reshape(4, CH, 128)
                dst[x, g, 4:] = o[:, 128:].reshape(4, CH, 128)

    loads[4].wait()
    for h in range(CHUNKS):
        loads[h].wait()
        z_forward(
            [
                f_ref[:, :, p, h * HC : (h + 1) * HC, :].reshape(32 * HC, 128)
                for p in range(8)
            ]
        )
        if h == 0:
            loads[5].wait()
        y_forward(s0, h)
        if h == 0:
            loads[6].wait()
            pl.semaphore_wait(barrier, 30)
        send_pencil(h, s0, r0, h)
        if h == 0:
            for i in range(6):
                moves[i].start()
        keep_pencil(s0, r0, h)

    loads[7].wait()
    lane64 = lax.broadcasted_iota(jnp.int32, (64, 128), 1)
    wl = wl_ref[...].astype(F32)
    wide = jnp.concatenate([wl] * 4, axis=1)
    tall = jnp.concatenate([wide] * 4, axis=0)
    row = lax.broadcasted_iota(jnp.int32, (256, 256), 0) // 64
    col = lax.broadcasted_iota(jnp.int32, (256, 256), 1) // 64
    block = jnp.where(row == col, tall, 0.0)
    bw[0] = block.T.astype(BF16)
    bw[1] = (0.5 * block).astype(BF16)
    mix(bw[0], f_ref, big, math.sqrt(0.5), 0, 2)
    arrived(0)
    arrived(1)
    for i in range(6, 10):
        moves[i].start()
    mix(bw[0], f_ref, big, math.sqrt(0.5), 2, 4)

    for h in range(CHUNKS):
        wait_pencil(rsem.at[h], r0, h)
        x_forward(r0, h)
    modes_out(us, False)
    ask_u = swap(0, us.at[1 - me_y], row_u)
    ask_u.start()
    arrived(2)
    arrived(3)
    moves[10].start()
    moves[11].start()
    arrived(6)
    arrived(7)
    moves[12].start()
    moves[13].start()
    loads[9].wait()
    loads[10].wait()
    loads[8].wait()

    row16 = lax.broadcasted_iota(jnp.int32, (16, 128), 0)
    lane16 = lax.broadcasted_iota(jnp.int32, (16, 128), 1)
    block16 = [(row16 % KH) == (2 * t + lane16 // 64) for t in range(4)]
    sign8 = jnp.where(lax.broadcasted_iota(jnp.int32, (8, 128), 1) < 64, -1.0, 1.0)
    first8 = lax.broadcasted_iota(jnp.int32, (8, 128), 0) == 0
    root = math.sqrt(0.5)

    def forward_mode(u, r):
        u = u.astype(F32)
        turned = roll(u, 64)
        v = []
        for kh in range(2):
            twice = halves(u, turned) if kh == 0 else halves(turned, u)
            lhs = jnp.concatenate([jnp.where(m, twice, 0.0) for m in block16], axis=1)
            o = dot(lhs.astype(BF16), wall[r, kh * KH : (kh + 1) * KH].reshape(512, 128))
            o = o[:8] + sign8 * roll(o[8:], 64)
            scale = jnp.where(first8, root * SCALE, 2.0 * root * SCALE) if kh == 0 else 2.0 * root * SCALE
            v.append(o * scale)
        return jnp.concatenate(
            [halves(v[0], roll(v[1], 64)), halves(roll(v[0], 64), v[1])], axis=0
        ).astype(BF16)

    def adjoint_mode(g, r):
        g = g.astype(F32)
        re, im = g[:8], g[8:]
        re_t, im_t = roll(re, 64), roll(im, 64)
        d = []
        for kh in range(2):
            if kh == 0:
                lhs = [halves(re, im_t), halves(im, -re_t)]
            else:
                lhs = [halves(re_t, im), halves(im_t, -re)]
            lhs = jnp.concatenate(lhs, axis=0).astype(BF16)
            o = dot_t(lhs, wall[r, kh * KH : (kh + 1) * KH].reshape(512, 128))
            o = sum(jnp.where(block16[t], o[:, t * 128 : (t + 1) * 128], 0.0) for t in range(4))
            d.append(o + roll(o, 64))
        return halves(d[0], d[1]).astype(BF16)

    def local_modes(mode, src, dst, pieces):
        for r in pieces:
            dst[me_y, r] = mode(src[me_y, r], r)

    def row_modes(mode, src, dst):
        for r in range(8):
            dst[r] = mode(src[r], r)

    local_modes(forward_mode, us, row_v, (own, up, down, far))
    for i in (4, 5, 8, 9, 10, 11, 12, 13):
        arrived(i)
    ask_u.wait_recv()
    row_modes(forward_mode, row_u, back_v)
    give_v = swap(1, back_v, row_v.at[me_y])
    give_v.start()
    local_modes(forward_mode, us, row_v, [piece(x, sib) for x in (me_x, x_up, x_down, x_far)])
    send_dp(16, us, ur)
    give_v.wait_recv()
    modes_in(row_v)
    x_inverse(s1, lambda h: send_pencil(4 + h, s1, r1, h))
    for h in range(CHUNKS):
        keep_pencil(s1, r1, h)

    @pl.loop(0, CHUNKS)
    def _(h):
        wait_pencil(rsem.at[4 + h], r1, h)
        y_inverse(r1, pl.multiple_of(h * HC, HC), HC, ly)
        vy[...] = dot(ly[...], tt_ref[...]).astype(BF16)
        lhs = jnp.concatenate(
            [
                jnp.concatenate(
                    [
                        vy[(kh * 4 + x) * HC : (kh * 4 + x + 1) * HC, g * 128 : (g + 1) * 128]
                        for kh in range(2)
                    ],
                    axis=1,
                )
                for x in range(4)
                for g in range(8)
            ],
            axis=0,
        )
        parts = []
        for n in range(4):
            v = dot(lhs, zt_ref[:, n * 256 : (n + 1) * 256])
            for i in range(2):
                at = (every, every, 2 * n + i, rows_of(h))
                t = v[:, i * 128 : (i + 1) * 128].reshape(4, 8, HC, 128) + big[at]
                sl = (c_ref[at].astype(F32) * gelu_slope_twice(t)).astype(BF16)
                slope[at] = sl
                parts.append(sl.reshape(32 * HC, 128))
        z_forward(parts)
        y_forward(s2, h)
        send_pencil(8 + h, s2, r2, h)
        keep_pencil(s2, r2, h)

    mix(bw[1], slope, sp, None, 0, 4)

    for h in range(CHUNKS):
        wait_pencil(rsem.at[8 + h], r2, h)
        x_forward(r2, h)
    modes_out(gs, True)
    ask_g = swap(2, gs.at[1 - me_y], row_g)
    ask_g.start()
    local_modes(adjoint_mode, gs, row_d, range(8))
    ask_g.wait_recv()
    row_modes(adjoint_mode, row_g, back_d)
    give_d = swap(3, back_d, row_d.at[me_y])
    give_d.start()
    send_dp(17, gs, gr)
    give_d.wait_recv()
    modes_in(row_d)
    x_inverse(s3, lambda h: send_pencil(12 + h, s3, r3, h))
    r3[me_p] = s3[me_p]

    def regroup(src, i):
        xf[...] = src[...].astype(F32).reshape(256, 128)
        for k in range(KH):
            re = xf[pl.ds(k, 16, stride=16), :]
            im = xf[pl.ds(KH + k, 16, stride=16), :]
            ukeep[i, k] = halves(re, roll(im, 64)).astype(BF16)
            ukeep[i, KH + k] = halves(roll(re, 64), im).astype(BF16)

    wait_dp(rsem.at[16], ur)
    regroup(ur, 0)
    wait_dp(rsem.at[17], gr)
    regroup(gr, 1)
    for k in range(MZ):
        cross = lax.dot_general(
            ukeep[0, k], ukeep[1, k], (((0,), (0,)), ((), ())), preferred_element_type=F32
        )
        low = roll(cross[64:], 64)
        gw_v[k] = cross[:64] + jnp.where(lane64 < 64, low, -low)

    for copy in moves + [ask_u, give_v, ask_g, give_d]:
        copy.wait_send()
    for h in range(CHUNKS):
        wait_pencil(ssem.at[h], s0, h)
        wait_pencil(ssem.at[4 + h], s1, h)
        wait_pencil(ssem.at[8 + h], s2, h)
    wait_dp(ssem.at[16], ur)
    wait_dp(ssem.at[17], gr)
    for h in range(CHUNKS):
        wait_pencil(ssem.at[12 + h], s3, h)
        wait_pencil(rsem.at[12 + h], r3, h)


def last_kernel(
    r_ref, sp, gw_v, tt_ref, zt_ref, out_hbm, gw_hbm, ly, vy, out_v, osem,
):
    gw_copy = pltpu.make_async_copy(gw_v, gw_hbm.at[0, 0], osem.at[4])
    gw_copy.start()
    y_inverse(r_ref, 0, CH, ly)
    vy[...] = dot(ly[...], tt_ref[...]).astype(BF16)
    outs = []
    for x in range(4):
        lhs = jnp.concatenate(
            [
                jnp.concatenate(
                    [
                        vy[(kh * 4 + x) * CH : (kh * 4 + x + 1) * CH, g * 128 : (g + 1) * 128]
                        for kh in range(2)
                    ],
                    axis=1,
                )
                for g in range(8)
            ],
            axis=0,
        )
        for n in range(4):
            v = dot(lhs, zt_ref[:, n * 256 : (n + 1) * 256])
            for i in range(2):
                part = v[:, i * 128 : (i + 1) * 128].reshape(8, CH, 128)
                out_v[x, :, 2 * n + i] = (part + sp[x, :, 2 * n + i].astype(F32)).astype(BF16)
        outs.append(pltpu.make_async_copy(out_v.at[x], out_hbm.at[0, x], osem.at[x]))
        outs[x].start()
    for copy in outs:
        copy.wait()
    gw_copy.wait()


def body(field, cotangent, w_spec, w_local):
    table, zf = line_table(), z_table()
    t, tt, zf, zt = (jnp.asarray(m.astype(jnp.bfloat16)) for m in (table, table.T, zf, zf.T))
    grid = (4, 8, 8, CH, NZ)
    any_spec = pl.BlockSpec(memory_space=pltpu.HBM)
    vmem_spec = pl.BlockSpec(memory_space=pltpu.VMEM)
    pencil_buf = pltpu.VMEM((16, CH, 128), BF16)
    dp_buf = pltpu.VMEM((16, 16, 128), BF16)
    both = pltpu.VMEM((2, 8, 16, 128), BF16)
    row = pltpu.VMEM((8, 16, 128), BF16)
    grid_b16 = pltpu.VMEM(grid, BF16)
    line = pltpu.VMEM((1024, 256), BF16)
    line_t = pltpu.VMEM((256, 1024), BF16)
    keep = pltpu.VMEM((2, MZ, 16, 128), BF16)
    r3, sp, gw, tt, zt = pl.pallas_call(
        kernel,
        out_shape=(
            pencil_buf,
            grid_b16,
            pltpu.VMEM((MZ, CH, 2 * CH), F32),
            line_t,
            line_t,
        ),
        in_specs=[any_spec] * 8,
        out_specs=[vmem_spec] * 5,
        scratch_shapes=[
            grid_b16,
            grid_b16,
            pltpu.VMEM((8, MZ, CH, 2 * CH), BF16),
            pltpu.VMEM((CH, CH), BF16),
            line,
            line,
            pltpu.VMEM(grid, F32),
            grid_b16,
            pltpu.VMEM((8 * HC, 1024), BF16),
            pltpu.VMEM((8 * HC, 256), BF16),
            pltpu.VMEM((8 * HC, 1024), BF16),
            pltpu.VMEM((128, 256), F32),
            pltpu.VMEM((128, 256), BF16),
            pltpu.VMEM((2, 256, 256), BF16),
            pltpu.VMEM((256, 128), F32),
            keep,
        ]
        + [pencil_buf] * 7
        + [both, dp_buf, both, dp_buf, row, both, row, row, both, row]
        + [
            pltpu.SemaphoreType.DMA((11,)),
            pltpu.SemaphoreType.DMA((18,)),
            pltpu.SemaphoreType.DMA((18,)),
            pltpu.SemaphoreType.DMA((14,)),
            pltpu.SemaphoreType.DMA((14,)),
            pltpu.SemaphoreType.DMA((4,)),
            pltpu.SemaphoreType.DMA((4,)),
        ],
        compiler_params=pltpu.CompilerParams(
            collective_id=0, has_side_effects=True, vmem_limit_bytes=60_900_000
        ),
        name="layer",
    )(field.reshape((1,) + grid), cotangent.reshape((1,) + grid), w_spec, w_local, t, tt, zf, zt)
    out, gw = pl.pallas_call(
        last_kernel,
        out_shape=(
            jax.ShapeDtypeStruct((1,) + grid, BF16),
            jax.ShapeDtypeStruct((1, 1, MZ, CH, 2 * CH), F32),
        ),
        in_specs=[vmem_spec] * 5,
        out_specs=[any_spec] * 2,
        scratch_shapes=[
            pltpu.VMEM((8 * CH, 256), BF16),
            pltpu.VMEM((8 * CH, 1024), BF16),
            grid_b16,
            pltpu.SemaphoreType.DMA((5,)),
        ],
        compiler_params=pltpu.CompilerParams(vmem_limit_bytes=20 * 1024 * 1024),
        name="last",
    )(r3, sp, gw, tt, zt)
    return (out.reshape(1, 4, NY, CH, NZ), gw)


def solution(mesh):
    placed = P("dp", "pencil", None, None, None)
    return jax.shard_map(
        body,
        mesh=mesh,
        in_specs=(placed, placed, placed, P()),
        out_specs=(placed, placed),
        check_vma=False,
    )
```

```python
import functools
import math

import jax
import jax.numpy as jnp
import numpy as np
from jax import lax
from jax.experimental import pallas as pl
from jax.experimental.pallas import tpu as pltpu
from jax.sharding import PartitionSpec as P

NX = 64
NY = 64
NZ = 128
CH = 64
MX = 16
MY = 16
MZ = 16
KH = 8
MESH = pl.DeviceIdType.MESH
F32 = jnp.float32
BF16 = jnp.bfloat16
CHUNKS = 4
HC = CH // CHUNKS
SCALE = 1.0 / (NX * NY * NZ)


def line_table():
    position = np.arange(NX)
    freq = np.arange(MX)
    freq = np.where(freq < MX // 2, freq, freq - MX)
    angle = 2.0 * math.pi * np.mod(position[:, None] * freq[None, :], NX) / NX
    cos, sin = np.cos(angle).reshape(8, 2, 4, MX), np.sin(angle).reshape(8, 2, 4, MX)
    table = np.zeros((8, 2, 2, 4, KH, 2, MX, KH), np.float32)
    for k in range(KH):
        table[:, :, 0, :, k, 0, :, k] = cos
        table[:, :, 1, :, k, 0, :, k] = sin
        table[:, :, 1, :, k, 1, :, k] = cos
        table[:, :, 0, :, k, 1, :, k] = -sin
    return table.reshape(1024, 256)


def z_table():
    angle = 2.0 * math.pi * np.mod(np.arange(NZ)[:, None] * np.arange(MZ)[None, :], NZ) / NZ
    angle = angle.reshape(NZ, 2, KH)
    table = np.zeros((2, 4, NZ, 2, 2, 2, 4, KH), np.float32)
    for half in range(2):
        for q in range(4):
            table[half, q, :, :, half, 0, q, :] = np.cos(angle)
            table[half, q, :, :, half, 1, q, :] = -np.sin(angle)
    return table.reshape(1024, 256)


def dot(a, b):
    return jnp.dot(a, b, preferred_element_type=F32)


def dot_t(a, b):
    return lax.dot_general(a, b, (((1,), (1,)), ((), ())), preferred_element_type=F32)


def gelu_slope_twice(t):
    bell = jnp.exp2(t * t * (-1.0 / math.log(2.0)) + math.log2(2.0 / math.sqrt(math.pi)))
    return lax.erf(t) + (t * bell + 1.0)


def roll(v, amount):
    amount %= 128
    return v if amount == 0 else pltpu.roll(v, amount, 1)


def halves(low, high):
    lane = lax.broadcasted_iota(jnp.int32, low.shape, 1)
    return jnp.where(lane < 64, low, high)


def slot_masks(rows):
    slot = lax.broadcasted_iota(jnp.int32, (rows, 128), 1) // KH
    return [slot == m for m in range(16)]


def turn_slots(masks, get, put):
    rolled = [roll(get(j), KH * j) for j in range(16)]
    for e in range(16):
        out = rolled[(0 - e) % 16]
        for m in range(1, 16):
            out = jnp.where(masks[m], rolled[(m - e) % 16], out)
        put(e, roll(out, -KH * e))


def y_inverse(rb, c0, rows, ly):
    masks = slot_masks(rows)

    def put(e, tile):
        kh, ri, x = e // 8, (e // 4) % 2, e % 4
        at = (kh * 4 + x) * rows
        ly[at : at + rows, ri * 128 : (ri + 1) * 128] = tile.astype(BF16)

    turn_slots(masks, lambda j: rb[j, pl.ds(c0, rows), :].astype(F32), put)


def grid_modes(ly, vy, tt_ref):
    vy[...] = dot(ly[...], tt_ref[...]).astype(BF16)
    return jnp.concatenate(
        [
            jnp.concatenate(
                [
                    vy[(kh * 4 + x) * HC : (kh * 4 + x + 1) * HC, g * 128 : (g + 1) * 128]
                    for kh in range(2)
                ],
                axis=1,
            )
            for x in range(4)
            for g in range(8)
        ],
        axis=0,
    )


def finish(lhs, zt_ref, sp, dst, c_from, c_to):
    for n in range(4):
        v = dot(lhs, zt_ref[:, n * 256 : (n + 1) * 256])
        for i in range(2):
            p = 2 * n + i
            part = v[:, i * 128 : (i + 1) * 128].reshape(4, 8, HC, 128)
            dst[:, :, p, c_to] = (part + sp[:, :, p, c_from].astype(F32)).astype(BF16)


def kernel(
    field_hbm, cot_hbm, w_hbm, wl_hbm, t_hbm, tt_hbm, zf_hbm, zt_hbm,
    r3, sp, gw_v, tt_ref, zt_ref, out_v,
    f_ref, c_ref, wall, wl_ref, t_ref, zf_ref, big, slope,
    a2, ly, vy, xo, xi, bw, xf, ukeep,
    s0, r0, s1, r1, s2, r2, s3,
    us, ur, gs, gr, row_u, row_v, back_v, row_g, row_d, back_d,
    lsem, ssem, rsem, wssem, wrsem, yssem, yrsem,
):
    me_d = lax.axis_index("dp")
    me_p = lax.axis_index("pencil")
    me_x, me_y, me_c = me_d // 4, lax.rem(me_d // 2, 2), lax.rem(me_d, 2)
    x_up, x_down, x_far = lax.rem(me_x + 1, 4), lax.rem(me_x + 3, 4), lax.rem(me_x + 2, 4)
    partner = me_d + 2 - 4 * me_y

    def load(src, dst, i):
        return pltpu.make_async_copy(src, dst, lsem.at[i])

    def rows_of(h):
        return pl.ds(pl.multiple_of(h * HC, HC), HC)

    every = slice(None)
    loads = [
        load(
            field_hbm.at[0, every, every, every, rows_of(h)],
            f_ref.at[every, every, every, rows_of(h)],
            h,
        )
        for h in range(CHUNKS)
    ]
    loads += [
        load(zf_hbm, zf_ref, 4),
        load(t_hbm, t_ref, 5),
        load(w_hbm.at[0, 0], wall.at[2 * me_x + me_c], 6),
        load(wl_hbm, wl_ref, 7),
        load(cot_hbm.at[0], c_ref, 8),
        load(tt_hbm, tt_ref, 9),
        load(zt_hbm, zt_ref, 10),
    ]
    for i in (4, 0, 5, 6, 1, 2, 3, 7, 9, 10, 8):
        loads[i].start()

    barrier = pltpu.get_barrier_semaphore()

    @pl.loop(1, 16)
    def _(d):
        pl.semaphore_signal(
            barrier, inc=1, device_id=(me_d, lax.rem(me_p + d, 16)), device_id_type=MESH
        )
        pl.semaphore_signal(
            barrier, inc=1, device_id=(lax.rem(me_d + d, 16), me_p), device_id_type=MESH
        )

    def send_pencil(e, sb, rb, h):
        for d in (8, 7, 9, 6, 10, 5, 11, 4, 12, 3, 13, 2, 14, 1, 15):
            to = lax.rem(me_p + d, 16)
            pltpu.make_async_remote_copy(
                src_ref=sb.at[to, rows_of(h)],
                dst_ref=rb.at[me_p, rows_of(h)],
                send_sem=ssem.at[e],
                recv_sem=rsem.at[e],
                device_id=(me_d, to),
                device_id_type=MESH,
            ).start()

    def keep_pencil(sb, rb, h):
        rb[me_p, rows_of(h)] = sb[me_p, rows_of(h)]

    def place(d):
        return lax.rem(d // 2, 2), 2 * (d // 4) + lax.rem(d, 2)

    def send_dp(e, sb, rb):
        @pl.loop(1, 16)
        def _(d):
            to = lax.rem(me_d + d, 16)
            pltpu.make_async_remote_copy(
                src_ref=sb.at[place(to)],
                dst_ref=rb.at[me_d],
                send_sem=ssem.at[e],
                recv_sem=rsem.at[e],
                device_id=(to, me_p),
                device_id_type=MESH,
            ).start()

        rb[me_d] = sb[place(me_d)]

    def swap(i, src, dst):
        return pltpu.make_async_remote_copy(
            src_ref=src,
            dst_ref=dst,
            send_sem=yssem.at[i],
            recv_sem=yrsem.at[i],
            device_id=(partner, me_p),
            device_id_type=MESH,
        )

    def piece(x, c):
        return 2 * x + c

    def part(r, half):
        return wall.at[r, pl.ds(half * KH, KH)]

    def weights(i, r, half, x, c):
        return pltpu.make_async_remote_copy(
            src_ref=part(r, half),
            dst_ref=part(r, half),
            send_sem=wssem.at[i],
            recv_sem=wrsem.at[i],
            device_id=(4 * x + 2 * me_y + c, me_p),
            device_id_type=MESH,
        )

    sib = 1 - me_c
    own, up, down, far = (piece(x, me_c) for x in (me_x, x_up, x_down, x_far))
    moves = [
        weights(0, own, 0, x_up, me_c),
        weights(1, own, 1, x_down, me_c),
        weights(2, own, 1, x_up, me_c),
        weights(3, own, 0, x_down, me_c),
        weights(4, own, 0, me_x, sib),
        weights(5, own, 1, me_x, sib),
        weights(6, down, 0, x_up, me_c),
        weights(7, up, 1, x_down, me_c),
        weights(8, down, 0, me_x, sib),
        weights(9, up, 1, me_x, sib),
        weights(10, down, 1, me_x, sib),
        weights(11, up, 0, me_x, sib),
        weights(12, far, 0, me_x, sib),
        weights(13, far, 1, me_x, sib),
    ]

    def arrived(i):
        moves[i].wait_recv()

    def wait_pencil(sem, buf, h):
        part = buf.at[pl.ds(0, 15), rows_of(h)]
        pltpu.make_async_copy(part, part, sem).wait()

    def wait_dp(sem, buf):
        part = buf.at[pl.ds(0, 15)]
        pltpu.make_async_copy(part, part, sem).wait()

    def z_forward(parts):
        a = dot(jnp.concatenate(parts, axis=1), zf_ref[...]).astype(BF16)
        for x in range(4):
            for g in range(8):
                for kh in range(2):
                    a2[(kh * 4 + x) * HC : (kh * 4 + x + 1) * HC, g * 128 : (g + 1) * 128] = a[
                        (x * 8 + g) * HC : (x * 8 + g + 1) * HC, kh * 128 : (kh + 1) * 128
                    ]

    def y_forward(sb, h):
        y = dot(a2[...], t_ref[...])

        def get(e):
            kh, ri, x = e // 8, (e // 4) % 2, e % 4
            at = (kh * 4 + x) * HC
            return y[at : at + HC, ri * 128 : (ri + 1) * 128]

        def put(j, tile):
            sb[j, rows_of(h), :] = tile.astype(BF16)

        turn_slots(slot_masks(HC), get, put)

    def x_forward(rb, h):
        low, high = [], []
        for g in range(8):
            a = rb[2 * g, h * HC : (h + 1) * HC, :].astype(F32)
            b = roll(rb[2 * g + 1, h * HC : (h + 1) * HC, :].astype(F32), 64)
            low.append(halves(a, b).astype(BF16))
            high.append(roll(halves(b, a), 64).astype(BF16))
        lhs = jnp.concatenate(
            [jnp.concatenate(low, axis=1), jnp.concatenate(high, axis=1)], axis=0
        )
        o = dot(lhs, t_ref[...])
        for kh in range(2):
            xo[kh * CH + h * HC : kh * CH + (h + 1) * HC, :] = o[kh * HC : (kh + 1) * HC]

    def modes_out(dst, scaled):
        turned = xo[...].T
        if scaled:
            row = lax.broadcasted_iota(jnp.int32, (256, 128), 0)
            lane = lax.broadcasted_iota(jnp.int32, (256, 128), 1)
            zero = ((row % KH) == 0) & (lane < 64)
            turned = turned * jnp.where(zero, 0.5 * SCALE, SCALE)
        for j in range(16):
            dst[(j // 2) % 2, 2 * (j // 4) + j % 2] = jnp.concatenate(
                [turned[j * 8 : j * 8 + 8], turned[128 + j * 8 : 136 + j * 8]], axis=0
            ).astype(BF16)

    def modes_in(src):
        v = [src[(j // 2) % 2, 2 * (j // 4) + j % 2].astype(F32) for j in range(16)]
        both = jnp.concatenate([t[:8] for t in v] + [t[8:] for t in v], axis=0)
        xi[...] = both.T.astype(BF16)

    def x_inverse(sb, send):
        o = dot(xi[...], tt_ref[...])
        for h in range(CHUNKS):
            for g in range(8):
                low = o[h * HC : (h + 1) * HC, g * 128 : (g + 1) * 128]
                high = o[CH + h * HC : CH + (h + 1) * HC, g * 128 : (g + 1) * 128]
                sb[2 * g, h * HC : (h + 1) * HC, :] = halves(low, roll(high, 64)).astype(BF16)
                sb[2 * g + 1, h * HC : (h + 1) * HC, :] = halves(roll(low, 64), high).astype(BF16)
            send(h)

    def mix(lhs, src, dst, scale, first, last):
        @pl.loop(first, last)
        def _(x):
            for g in range(8):
                rhs = jnp.concatenate(
                    [src[x, g, :4].reshape(256, 128), src[x, g, 4:].reshape(256, 128)], axis=1
                )
                o = dot(lhs, rhs)
                o = (o if scale is None else o * scale).astype(dst.dtype)
                dst[x, g, :4] = o[:, :128].reshape(4, CH, 128)
                dst[x, g, 4:] = o[:, 128:].reshape(4, CH, 128)

    loads[4].wait()
    for h in range(CHUNKS):
        loads[h].wait()
        z_forward(
            [
                f_ref[:, :, p, h * HC : (h + 1) * HC, :].reshape(32 * HC, 128)
                for p in range(8)
            ]
        )
        if h == 0:
            loads[5].wait()
        y_forward(s0, h)
        if h == 0:
            loads[6].wait()
            pl.semaphore_wait(barrier, 30)
        send_pencil(h, s0, r0, h)
        if h == 0:
            for i in range(6):
                moves[i].start()
        keep_pencil(s0, r0, h)

    loads[7].wait()
    lane64 = lax.broadcasted_iota(jnp.int32, (64, 128), 1)
    wl = wl_ref[...].astype(F32)
    wide = jnp.concatenate([wl] * 4, axis=1)
    tall = jnp.concatenate([wide] * 4, axis=0)
    row = lax.broadcasted_iota(jnp.int32, (256, 256), 0) // 64
    col = lax.broadcasted_iota(jnp.int32, (256, 256), 1) // 64
    block = jnp.where(row == col, tall, 0.0)
    bw[0] = block.T.astype(BF16)
    bw[1] = (0.5 * block).astype(BF16)
    mix(bw[0], f_ref, big, math.sqrt(0.5), 0, 2)
    arrived(0)
    arrived(1)
    for i in range(6, 10):
        moves[i].start()
    mix(bw[0], f_ref, big, math.sqrt(0.5), 2, 4)

    for h in range(CHUNKS):
        wait_pencil(rsem.at[h], r0, h)
        x_forward(r0, h)
    modes_out(us, False)
    ask_u = swap(0, us.at[1 - me_y], row_u)
    ask_u.start()
    arrived(2)
    arrived(3)
    moves[10].start()
    moves[11].start()
    arrived(6)
    arrived(7)
    moves[12].start()
    moves[13].start()
    loads[9].wait()
    loads[10].wait()
    loads[8].wait()

    row16 = lax.broadcasted_iota(jnp.int32, (16, 128), 0)
    lane16 = lax.broadcasted_iota(jnp.int32, (16, 128), 1)
    block16 = [(row16 % KH) == (2 * t + lane16 // 64) for t in range(4)]
    sign8 = jnp.where(lax.broadcasted_iota(jnp.int32, (8, 128), 1) < 64, -1.0, 1.0)
    first8 = lax.broadcasted_iota(jnp.int32, (8, 128), 0) == 0
    root = math.sqrt(0.5)

    def forward_mode(u, r):
        u = u.astype(F32)
        turned = roll(u, 64)
        v = []
        for kh in range(2):
            twice = halves(u, turned) if kh == 0 else halves(turned, u)
            lhs = jnp.concatenate([jnp.where(m, twice, 0.0) for m in block16], axis=1)
            o = dot(lhs.astype(BF16), wall[r, kh * KH : (kh + 1) * KH].reshape(512, 128))
            o = o[:8] + sign8 * roll(o[8:], 64)
            scale = jnp.where(first8, root * SCALE, 2.0 * root * SCALE) if kh == 0 else 2.0 * root * SCALE
            v.append(o * scale)
        return jnp.concatenate(
            [halves(v[0], roll(v[1], 64)), halves(roll(v[0], 64), v[1])], axis=0
        ).astype(BF16)

    def adjoint_mode(g, r):
        g = g.astype(F32)
        re, im = g[:8], g[8:]
        re_t, im_t = roll(re, 64), roll(im, 64)
        d = []
        for kh in range(2):
            if kh == 0:
                lhs = [halves(re, im_t), halves(im, -re_t)]
            else:
                lhs = [halves(re_t, im), halves(im_t, -re)]
            lhs = jnp.concatenate(lhs, axis=0).astype(BF16)
            o = dot_t(lhs, wall[r, kh * KH : (kh + 1) * KH].reshape(512, 128))
            o = sum(jnp.where(block16[t], o[:, t * 128 : (t + 1) * 128], 0.0) for t in range(4))
            d.append(o + roll(o, 64))
        return halves(d[0], d[1]).astype(BF16)

    def local_modes(mode, src, dst, pieces):
        for r in pieces:
            dst[me_y, r] = mode(src[me_y, r], r)

    def row_modes(mode, src, dst):
        for r in range(8):
            dst[r] = mode(src[r], r)

    local_modes(forward_mode, us, row_v, (own, up, down, far))
    for i in (4, 5, 8, 9, 10, 11, 12, 13):
        arrived(i)
    ask_u.wait_recv()
    row_modes(forward_mode, row_u, back_v)
    give_v = swap(1, back_v, row_v.at[me_y])
    give_v.start()
    local_modes(forward_mode, us, row_v, [piece(x, sib) for x in (me_x, x_up, x_down, x_far)])
    send_dp(16, us, ur)
    give_v.wait_recv()
    modes_in(row_v)
    x_inverse(s1, lambda h: send_pencil(4 + h, s1, r1, h))
    for h in range(CHUNKS):
        keep_pencil(s1, r1, h)

    @pl.loop(0, CHUNKS)
    def _(h):
        wait_pencil(rsem.at[4 + h], r1, h)
        y_inverse(r1, pl.multiple_of(h * HC, HC), HC, ly)
        lhs = grid_modes(ly, vy, tt_ref)
        parts = []
        for n in range(4):
            v = dot(lhs, zt_ref[:, n * 256 : (n + 1) * 256])
            for i in range(2):
                at = (every, every, 2 * n + i, rows_of(h))
                t = v[:, i * 128 : (i + 1) * 128].reshape(4, 8, HC, 128) + big[at]
                sl = (c_ref[at].astype(F32) * gelu_slope_twice(t)).astype(BF16)
                slope[at] = sl
                parts.append(sl.reshape(32 * HC, 128))
        z_forward(parts)
        y_forward(s2, h)
        send_pencil(8 + h, s2, r2, h)
        keep_pencil(s2, r2, h)

    mix(bw[1], slope, sp, None, 0, 4)

    for h in range(CHUNKS):
        wait_pencil(rsem.at[8 + h], r2, h)
        x_forward(r2, h)
    modes_out(gs, True)
    ask_g = swap(2, gs.at[1 - me_y], row_g)
    ask_g.start()
    local_modes(adjoint_mode, gs, row_d, range(8))
    ask_g.wait_recv()
    row_modes(adjoint_mode, row_g, back_d)
    give_d = swap(3, back_d, row_d.at[me_y])
    give_d.start()
    send_dp(17, gs, gr)
    give_d.wait_recv()
    modes_in(row_d)
    x_inverse(s3, lambda h: send_pencil(12 + h, s3, r3, h))
    r3[me_p] = s3[me_p]

    def regroup(src, i):
        xf[...] = src[...].astype(F32).reshape(256, 128)
        for k in range(KH):
            re = xf[pl.ds(k, 16, stride=16), :]
            im = xf[pl.ds(KH + k, 16, stride=16), :]
            ukeep[i, k] = halves(re, roll(im, 64)).astype(BF16)
            ukeep[i, KH + k] = halves(roll(re, 64), im).astype(BF16)

    wait_dp(rsem.at[16], ur)
    regroup(ur, 0)
    wait_dp(rsem.at[17], gr)
    regroup(gr, 1)
    for k in range(MZ):
        cross = lax.dot_general(
            ukeep[0, k], ukeep[1, k], (((0,), (0,)), ((), ())), preferred_element_type=F32
        )
        low = roll(cross[64:], 64)
        gw_v[k] = cross[:64] + jnp.where(lane64 < 64, low, -low)

    @pl.loop(0, CHUNKS - 1)
    def _(h):
        wait_pencil(rsem.at[12 + h], r3, h)
        y_inverse(r3, pl.multiple_of(h * HC, HC), HC, ly)
        finish(grid_modes(ly, vy, tt_ref), zt_ref, sp, out_v, rows_of(h), rows_of(h))

    for copy in moves + [ask_u, give_v, ask_g, give_d]:
        copy.wait_send()
    for h in range(CHUNKS):
        wait_pencil(ssem.at[h], s0, h)
        wait_pencil(ssem.at[4 + h], s1, h)
        wait_pencil(ssem.at[8 + h], s2, h)
    wait_dp(ssem.at[16], ur)
    wait_dp(ssem.at[17], gr)
    for h in range(CHUNKS):
        wait_pencil(ssem.at[12 + h], s3, h)
    wait_pencil(rsem.at[12 + CHUNKS - 1], r3, CHUNKS - 1)


def last_kernel(
    r_ref, sp, gw_v, tt_ref, zt_ref, done, out_hbm, gw_hbm, ly, vy, out_v, osem,
):
    every, rest = slice(None), CH - HC
    copies = [
        pltpu.make_async_copy(
            done.at[x], out_hbm.at[0, x, every, every, pl.ds(0, rest)], osem.at[x]
        )
        for x in range(4)
    ]
    copies.append(pltpu.make_async_copy(gw_v, gw_hbm.at[0, 0], osem.at[4]))
    for copy in copies:
        copy.start()
    y_inverse(r_ref, rest, HC, ly)
    finish(grid_modes(ly, vy, tt_ref), zt_ref, sp, out_v, pl.ds(rest, HC), pl.ds(0, HC))
    copies.append(
        pltpu.make_async_copy(
            out_v, out_hbm.at[0, every, every, every, pl.ds(rest, HC)], osem.at[5]
        )
    )
    copies[5].start()
    for copy in copies:
        copy.wait()


def body(field, cotangent, w_spec, w_local):
    table, zf = line_table(), z_table()
    t, tt, zf, zt = (jnp.asarray(m.astype(jnp.bfloat16)) for m in (table, table.T, zf, zf.T))
    grid = (4, 8, 8, CH, NZ)
    any_spec = pl.BlockSpec(memory_space=pltpu.HBM)
    vmem_spec = pl.BlockSpec(memory_space=pltpu.VMEM)
    pencil_buf = pltpu.VMEM((16, CH, 128), BF16)
    dp_buf = pltpu.VMEM((16, 16, 128), BF16)
    both = pltpu.VMEM((2, 8, 16, 128), BF16)
    row = pltpu.VMEM((8, 16, 128), BF16)
    grid_b16 = pltpu.VMEM(grid, BF16)
    line = pltpu.VMEM((1024, 256), BF16)
    line_t = pltpu.VMEM((256, 1024), BF16)
    keep = pltpu.VMEM((2, MZ, 16, 128), BF16)
    r3, sp, gw, tt, zt, done = pl.pallas_call(
        kernel,
        out_shape=(
            pencil_buf,
            grid_b16,
            pltpu.VMEM((MZ, CH, 2 * CH), F32),
            line_t,
            line_t,
            pltpu.VMEM((4, 8, 8, CH - HC, NZ), BF16),
        ),
        in_specs=[any_spec] * 8,
        out_specs=[vmem_spec] * 6,
        scratch_shapes=[
            grid_b16,
            grid_b16,
            pltpu.VMEM((8, MZ, CH, 2 * CH), BF16),
            pltpu.VMEM((CH, CH), BF16),
            line,
            line,
            pltpu.VMEM(grid, F32),
            grid_b16,
            pltpu.VMEM((8 * HC, 1024), BF16),
            pltpu.VMEM((8 * HC, 256), BF16),
            pltpu.VMEM((8 * HC, 1024), BF16),
            pltpu.VMEM((128, 256), F32),
            pltpu.VMEM((128, 256), BF16),
            pltpu.VMEM((2, 256, 256), BF16),
            pltpu.VMEM((256, 128), F32),
            keep,
        ]
        + [pencil_buf] * 7
        + [both, dp_buf, both, dp_buf, row, both, row, row, both, row]
        + [
            pltpu.SemaphoreType.DMA((11,)),
            pltpu.SemaphoreType.DMA((18,)),
            pltpu.SemaphoreType.DMA((18,)),
            pltpu.SemaphoreType.DMA((14,)),
            pltpu.SemaphoreType.DMA((14,)),
            pltpu.SemaphoreType.DMA((4,)),
            pltpu.SemaphoreType.DMA((4,)),
        ],
        compiler_params=pltpu.CompilerParams(
            collective_id=0, has_side_effects=True, vmem_limit_bytes=57_700_000
        ),
        name="layer",
    )(field.reshape((1,) + grid), cotangent.reshape((1,) + grid), w_spec, w_local, t, tt, zf, zt)
    out, gw = pl.pallas_call(
        last_kernel,
        out_shape=(
            jax.ShapeDtypeStruct((1,) + grid, BF16),
            jax.ShapeDtypeStruct((1, 1, MZ, CH, 2 * CH), F32),
        ),
        in_specs=[vmem_spec] * 6,
        out_specs=[any_spec] * 2,
        scratch_shapes=[
            pltpu.VMEM((8 * HC, 256), BF16),
            pltpu.VMEM((8 * HC, 1024), BF16),
            pltpu.VMEM((4, 8, 8, HC, NZ), BF16),
            pltpu.SemaphoreType.DMA((6,)),
        ],
        compiler_params=pltpu.CompilerParams(vmem_limit_bytes=20 * 1024 * 1024),
        name="last",
    )(r3, sp, gw, tt, zt, done)
    return (out.reshape(1, 4, NY, CH, NZ), gw)


def solution(mesh):
    placed = P("dp", "pencil", None, None, None)
    return jax.shard_map(
        body,
        mesh=mesh,
        in_specs=(placed, placed, placed, P()),
        out_specs=(placed, placed),
        check_vma=False,
    )
```

```python
import functools
import math

import jax
import jax.numpy as jnp
import numpy as np
from jax import lax
from jax.experimental import pallas as pl
from jax.experimental.pallas import tpu as pltpu
from jax.sharding import PartitionSpec as P

NX = 64
NY = 64
NZ = 128
CH = 64
MX = 16
MY = 16
MZ = 16
KH = 8
MESH = pl.DeviceIdType.MESH
F32 = jnp.float32
BF16 = jnp.bfloat16
CHUNKS = 4
HC = CH // CHUNKS
EARLY = 2
SCALE = 1.0 / (NX * NY * NZ)


def line_table():
    position = np.arange(NX)
    freq = np.arange(MX)
    freq = np.where(freq < MX // 2, freq, freq - MX)
    angle = 2.0 * math.pi * np.mod(position[:, None] * freq[None, :], NX) / NX
    cos, sin = np.cos(angle).reshape(8, 2, 4, MX), np.sin(angle).reshape(8, 2, 4, MX)
    table = np.zeros((8, 2, 2, 4, KH, 2, MX, KH), np.float32)
    for k in range(KH):
        table[:, :, 0, :, k, 0, :, k] = cos
        table[:, :, 1, :, k, 0, :, k] = sin
        table[:, :, 1, :, k, 1, :, k] = cos
        table[:, :, 0, :, k, 1, :, k] = -sin
    return table.reshape(1024, 256)


def z_table():
    angle = 2.0 * math.pi * np.mod(np.arange(NZ)[:, None] * np.arange(MZ)[None, :], NZ) / NZ
    angle = angle.reshape(NZ, 2, KH)
    table = np.zeros((2, 4, NZ, 2, 2, 2, 4, KH), np.float32)
    for half in range(2):
        for q in range(4):
            table[half, q, :, :, half, 0, q, :] = np.cos(angle)
            table[half, q, :, :, half, 1, q, :] = -np.sin(angle)
    return table.reshape(1024, 256)


def dot(a, b):
    return jnp.dot(a, b, preferred_element_type=F32)


def dot_t(a, b):
    return lax.dot_general(a, b, (((1,), (1,)), ((), ())), preferred_element_type=F32)


def gelu_slope_twice(t):
    bell = jnp.exp2(t * t * (-1.0 / math.log(2.0)) + math.log2(2.0 / math.sqrt(math.pi)))
    return lax.erf(t) + (t * bell + 1.0)


def roll(v, amount):
    amount %= 128
    return v if amount == 0 else pltpu.roll(v, amount, 1)


def halves(low, high):
    lane = lax.broadcasted_iota(jnp.int32, low.shape, 1)
    return jnp.where(lane < 64, low, high)


def slot_masks(rows):
    slot = lax.broadcasted_iota(jnp.int32, (rows, 128), 1) // KH
    return [slot == m for m in range(16)]


def turn_slots(masks, get, put):
    rolled = [roll(get(j), KH * j) for j in range(16)]
    for e in range(16):
        out = rolled[(0 - e) % 16]
        for m in range(1, 16):
            out = jnp.where(masks[m], rolled[(m - e) % 16], out)
        put(e, roll(out, -KH * e))


def y_inverse(rb, c0, rows, ly):
    masks = slot_masks(rows)

    def put(e, tile):
        kh, ri, x = e // 8, (e // 4) % 2, e % 4
        at = (kh * 4 + x) * rows
        ly[at : at + rows, ri * 128 : (ri + 1) * 128] = tile.astype(BF16)

    turn_slots(masks, lambda j: rb[j, pl.ds(c0, rows), :].astype(F32), put)


def grid_modes(ly, vy, tt_ref):
    vy[...] = dot(ly[...], tt_ref[...]).astype(BF16)
    return jnp.concatenate(
        [
            jnp.concatenate(
                [
                    vy[(kh * 4 + x) * HC : (kh * 4 + x + 1) * HC, g * 128 : (g + 1) * 128]
                    for kh in range(2)
                ],
                axis=1,
            )
            for x in range(4)
            for g in range(8)
        ],
        axis=0,
    )


def finish(lhs, zt_ref, sp, dst, c_from, c_to):
    for n in range(4):
        v = dot(lhs, zt_ref[:, n * 256 : (n + 1) * 256])
        for i in range(2):
            p = 2 * n + i
            part = v[:, i * 128 : (i + 1) * 128].reshape(4, 8, HC, 128)
            dst[:, :, p, c_to] = (part + sp[:, :, p, c_from].astype(F32)).astype(BF16)


def kernel(
    field_hbm, cot_hbm, w_hbm, wl_hbm, t_hbm, tt_hbm, zf_hbm, zt_hbm,
    r3, sp, gw_v, tt_ref, zt_ref, out_v,
    f_ref, c_ref, wall, wl_ref, t_ref, zf_ref, big, slope,
    a2, ly, vy, xo, xi, bw, xf, ukeep,
    s0, r0, s1, r1, s2, r2, s3,
    us, ur, gs, gr, row_u, row_v, back_v, row_g, row_d, back_d,
    lsem, ssem, rsem, wssem, wrsem, yssem, yrsem,
):
    me_d = lax.axis_index("dp")
    me_p = lax.axis_index("pencil")
    me_x, me_y, me_c = me_d // 4, lax.rem(me_d // 2, 2), lax.rem(me_d, 2)
    x_up, x_down, x_far = lax.rem(me_x + 1, 4), lax.rem(me_x + 3, 4), lax.rem(me_x + 2, 4)
    partner = me_d + 2 - 4 * me_y

    def load(src, dst, i):
        return pltpu.make_async_copy(src, dst, lsem.at[i])

    def rows_of(h):
        return pl.ds(pl.multiple_of(h * HC, HC), HC)

    every = slice(None)
    loads = [
        load(
            field_hbm.at[0, every, every, every, rows_of(h)],
            f_ref.at[every, every, every, rows_of(h)],
            h,
        )
        for h in range(CHUNKS)
    ]
    loads += [
        load(zf_hbm, zf_ref, 4),
        load(t_hbm, t_ref, 5),
        load(w_hbm.at[0, 0], wall.at[2 * me_x + me_c], 6),
        load(wl_hbm, wl_ref, 7),
        load(cot_hbm.at[0], c_ref, 8),
        load(tt_hbm, tt_ref, 9),
        load(zt_hbm, zt_ref, 10),
    ]
    for i in (4, 0, 5, 6, 1, 2, 3, 7, 9, 10, 8):
        loads[i].start()

    barrier = pltpu.get_barrier_semaphore()

    @pl.loop(1, 16)
    def _(d):
        pl.semaphore_signal(
            barrier, inc=1, device_id=(me_d, lax.rem(me_p + d, 16)), device_id_type=MESH
        )
        pl.semaphore_signal(
            barrier, inc=1, device_id=(lax.rem(me_d + d, 16), me_p), device_id_type=MESH
        )

    def send_pencil(e, sb, rb, h):
        for d in (8, 7, 9, 6, 10, 5, 11, 4, 12, 3, 13, 2, 14, 1, 15):
            to = lax.rem(me_p + d, 16)
            pltpu.make_async_remote_copy(
                src_ref=sb.at[to, rows_of(h)],
                dst_ref=rb.at[me_p, rows_of(h)],
                send_sem=ssem.at[e],
                recv_sem=rsem.at[e],
                device_id=(me_d, to),
                device_id_type=MESH,
            ).start()

    def keep_pencil(sb, rb, h):
        rb[me_p, rows_of(h)] = sb[me_p, rows_of(h)]

    def place(d):
        return lax.rem(d // 2, 2), 2 * (d // 4) + lax.rem(d, 2)

    def send_dp(e, sb, rb):
        @pl.loop(1, 16)
        def _(d):
            to = lax.rem(me_d + d, 16)
            pltpu.make_async_remote_copy(
                src_ref=sb.at[place(to)],
                dst_ref=rb.at[me_d],
                send_sem=ssem.at[e],
                recv_sem=rsem.at[e],
                device_id=(to, me_p),
                device_id_type=MESH,
            ).start()

        rb[me_d] = sb[place(me_d)]

    def swap(i, src, dst):
        return pltpu.make_async_remote_copy(
            src_ref=src,
            dst_ref=dst,
            send_sem=yssem.at[i],
            recv_sem=yrsem.at[i],
            device_id=(partner, me_p),
            device_id_type=MESH,
        )

    def piece(x, c):
        return 2 * x + c

    def part(r, half):
        return wall.at[r, pl.ds(half * KH, KH)]

    def weights(i, r, half, x, c):
        return pltpu.make_async_remote_copy(
            src_ref=part(r, half),
            dst_ref=part(r, half),
            send_sem=wssem.at[i],
            recv_sem=wrsem.at[i],
            device_id=(4 * x + 2 * me_y + c, me_p),
            device_id_type=MESH,
        )

    sib = 1 - me_c
    own, up, down, far = (piece(x, me_c) for x in (me_x, x_up, x_down, x_far))
    moves = [
        weights(0, own, 0, x_up, me_c),
        weights(1, own, 1, x_down, me_c),
        weights(2, own, 1, x_up, me_c),
        weights(3, own, 0, x_down, me_c),
        weights(4, own, 0, me_x, sib),
        weights(5, own, 1, me_x, sib),
        weights(6, down, 0, x_up, me_c),
        weights(7, up, 1, x_down, me_c),
        weights(8, down, 0, me_x, sib),
        weights(9, up, 1, me_x, sib),
        weights(10, down, 1, me_x, sib),
        weights(11, up, 0, me_x, sib),
        weights(12, far, 0, me_x, sib),
        weights(13, far, 1, me_x, sib),
    ]

    def arrived(i):
        moves[i].wait_recv()

    def wait_pencil(sem, buf, h):
        part = buf.at[pl.ds(0, 15), rows_of(h)]
        pltpu.make_async_copy(part, part, sem).wait()

    def wait_dp(sem, buf):
        part = buf.at[pl.ds(0, 15)]
        pltpu.make_async_copy(part, part, sem).wait()

    def z_forward(parts):
        a = dot(jnp.concatenate(parts, axis=1), zf_ref[...]).astype(BF16)
        for x in range(4):
            for g in range(8):
                for kh in range(2):
                    a2[(kh * 4 + x) * HC : (kh * 4 + x + 1) * HC, g * 128 : (g + 1) * 128] = a[
                        (x * 8 + g) * HC : (x * 8 + g + 1) * HC, kh * 128 : (kh + 1) * 128
                    ]

    def y_forward(sb, h):
        y = dot(a2[...], t_ref[...])

        def get(e):
            kh, ri, x = e // 8, (e // 4) % 2, e % 4
            at = (kh * 4 + x) * HC
            return y[at : at + HC, ri * 128 : (ri + 1) * 128]

        def put(j, tile):
            sb[j, rows_of(h), :] = tile.astype(BF16)

        turn_slots(slot_masks(HC), get, put)

    def x_forward(rb, h):
        low, high = [], []
        for g in range(8):
            a = rb[2 * g, h * HC : (h + 1) * HC, :].astype(F32)
            b = roll(rb[2 * g + 1, h * HC : (h + 1) * HC, :].astype(F32), 64)
            low.append(halves(a, b).astype(BF16))
            high.append(roll(halves(b, a), 64).astype(BF16))
        lhs = jnp.concatenate(
            [jnp.concatenate(low, axis=1), jnp.concatenate(high, axis=1)], axis=0
        )
        o = dot(lhs, t_ref[...])
        for kh in range(2):
            xo[kh * CH + h * HC : kh * CH + (h + 1) * HC, :] = o[kh * HC : (kh + 1) * HC]

    def modes_out(dst, scaled):
        turned = xo[...].T
        if scaled:
            row = lax.broadcasted_iota(jnp.int32, (256, 128), 0)
            lane = lax.broadcasted_iota(jnp.int32, (256, 128), 1)
            zero = ((row % KH) == 0) & (lane < 64)
            turned = turned * jnp.where(zero, 0.5 * SCALE, SCALE)
        for j in range(16):
            dst[(j // 2) % 2, 2 * (j // 4) + j % 2] = jnp.concatenate(
                [turned[j * 8 : j * 8 + 8], turned[128 + j * 8 : 136 + j * 8]], axis=0
            ).astype(BF16)

    def modes_in(src):
        v = [src[(j // 2) % 2, 2 * (j // 4) + j % 2].astype(F32) for j in range(16)]
        both = jnp.concatenate([t[:8] for t in v] + [t[8:] for t in v], axis=0)
        xi[...] = both.T.astype(BF16)

    def x_inverse(sb, send):
        o = dot(xi[...], tt_ref[...])
        for h in range(CHUNKS):
            for g in range(8):
                low = o[h * HC : (h + 1) * HC, g * 128 : (g + 1) * 128]
                high = o[CH + h * HC : CH + (h + 1) * HC, g * 128 : (g + 1) * 128]
                sb[2 * g, h * HC : (h + 1) * HC, :] = halves(low, roll(high, 64)).astype(BF16)
                sb[2 * g + 1, h * HC : (h + 1) * HC, :] = halves(roll(low, 64), high).astype(BF16)
            send(h)

    def mix(lhs, src, dst, scale, first, last):
        @pl.loop(first, last)
        def _(x):
            for g in range(8):
                rhs = jnp.concatenate(
                    [src[x, g, :4].reshape(256, 128), src[x, g, 4:].reshape(256, 128)], axis=1
                )
                o = dot(lhs, rhs)
                o = (o if scale is None else o * scale).astype(dst.dtype)
                dst[x, g, :4] = o[:, :128].reshape(4, CH, 128)
                dst[x, g, 4:] = o[:, 128:].reshape(4, CH, 128)

    loads[4].wait()
    for h in range(CHUNKS):
        loads[h].wait()
        z_forward(
            [
                f_ref[:, :, p, h * HC : (h + 1) * HC, :].reshape(32 * HC, 128)
                for p in range(8)
            ]
        )
        if h == 0:
            loads[5].wait()
        y_forward(s0, h)
        if h == 0:
            loads[6].wait()
            pl.semaphore_wait(barrier, 30)
        send_pencil(h, s0, r0, h)
        if h == 0:
            for i in range(6):
                moves[i].start()
        keep_pencil(s0, r0, h)

    loads[7].wait()
    lane64 = lax.broadcasted_iota(jnp.int32, (64, 128), 1)
    wl = wl_ref[...].astype(F32)
    wide = jnp.concatenate([wl] * 4, axis=1)
    tall = jnp.concatenate([wide] * 4, axis=0)
    row = lax.broadcasted_iota(jnp.int32, (256, 256), 0) // 64
    col = lax.broadcasted_iota(jnp.int32, (256, 256), 1) // 64
    block = jnp.where(row == col, tall, 0.0)
    bw[0] = block.T.astype(BF16)
    bw[1] = (0.5 * block).astype(BF16)
    mix(bw[0], f_ref, big, math.sqrt(0.5), 0, 2)
    arrived(0)
    arrived(1)
    for i in range(6, 10):
        moves[i].start()
    mix(bw[0], f_ref, big, math.sqrt(0.5), 2, 4)

    for h in range(CHUNKS):
        wait_pencil(rsem.at[h], r0, h)
        x_forward(r0, h)
        if h == 1:
            arrived(2)
            arrived(3)
            moves[10].start()
            moves[11].start()
    modes_out(us, False)
    ask_u = swap(0, us.at[1 - me_y], row_u)
    ask_u.start()
    arrived(6)
    arrived(7)
    moves[12].start()
    moves[13].start()
    loads[9].wait()
    loads[10].wait()
    loads[8].wait()

    row16 = lax.broadcasted_iota(jnp.int32, (16, 128), 0)
    lane16 = lax.broadcasted_iota(jnp.int32, (16, 128), 1)
    block16 = [(row16 % KH) == (2 * t + lane16 // 64) for t in range(4)]
    sign8 = jnp.where(lax.broadcasted_iota(jnp.int32, (8, 128), 1) < 64, -1.0, 1.0)
    first8 = lax.broadcasted_iota(jnp.int32, (8, 128), 0) == 0
    root = math.sqrt(0.5)

    def forward_mode(u, r):
        u = u.astype(F32)
        turned = roll(u, 64)
        v = []
        for kh in range(2):
            twice = halves(u, turned) if kh == 0 else halves(turned, u)
            lhs = jnp.concatenate([jnp.where(m, twice, 0.0) for m in block16], axis=1)
            o = dot(lhs.astype(BF16), wall[r, kh * KH : (kh + 1) * KH].reshape(512, 128))
            o = o[:8] + sign8 * roll(o[8:], 64)
            scale = jnp.where(first8, root * SCALE, 2.0 * root * SCALE) if kh == 0 else 2.0 * root * SCALE
            v.append(o * scale)
        return jnp.concatenate(
            [halves(v[0], roll(v[1], 64)), halves(roll(v[0], 64), v[1])], axis=0
        ).astype(BF16)

    def adjoint_mode(g, r):
        g = g.astype(F32)
        re, im = g[:8], g[8:]
        re_t, im_t = roll(re, 64), roll(im, 64)
        d = []
        for kh in range(2):
            if kh == 0:
                lhs = [halves(re, im_t), halves(im, -re_t)]
            else:
                lhs = [halves(re_t, im), halves(im_t, -re)]
            lhs = jnp.concatenate(lhs, axis=0).astype(BF16)
            o = dot_t(lhs, wall[r, kh * KH : (kh + 1) * KH].reshape(512, 128))
            o = sum(jnp.where(block16[t], o[:, t * 128 : (t + 1) * 128], 0.0) for t in range(4))
            d.append(o + roll(o, 64))
        return halves(d[0], d[1]).astype(BF16)

    def local_modes(mode, src, dst, pieces):
        for r in pieces:
            dst[me_y, r] = mode(src[me_y, r], r)

    def row_modes(mode, src, dst):
        for r in range(8):
            dst[r] = mode(src[r], r)

    local_modes(forward_mode, us, row_v, (own, up, down, far))
    for i in (4, 5, 8, 9, 10, 11, 12, 13):
        arrived(i)
    ask_u.wait_recv()
    row_modes(forward_mode, row_u, back_v)
    give_v = swap(1, back_v, row_v.at[me_y])
    give_v.start()
    local_modes(forward_mode, us, row_v, [piece(x, sib) for x in (me_x, x_up, x_down, x_far)])
    send_dp(16, us, ur)
    give_v.wait_recv()
    modes_in(row_v)
    x_inverse(s1, lambda h: send_pencil(4 + h, s1, r1, h))
    for h in range(CHUNKS):
        keep_pencil(s1, r1, h)

    @pl.loop(0, CHUNKS)
    def _(h):
        wait_pencil(rsem.at[4 + h], r1, h)
        y_inverse(r1, pl.multiple_of(h * HC, HC), HC, ly)
        lhs = grid_modes(ly, vy, tt_ref)
        parts = []
        for n in range(4):
            v = dot(lhs, zt_ref[:, n * 256 : (n + 1) * 256])
            for i in range(2):
                at = (every, every, 2 * n + i, rows_of(h))
                t = v[:, i * 128 : (i + 1) * 128].reshape(4, 8, HC, 128) + big[at]
                sl = (c_ref[at].astype(F32) * gelu_slope_twice(t)).astype(BF16)
                slope[at] = sl
                parts.append(sl.reshape(32 * HC, 128))
        z_forward(parts)
        y_forward(s2, h)
        send_pencil(8 + h, s2, r2, h)
        keep_pencil(s2, r2, h)

    mix(bw[1], slope, sp, None, 0, 4)

    for h in range(CHUNKS):
        wait_pencil(rsem.at[8 + h], r2, h)
        x_forward(r2, h)
    modes_out(gs, True)
    ask_g = swap(2, gs.at[1 - me_y], row_g)
    ask_g.start()
    local_modes(adjoint_mode, gs, row_d, range(8))
    ask_g.wait_recv()
    row_modes(adjoint_mode, row_g, back_d)
    give_d = swap(3, back_d, row_d.at[me_y])
    give_d.start()
    send_dp(17, gs, gr)
    give_d.wait_recv()
    modes_in(row_d)
    x_inverse(s3, lambda h: send_pencil(12 + h, s3, r3, h))
    r3[me_p] = s3[me_p]

    def regroup(src, i):
        xf[...] = src[...].astype(F32).reshape(256, 128)
        for k in range(KH):
            re = xf[pl.ds(k, 16, stride=16), :]
            im = xf[pl.ds(KH + k, 16, stride=16), :]
            ukeep[i, k] = halves(re, roll(im, 64)).astype(BF16)
            ukeep[i, KH + k] = halves(roll(re, 64), im).astype(BF16)

    wait_dp(rsem.at[16], ur)
    regroup(ur, 0)
    wait_dp(rsem.at[17], gr)
    regroup(gr, 1)
    for k in range(MZ):
        cross = lax.dot_general(
            ukeep[0, k], ukeep[1, k], (((0,), (0,)), ((), ())), preferred_element_type=F32
        )
        low = roll(cross[64:], 64)
        gw_v[k] = cross[:64] + jnp.where(lane64 < 64, low, -low)

    @pl.loop(0, EARLY)
    def _(h):
        wait_pencil(rsem.at[12 + h], r3, h)
        y_inverse(r3, pl.multiple_of(h * HC, HC), HC, ly)
        finish(grid_modes(ly, vy, tt_ref), zt_ref, sp, out_v, rows_of(h), rows_of(h))

    for copy in moves + [ask_u, give_v, ask_g, give_d]:
        copy.wait_send()
    for h in range(CHUNKS):
        wait_pencil(ssem.at[h], s0, h)
        wait_pencil(ssem.at[4 + h], s1, h)
        wait_pencil(ssem.at[8 + h], s2, h)
    wait_dp(ssem.at[16], ur)
    wait_dp(ssem.at[17], gr)
    for h in range(CHUNKS):
        wait_pencil(ssem.at[12 + h], s3, h)
    for h in range(EARLY, CHUNKS):
        wait_pencil(rsem.at[12 + h], r3, h)


def last_kernel(
    r_ref, sp, gw_v, tt_ref, zt_ref, done, out_hbm, gw_hbm, ly, vy, out_v, osem,
):
    every = slice(None)
    copies = [
        pltpu.make_async_copy(
            done.at[x], out_hbm.at[0, x, every, every, pl.ds(0, EARLY * HC)], osem.at[x]
        )
        for x in range(4)
    ]
    copies.append(pltpu.make_async_copy(gw_v, gw_hbm.at[0, 0], osem.at[4]))
    for copy in copies:
        copy.start()
    for h in range(EARLY, CHUNKS):
        i = h - EARLY
        y_inverse(r_ref, h * HC, HC, ly.at[i])
        lhs = grid_modes(ly.at[i], vy.at[i], tt_ref)
        finish(lhs, zt_ref, sp, out_v.at[i], pl.ds(h * HC, HC), every)
        copies.append(
            pltpu.make_async_copy(
                out_v.at[i], out_hbm.at[0, every, every, every, pl.ds(h * HC, HC)], osem.at[5 + i]
            )
        )
        copies[5 + i].start()
    for copy in copies:
        copy.wait()


def body(field, cotangent, w_spec, w_local):
    table, zf = line_table(), z_table()
    t, tt, zf, zt = (jnp.asarray(m.astype(jnp.bfloat16)) for m in (table, table.T, zf, zf.T))
    grid = (4, 8, 8, CH, NZ)
    any_spec = pl.BlockSpec(memory_space=pltpu.HBM)
    vmem_spec = pl.BlockSpec(memory_space=pltpu.VMEM)
    pencil_buf = pltpu.VMEM((16, CH, 128), BF16)
    dp_buf = pltpu.VMEM((16, 16, 128), BF16)
    both = pltpu.VMEM((2, 8, 16, 128), BF16)
    row = pltpu.VMEM((8, 16, 128), BF16)
    grid_b16 = pltpu.VMEM(grid, BF16)
    line = pltpu.VMEM((1024, 256), BF16)
    line_t = pltpu.VMEM((256, 1024), BF16)
    keep = pltpu.VMEM((2, MZ, 16, 128), BF16)
    r3, sp, gw, tt, zt, done = pl.pallas_call(
        kernel,
        out_shape=(
            pencil_buf,
            grid_b16,
            pltpu.VMEM((MZ, CH, 2 * CH), F32),
            line_t,
            line_t,
            pltpu.VMEM((4, 8, 8, EARLY * HC, NZ), BF16),
        ),
        in_specs=[any_spec] * 8,
        out_specs=[vmem_spec] * 6,
        scratch_shapes=[
            grid_b16,
            grid_b16,
            pltpu.VMEM((8, MZ, CH, 2 * CH), BF16),
            pltpu.VMEM((CH, CH), BF16),
            line,
            line,
            pltpu.VMEM(grid, F32),
            grid_b16,
            pltpu.VMEM((8 * HC, 1024), BF16),
            pltpu.VMEM((8 * HC, 256), BF16),
            pltpu.VMEM((8 * HC, 1024), BF16),
            pltpu.VMEM((128, 256), F32),
            pltpu.VMEM((128, 256), BF16),
            pltpu.VMEM((2, 256, 256), BF16),
            pltpu.VMEM((256, 128), F32),
            keep,
        ]
        + [pencil_buf] * 7
        + [both, dp_buf, both, dp_buf, row, both, row, row, both, row]
        + [
            pltpu.SemaphoreType.DMA((11,)),
            pltpu.SemaphoreType.DMA((18,)),
            pltpu.SemaphoreType.DMA((18,)),
            pltpu.SemaphoreType.DMA((14,)),
            pltpu.SemaphoreType.DMA((14,)),
            pltpu.SemaphoreType.DMA((4,)),
            pltpu.SemaphoreType.DMA((4,)),
        ],
        compiler_params=pltpu.CompilerParams(
            collective_id=0, has_side_effects=True, vmem_limit_bytes=58_700_000
        ),
        name="layer",
    )(field.reshape((1,) + grid), cotangent.reshape((1,) + grid), w_spec, w_local, t, tt, zf, zt)
    out, gw = pl.pallas_call(
        last_kernel,
        out_shape=(
            jax.ShapeDtypeStruct((1,) + grid, BF16),
            jax.ShapeDtypeStruct((1, 1, MZ, CH, 2 * CH), F32),
        ),
        in_specs=[vmem_spec] * 6,
        out_specs=[any_spec] * 2,
        scratch_shapes=[
            pltpu.VMEM((CHUNKS - EARLY, 8 * HC, 256), BF16),
            pltpu.VMEM((CHUNKS - EARLY, 8 * HC, 1024), BF16),
            pltpu.VMEM((CHUNKS - EARLY, 4, 8, 8, HC, NZ), BF16),
            pltpu.SemaphoreType.DMA((5 + CHUNKS - EARLY,)),
        ],
        compiler_params=pltpu.CompilerParams(vmem_limit_bytes=20 * 1024 * 1024),
        name="last",
    )(r3, sp, gw, tt, zt, done)
    return (out.reshape(1, 4, NY, CH, NZ), gw)


def solution(mesh):
    placed = P("dp", "pencil", None, None, None)
    return jax.shard_map(
        body,
        mesh=mesh,
        in_specs=(placed, placed, placed, P()),
        out_specs=(placed, placed),
        check_vma=False,
    )
```
